32 devices in a mesh: grp: 4 (over y, x), clu: 8 (over z, core).
Axes of the slice: x: 2, y: 2, z: 4, core: 2. Of those that a mesh axis runs over, the one named last changes fastest.
Arguments:
- forces: bfloat16 [3, 2048, 512], P(None, 'clu'), may hold values from -6 to 6
- order: int32 [2048], P('clu'), may hold values from 0 to 2047, as said below
- bases: bfloat16 [2, 32, 3, 2048], P(None, None, None, 'clu'), may hold values from -0.21875 to 0.21875
- near_tiles: bfloat16 [8, 8, 768, 768], P('clu', 'grp'), may hold values from -0.078125 to 0.078125
- near_col: int32 [8, 8], P('clu', 'grp'), may hold values from 0 to 7, as said below
- far_basis: bfloat16 [8, 64, 32, 768], P('clu', 'grp'), may hold values from -0.125 to 0.125
- far_coupling: bfloat16 [8, 64, 32, 32], P('clu', 'grp'), may hold values from -1 to 1
- far_scale: float32 [8, 64], P('clu', 'grp'), may hold values from 0.5 to 2
- far_rank: int32 [8, 64], P('clu', 'grp'), may hold values from 8 to 32
- far_target: int32 [8, 64], P('clu', 'grp'), may hold values from 0 to 5, as said below
Outputs:
- velocity: float32 [3, 2048, 512], P(None, 'clu', 'grp')
The draws below stay inside these ranges and needn't reach their ends.
Inputs may be any that keep to these rules, and one draw needn't show every extreme that they name: `order`: A permutation of the bead numbers; the 256 positions of row block c hold beads of chain blocks c - 1, c and c + 1 only, counted cyclically, exactly 64 of them from chain block c - 1 and exactly 64 from chain block c + 1. `near_col`: each near tile's column block lies within two blocks of its row block, counted cyclically. `far_target`: level l takes indices 2 ** (l + 1) - 2 to 2 ** (l + 2) - 3; the named cluster never contains the block's own row block.
All inputs are finite; a program needn't handle non-finite values.
Results may differ from the reference program's by a relative error of at most 0.0025.
Values may be sent and summed in bfloat16 or wider, within the bound.
A program may use at most 64 MiB of HBM per device.

```python
import math
import jax
import jax.numpy as jnp
from jax import lax

TILE = 256
RANK = 32
LEVELS = 2
NRHS = 512
FAR_DEV = 16
N_BEADS = 2048
NEARS = 8
FARS = 64
N_CLU = 8


def draw_order(key, part):
    clusters = N_BEADS // TILE
    quarter = TILE // 4
    first_key, second_key = jax.random.split(jax.random.fold_in(key, 11))
    chain_perm = jax.vmap(lambda k: jax.random.permutation(k, TILE))(jax.random.split(first_key, clusters))
    beads = (chain_perm + jnp.arange(clusters)[:, None] * TILE).astype(jnp.int32)
    to_left = beads[:, :quarter]
    to_right = beads[:, quarter:2 * quarter]
    staying = beads[:, 2 * quarter:]
    grouped = jnp.concatenate([staying, jnp.roll(to_left, -1, axis=0), jnp.roll(to_right, 1, axis=0)], axis=1)
    shuffle = jax.vmap(lambda k: jax.random.permutation(k, TILE))(jax.random.split(second_key, clusters))
    grouped = jnp.take_along_axis(grouped, shuffle, axis=1)
    return grouped.reshape(-1).astype(jnp.int32)


def draw_near_col(key, part):
    clusters = N_BEADS // TILE
    offsets = jax.random.randint(jax.random.fold_in(key, 23), (clusters, NEARS), -2, 3)
    rows = jnp.arange(clusters, dtype=jnp.int32)[:, None]
    return jnp.mod(rows + offsets, clusters).astype(jnp.int32)


def draw_far_target(key, part):
    clusters = N_BEADS // TILE
    level_key, step_key = jax.random.split(jax.random.fold_in(key, 37))
    level = jax.random.randint(level_key, (clusters, FARS), 0, LEVELS)
    count = jnp.left_shift(jnp.full((clusters, FARS), 2, jnp.int32), level.astype(jnp.int32))
    members = clusters // count
    rows = jnp.arange(clusters, dtype=jnp.int32)[:, None]
    own = rows // members
    step = jax.random.randint(step_key, (clusters, FARS), 0, count - 1)
    target = jnp.mod(own + 1 + step, count)
    return (count - 2 + target).astype(jnp.int32)


def place_ends(result, own_key, smallest, largest):
    dims = result.shape
    spot = [jax.random.randint(jax.random.fold_in(own_key, axis), (), 0, dims[axis]) for axis in range(len(dims))]
    result = result.at[tuple(spot)].set(smallest)
    longest = dims.index(max(dims))
    spot[longest] = (spot[longest] + 1) % dims[longest]
    return result.at[tuple(spot)].set(largest)


def shard_levels(stream_key, extent, cuts, least, top_value):
    factor_of, own = 1.0, jax.random.fold_in(stream_key, 6)
    for axis_at, parts in cuts:
        steps = jnp.exp(jax.random.uniform(jax.random.fold_in(own, axis_at), (parts,), jnp.float32, least / len(cuts), top_value / len(cuts)))
        factor_of = factor_of * jnp.repeat(steps, extent[axis_at] // parts).reshape([-1 if axis == axis_at else 1 for axis in range(len(extent))])
    return factor_of


def gaussian(own_key, extent, width, reach, cuts=(), held_as=jnp.bfloat16):
    drawn = width * jax.random.normal(own_key, extent, jnp.float32)
    if cuts:
        drawn = drawn * shard_levels(own_key, extent, cuts, -0.22, 0.18)
    return jnp.clip(drawn, -reach, reach).astype(held_as)


def setup_inputs(seed: int = 0) -> dict:
    keys = jax.random.split(jax.random.key(seed), 11)
    return {
        "forces": gaussian(keys[0], (3, N_BEADS, NRHS), 1.0, 6.0, ((1, 8),)),
        "order": draw_order(jax.random.fold_in(keys[10], 71), 0),
        "bases": gaussian(keys[2], (LEVELS, RANK, 3, N_BEADS), (3 * TILE) ** -0.5, 0.21875, ((3, 8),)),
        "near_tiles": gaussian(keys[3], (N_CLU, NEARS, 3 * TILE, 3 * TILE), (3 * TILE * NEARS) ** -0.5, 0.078125, ((0, 8), (1, 4))),
        "near_col": draw_near_col(jax.random.fold_in(keys[10], 71), 0),
        "far_basis": gaussian(keys[5], (N_CLU, FARS, RANK, 3 * TILE), (FAR_DEV * RANK * N_CLU // 2) ** -0.5, 0.125, ((0, 8), (1, 4))),
        "far_coupling": gaussian(keys[6], (N_CLU, FARS, RANK, RANK), RANK ** -0.5, 1.0, ((0, 8), (1, 4))),
        "far_scale": jnp.clip(jnp.exp(math.log(2.0) - 1.3862944 * jax.random.uniform(keys[7], (N_CLU, FARS), jnp.float32) ** shard_levels(keys[7], (N_CLU, FARS), ((0, 8), (1, 4)), -0.2, 0.2)), 0.5, 2.0),
        "far_rank": place_ends(jax.random.randint(keys[8], (N_CLU, FARS), 8, RANK + 1), jax.random.fold_in(keys[8], 1), 8, RANK).astype(jnp.int32),
        "far_target": draw_far_target(jax.random.fold_in(keys[10], 71), 0),
    }


def reference(forces, order, bases, near_tiles, near_col, far_basis, far_coupling, far_scale, far_rank, far_target):
    clusters = N_BEADS // TILE
    clustered = jnp.take(forces, order, axis=1)
    blocks = clustered.reshape(3, clusters, TILE, NRHS).transpose(1, 0, 2, 3).reshape(clusters, 3 * TILE, NRHS)
    basis_blocks = bases.reshape(LEVELS, RANK, 3, clusters, TILE).transpose(3, 0, 1, 2, 4).reshape(clusters, LEVELS * RANK, 3 * TILE)

    def piece_of(pair):
        return jnp.dot(pair[0], pair[1], preferred_element_type=jnp.float32)

    pieces = lax.map(piece_of, (basis_blocks, blocks)).reshape(clusters, LEVELS, RANK, NRHS)
    levels_list = []
    for level in range(LEVELS):
        count = 2 ** (level + 1)
        levels_list.append(pieces[:, level].reshape(count, clusters // count, RANK, NRHS).sum(axis=1))
    table = jnp.concatenate(levels_list, axis=0)

    def row(index):
        columns = near_col[index]
        total = jnp.zeros((3 * TILE, NRHS), jnp.float32)
        for slot in range(NEARS):
            total = total + jnp.dot(near_tiles[index, slot], blocks[columns[slot]], preferred_element_type=jnp.float32)
        picked = table[far_target[index]]
        keep = (jnp.arange(RANK, dtype=jnp.int32)[None, :] < far_rank[index][:, None]).astype(jnp.float32)
        masked = picked * keep[:, :, None]
        coupled = jnp.einsum("brs,bsn->brn", far_coupling[index].astype(jnp.float32), masked, precision=lax.Precision.HIGHEST)
        coupled = (coupled * far_scale[index][:, None, None]).astype(jnp.bfloat16)
        far = lax.dot_general(far_basis[index].reshape(FARS * RANK, 3 * TILE), coupled.reshape(FARS * RANK, NRHS), (((0,), (0,)), ((), ())), preferred_element_type=jnp.float32)
        return total + far

    rows = lax.map(row, jnp.arange(clusters, dtype=jnp.int32))
    return rows.reshape(clusters, 3, TILE, NRHS).transpose(1, 0, 2, 3).reshape(3, N_BEADS, NRHS)
```

```python
import functools

import jax
import jax.numpy as jnp
from jax import lax
from jax.experimental import pallas as pl
from jax.experimental.pallas import tpu as pltpu
from jax.sharding import PartitionSpec as P

MESH = pl.DeviceIdType.MESH
F32, BF16 = jnp.float32, jnp.bfloat16
SENDS = 112


def kernel(
    n, groups, levels, rank,
    forces, order_hbm, bases_hbm, tiles_hbm, near_col_hbm, basis_hbm, coupling_hbm, scale_hbm, ranks_hbm, targets_hbm,
    out,
    order, bases, coupling, near_col, scale, ranks, targets,
    raw, ext, ext_out, ext_near, orders, tiles, basis, spread, picks, own_pick, piece_out, piece_mate, pieces,
    table_out, tables, coupled, total, y_out, y_in,
    local_sem, own_sem, send_sem, piece_send, order_recv, mate_recv, raw_recv, ext_recv, near_recv,
    pair_recv, piece_recv, table_recv, y_recv,
):
    g, c = lax.axis_index("grp"), lax.axis_index("clu")
    core = lax.rem(c, 2)
    comps, tile, columns = forces.shape
    width = columns // groups
    quarter = tile // 4
    slots = raw.shape[1]
    rows = comps * tile
    near_count = tiles.shape[0]
    far_count = targets.shape[1]
    half = n // 2
    cut = rank // 2
    piece_rows = levels * cut
    blocks = [(level, 2 ** (level + 1)) for level in range(levels)]
    table_rows = sum(count - 1 for _, count in blocks) * cut
    last = groups - 1

    def at_clu(by):
        return {"grp": g, "clu": lax.rem(c + by + n, n)}

    partners = (g, g + 1 - 2 * lax.rem(g, 2), lax.rem(g + 2, groups), groups - 1 - g)

    def at_grp(i):
        return {"grp": partners[i], "clu": c}

    mate = {"grp": g, "clu": c + 1 - 2 * core}
    sends = []

    def remote(src, dst, recv, where, index=0):
        return pltpu.make_async_remote_copy(
            src_ref=src, dst_ref=dst, send_sem=send_sem.at[index], recv_sem=recv, device_id=where, device_id_type=MESH
        )

    def push(src, dst, recv, where):
        assert len(sends) < SENDS
        copy = remote(src, dst, recv, where, len(sends))
        copy.start()
        sends.append(copy)

    def landed(ref, recv):
        remote(ref, ref, recv, mate).wait_recv()

    def columns_of(i, d):
        return forces.at[d, :, pl.ds(pl.multiple_of(partners[i] * width, width), width)]

    def part(i, slot, d):
        return raw.at[i, slot, :, pl.ds(d * width, width)]

    small = [
        pltpu.make_async_copy(src, dst, local_sem.at[at])
        for at, (src, dst) in enumerate((
            (order_hbm, order), (bases_hbm, bases), (near_col_hbm, near_col), (ranks_hbm, ranks),
            (targets_hbm, targets), (scale_hbm, scale), (coupling_hbm, coupling), (basis_hbm, basis), (tiles_hbm, tiles),
        ))
    ]
    for copy in small[:2]:
        copy.start()
    for i in (0, last, 1, 2):
        for d in range(comps):
            pltpu.make_async_copy(columns_of(i, d), part(i, 2 + core, d), own_sem.at[i]).start()
    for copy in small[2:]:
        copy.start()

    barrier = pltpu.get_barrier_semaphore()

    def greet(d, carry):
        pl.semaphore_signal(barrier, inc=1, device_id=at_clu(d), device_id_type=MESH)
        return carry

    lax.fori_loop(1, n, greet, 0)
    for d in range(1, groups):
        pl.semaphore_signal(barrier, inc=1, device_id=at_grp(d), device_id_type=MESH)

    ext[:, quarter:, :] = jnp.zeros((groups, ext.shape[1] - quarter, ext.shape[2]), BF16)
    ext_near[quarter:, :] = jnp.zeros((ext.shape[1] - quarter, ext.shape[2]), BF16)
    small[0].wait()
    pl.semaphore_wait(barrier, n - 1 + groups - 1)

    offsets = (-1, 1, -2, 2)
    for by in offsets:
        push(order, orders.at[2 - by], order_recv.at[2 - by], at_clu(by))

    def send_z(i, d):
        push(columns_of(i, d), part(i, core, d), raw_recv.at[i, core, d], at_clu(2))
        push(columns_of(i, d), part(i, 4 + core, d), raw_recv.at[i, 4 + core, d], at_clu(-2))

    send_z(last, 0)
    for i in (0, last, 1, 2):
        for d in range(comps):
            push(columns_of(i, d), part(i, 2 + core, d), mate_recv.at[i], mate)

    def relay(i, d, across=False):
        for slot in (core, 4 + core):
            landed(part(i, slot, d), raw_recv.at[i, slot, d])
            if across:
                for to, at in ((1, 2), (2, 1)):
                    push(part(i, slot, d), part(at, slot, d), raw_recv.at[at, slot, d], at_grp(to))
            push(part(i, slot, d), part(i, slot, d), raw_recv.at[i, slot, d], mate)

    def take(i, d):
        for slot in (1 - core, 5 - core):
            landed(part(i, slot, d), raw_recv.at[i, slot, d])

    sub = lax.broadcasted_iota(jnp.int32, (tile, tile), 0)
    lan = lax.broadcasted_iota(jnp.int32, (tile, tile), 1)
    upto = (sub <= lan).astype(BF16)

    def ranked(chosen):
        spots = jnp.broadcast_to(chosen.astype(F32), (8, tile)).astype(BF16)
        return (jnp.dot(spots, upto, preferred_element_type=F32)[0:1, :] - 1.0).astype(jnp.int32)

    def one_hot(cluster_order, first, held, dst):
        spot = cluster_order - first * tile
        spot = jnp.where(spot < 0, spot + n * tile, spot)
        spot = jnp.where(spot >= n * tile, spot - n * tile, spot)
        beyond = spot >= held * tile
        spot = jnp.where(beyond, held * tile + ranked(beyond), spot)
        down = jnp.broadcast_to(spot.astype(F32), (128, tile)).T
        at = lax.broadcasted_iota(jnp.int32, (tile, 128), 1).astype(F32)
        for j in range(dst.shape[1] // 128):
            dst[:, j * 128:(j + 1) * 128] = (down == at + float(j * 128)).astype(F32).astype(BF16)

    one_hot(order[...], c - core, 2, own_pick)

    def whole(i, slot):
        return raw.at[i, slot]

    def own_arrived(i):
        pltpu.make_async_copy(whole(i, 2 + core), whole(i, 2 + core), own_sem.at[i]).wait()

    for i in (0, last):
        own_arrived(i)

    def order_landed(by):
        landed(orders.at[2 + by], order_recv.at[2 + by])

    for by in (-1, 1):
        order_landed(by)
    away = orders[1 + 2 * core] - c * tile
    chosen = (away >= 0) & (away < tile)
    place = jnp.where(chosen, ranked(chosen), -1)
    left = (lax.broadcasted_iota(jnp.int32, (ext.shape[1], tile), 0) == place).astype(F32).astype(BF16)
    right = (sub == away).astype(F32).astype(BF16)
    pick = lax.dot_general(left, right, (((1,), (1,)), ((), ())), preferred_element_type=F32).astype(BF16)
    for at, i in enumerate((0, last)):
        ext_out[at] = jnp.dot(pick, raw[i, 2 + core], preferred_element_type=F32).astype(BF16)[:quarter]
        if i == 0:
            push(ext_out.at[0], ext_near.at[0:quarter], near_recv.at[0], at_clu(2 * core - 1))
    send_z(last, 1)

    def ext_in(i):
        return ext.at[i, 0:quarter]

    def send_ext(at, i):
        push(ext_out.at[at], ext_in(i), ext_recv.at[i], at_clu(6 * core - 3))

    send_ext(1, last)

    for copy in small[1:7]:
        copy.wait()
    lane = lax.broadcasted_iota(jnp.int32, (rank, 2 * table_rows), 1)
    row = lax.broadcasted_iota(jnp.int32, (rank, 2 * table_rows), 0)
    lane_row = (lane // table_rows) * cut + lax.rem(lane, cut)
    lane_slot = lax.rem(lane, table_rows) // cut
    repeat = (lane_row == row).astype(F32).astype(BF16)
    wide = jnp.dot(coupling[...], repeat, preferred_element_type=F32)
    for b in range(far_count):
        target = targets[0, b]
        slot_of, base, offset = target, 0, 0
        for level, count in blocks:
            own = (c // 2) // (half // count)
            here = target - base - own - 1
            here = jnp.where(here < 0, here + count, here) + offset
            slot_of = jnp.where((target >= base) & (target < base + count), here, slot_of)
            base, offset = base + count, offset + count - 1
        keep = (lane_slot == slot_of) & (lane_row < ranks[0, b])
        spread[b * rank:(b + 1) * rank, :] = jnp.where(keep, wide[b * rank:(b + 1) * rank, :], 0.0).astype(BF16)

    relay(last, 0, True)

    landed(ext_near.at[0:quarter], near_recv.at[0])
    own_mate = whole(0, 3 - core)
    landed(own_mate, mate_recv.at[0])
    lanes = comps * width
    x = jnp.dot(own_pick[:, :2 * tile], raw[0, 2:4].reshape(2 * tile, lanes), preferred_element_type=F32)
    x = x + jnp.dot(own_pick[:, 2 * tile:], ext_near[...], preferred_element_type=F32)
    x = x.astype(BF16)
    piece = jnp.zeros((2 * piece_rows, width), F32)
    for d in range(comps):
        weights = jnp.concatenate(
            [bases[level, d, h * cut:(h + 1) * cut] for h in range(2) for level in range(levels)], axis=0
        )
        piece = piece + jnp.dot(weights, x[:, d * width:(d + 1) * width], preferred_element_type=F32)
    for h in range(2):
        piece_out[h] = piece[h * piece_rows:(h + 1) * piece_rows]
    push(piece_out.at[1 - core], piece_mate, pair_recv.at[0], mate)
    for by in (-2, 2):
        order_landed(by)
    orders[2] = order[...]
    landed(piece_mate, pair_recv.at[0])
    pair = piece_out[core] + piece_mate[...]
    piece_out[2] = pair
    pieces[c // 2] = pair

    def piece_copy(d):
        return pltpu.make_async_remote_copy(
            src_ref=piece_out.at[2], dst_ref=pieces.at[c // 2], send_sem=piece_send.at[d],
            recv_sem=piece_recv.at[c // 2], device_id=at_clu(2 * d), device_id_type=MESH,
        )

    def start_piece(d, carry):
        piece_copy(d).start()
        return carry

    lax.fori_loop(1, half, start_piece, 0)
    send_z(last, 2)
    send_ext(0, 0)
    for d in range(comps):
        send_z(0, d)

    first = c - core - 2
    for j in range(near_count):
        spot = near_col[0, j] - c + 2
        spot = jnp.where(spot < 0, spot + n, spot)
        spot = jnp.where(spot >= n, spot - n, spot)
        one_hot(orders[jnp.clip(spot, 0, 4)], first, slots, picks.at[j * tile:(j + 1) * tile])
    relay(last, 1, True)

    def await_piece(d, carry):
        source = lax.rem(c // 2 + d, half)
        landed(pieces.at[source], piece_recv.at[source])
        return carry

    lax.fori_loop(1, half, await_piece, 0)
    at = 0
    for level, count in blocks:
        members = half // count
        own = (c // 2) // members
        for step in range(count - 1):
            k = lax.rem(own + 1 + step, count)
            entry = lax.fori_loop(
                0, members,
                lambda m, acc, k=k, members=members, level=level: acc
                + pieces[k * members + m, level * cut:(level + 1) * cut, :],
                jnp.zeros((cut, width), F32),
            )
            table_out[at:at + cut, :] = entry
            at += cut
    tables[0, core] = table_out[...]
    for i in range(1, groups):
        push(table_out, tables.at[i, core], table_recv.at[i, core], at_grp(i))
    push(table_out, tables.at[0, core], table_recv.at[0, core], mate)

    relay(last, 2, True)
    small[7].wait()
    small[8].wait()

    def gathered(i):
        x = jnp.dot(picks[:, :slots * tile], raw[i].reshape(slots * tile, lanes), preferred_element_type=F32)
        x = x + jnp.dot(picks[:, slots * tile:], ext[i], preferred_element_type=F32)
        return x.astype(BF16)

    def near(i):
        x = gathered(i)
        acc = jnp.zeros((rows, width), F32)
        for j in range(near_count):
            mine = jnp.concatenate(
                [x[j * tile:(j + 1) * tile, d * width:(d + 1) * width] for d in range(comps)], axis=0
            )
            acc = acc + jnp.dot(tiles[j], mine, preferred_element_type=F32)
        return acc

    landed(ext_in(last), ext_recv.at[last])
    for to, at in ((1, 2), (2, 1)):
        push(ext_in(last), ext_in(at), ext_recv.at[at], at_grp(to))
    for i in (1, 2, last):
        own_arrived(i) if i != last else None
        landed(whole(i, 3 - core), mate_recv.at[i])

    for i in (1, 2):
        relay(i, 0)
    for i in range(1, groups):
        landed(tables.at[i, core], table_recv.at[i, core])
        push(tables.at[i, core], tables.at[i, core], table_recv.at[i, core], mate)
    for d in range(comps):
        take(last, d)
    total[last] = near(last)
    for i in (1, 2):
        relay(i, 1)

    for i in range(groups):
        landed(tables.at[i, 1 - core], table_recv.at[i, 1 - core])
    table = jnp.concatenate([tables[i].reshape(2 * table_rows, width) for i in range(groups)], axis=1)
    high = table.astype(BF16)
    low = (table - high.astype(F32)).astype(BF16)
    mixed = jnp.dot(spread[...], high, preferred_element_type=F32)
    mixed = mixed + jnp.dot(spread[...], low, preferred_element_type=F32)
    for b in range(far_count):
        coupled[b * rank:(b + 1) * rank, :] = (mixed[b * rank:(b + 1) * rank, :] * scale[0, b]).astype(BF16)
    far = lax.dot_general(basis[...], coupled[...], (((0,), (0,)), ((), ())), preferred_element_type=F32)

    def send_y(i, value):
        y_out[i] = value.astype(BF16)
        push(y_out.at[i], y_in.at[i], y_recv.at[i], at_grp(i))

    send_y(last, total[last] + far[:, last * width:])
    for i in range(last):
        total[i] = far[:, i * width:(i + 1) * width]
    for i in (1, 2):
        relay(i, 2)
    for i in (1, 2):
        for d in range(comps):
            take(i, d)
        landed(ext_in(i), ext_recv.at[i])
        send_y(i, total[i] + near(i))
    for d in range(comps):
        relay(0, d)
    landed(ext_in(0), ext_recv.at[0])
    for d in range(comps):
        take(0, d)
    answer = total[0] + near(0)
    for i in range(1, groups):
        landed(y_in.at[i], y_recv.at[i])
        answer = answer + y_in[i].astype(F32)
    out[...] = answer.reshape(comps, tile, width)

    for copy in sends:
        copy.wait_send()

    def end_piece(d, carry):
        piece_copy(d).wait_send()
        return carry

    lax.fori_loop(1, half, end_piece, 0)


def solution(mesh):
    n, groups = mesh.shape["clu"], mesh.shape["grp"]

    def on_device(forces, order, bases, near_tiles, near_col, far_basis, far_coupling, far_scale, far_rank, far_target):
        comps, tile, columns = forces.shape
        levels, rank = bases.shape[:2]
        near_count, far_count = near_tiles.shape[1], far_basis.shape[1]
        width, rows, quarter = columns // groups, comps * tile, tile // 4
        lanes = comps * width
        cut = rank // 2
        piece_rows = levels * cut
        table_rows = sum(2 ** (level + 1) - 1 for level in range(levels)) * cut
        slots = 6
        pad = 128
        vmem, hbm = (pl.BlockSpec(memory_space=m) for m in (pltpu.VMEM, pl.ANY))
        dma = pltpu.SemaphoreType.DMA
        operands = (
            forces,
            order.reshape(1, tile),
            jnp.transpose(bases, (0, 2, 1, 3)),
            near_tiles.reshape(near_count, rows, rows),
            near_col,
            far_basis.reshape(far_count * rank, rows),
            far_coupling.reshape(far_count * rank, rank),
            far_scale,
            far_rank,
            far_target,
        )
        return pl.pallas_call(
            functools.partial(kernel, n, groups, levels, rank),
            out_shape=jax.ShapeDtypeStruct((comps, tile, width), F32),
            in_specs=[hbm] * len(operands),
            out_specs=vmem,
            scratch_shapes=[
                pltpu.VMEM((1, tile), jnp.int32),
                pltpu.VMEM((levels, comps, rank, tile), BF16),
                pltpu.VMEM((far_count * rank, rank), BF16),
                pltpu.SMEM((1, near_count), jnp.int32),
                pltpu.SMEM((1, far_count), F32),
                pltpu.SMEM((1, far_count), jnp.int32),
                pltpu.SMEM((1, far_count), jnp.int32),
                pltpu.VMEM((groups, slots, tile, lanes), BF16),
                pltpu.VMEM((groups, pad, lanes), BF16),
                pltpu.VMEM((2, quarter, lanes), BF16),
                pltpu.VMEM((pad, lanes), BF16),
                pltpu.VMEM((5, 1, tile), jnp.int32),
                pltpu.VMEM((near_count, rows, rows), BF16),
                pltpu.VMEM((far_count * rank, rows), BF16),
                pltpu.VMEM((far_count * rank, 2 * table_rows), BF16),
                pltpu.VMEM((near_count * tile, slots * tile + pad), BF16),
                pltpu.VMEM((tile, 2 * tile + pad), BF16),
                pltpu.VMEM((3, piece_rows, width), F32),
                pltpu.VMEM((piece_rows, width), F32),
                pltpu.VMEM((n // 2, piece_rows, width), F32),
                pltpu.VMEM((table_rows, width), F32),
                pltpu.VMEM((groups, 2, table_rows, width), F32),
                pltpu.VMEM((far_count * rank, columns), BF16),
                pltpu.VMEM((groups, rows, width), F32),
                pltpu.VMEM((groups, rows, width), BF16),
                pltpu.VMEM((groups, rows, width), BF16),
                dma((9,)), dma((groups,)), dma((SENDS,)), dma((n // 2,)),
                dma((5,)), dma((groups,)), dma((groups, slots, comps)), dma((groups,)), dma((1,)),
                dma((1,)), dma((n // 2,)), dma((groups, 2)), dma((groups,)),
            ],
            compiler_params=pltpu.CompilerParams(
                collective_id=0, has_side_effects=True, vmem_limit_bytes=28 * 1024 * 1024
            ),
        )(*(pltpu.with_memory_space_constraint(operand, pltpu.HBM) for operand in operands))

    placed = (
        P(None, "clu", None),
        P("clu"),
        P(None, None, None, "clu"),
        P("clu", "grp", None, None),
        P("clu", "grp"),
        P("clu", "grp", None, None),
        P("clu", "grp", None, None),
        P("clu", "grp"),
        P("clu", "grp"),
        P("clu", "grp"),
    )
    return jax.shard_map(
        on_device, mesh=mesh, in_specs=placed, out_specs=P(None, "clu", "grp"), check_vma=False
    )
```

```python
import functools

import jax
import jax.numpy as jnp
from jax import lax
from jax.experimental import pallas as pl
from jax.experimental.pallas import tpu as pltpu
from jax.sharding import PartitionSpec as P

MESH = pl.DeviceIdType.MESH
F32, BF16 = jnp.float32, jnp.bfloat16
SENDS = 48


def kernel(
    n, groups, levels, rank, comps,
    forces, order_hbm, bases_hbm, tiles_hbm, near_col_hbm, basis_hbm, coupling_hbm, scale_hbm, ranks_hbm, targets_hbm,
    out,
    order, bases, coupling, near_col, scale, ranks, targets, tiles, basis,
    ext_out, ext_near, orders, spread, picks, own_pick, piece_out, piece_mate, pieces,
    table, w_out, w_in, w_own, w_all, y_out, y_in, totals, pair_total,
    local_sem, own_sem, send_sem, piece_send, order_recv, mate_recv, z_recv, across_recv, ext_recv, near_recv,
    pair_recv, piece_recv, table_recv, w_recv, y_recv,
    *blocks,
):
    g, c = lax.axis_index("grp"), lax.axis_index("clu")
    core = lax.rem(c, 2)
    tile, columns = forces.shape[1:]
    width = columns // groups
    quarter = tile // 4
    rows = comps * tile
    near_count = tiles.shape[0]
    far_count = targets.shape[1]
    half = n // 2
    cut = rank // 2
    piece_rows = levels * cut
    spans = [(level, 2 ** (level + 1)) for level in range(levels)]
    table_rows = sum(count - 1 for _, count in spans) * cut
    last = groups - 1
    own_blocks, far_blocks, side_blocks = (blocks[at * comps:(at + 1) * comps] for at in range(3))
    edge = 7 * core

    def at_clu(by):
        return {"grp": g, "clu": lax.rem(c + by + n, n)}

    partners = (g, g + 1 - 2 * lax.rem(g, 2), lax.rem(g + 2, groups), groups - 1 - g)

    def at_grp(i):
        return {"grp": partners[i], "clu": c}

    mate = {"grp": g, "clu": c + 1 - 2 * core}
    sends = []

    def remote(src, dst, recv, where, index=0):
        return pltpu.make_async_remote_copy(
            src_ref=src, dst_ref=dst, send_sem=send_sem.at[index], recv_sem=recv, device_id=where, device_id_type=MESH
        )

    def push(copies, bytes_of):
        assert len(sends) < SENDS
        for src, dst, recv, where in copies:
            remote(src, dst, recv, where, len(sends)).start()
        sends.append(remote(bytes_of, bytes_of, near_recv.at[0], mate, len(sends)))

    def landed(ref, recv):
        remote(ref, ref, recv, mate).wait_recv()

    def several(count):
        return own_blocks[0].at[0:count]

    def columns_of(i, d):
        return forces.at[d, :, pl.ds(pl.multiple_of(partners[i] * width, width), width)]

    def part(i, p, d):
        if i == 0:
            return own_blocks[d].at[p]
        if i == last:
            return far_blocks[d].at[p]
        return side_blocks[d].at[p, :, pl.ds((i - 1) * width, width)]

    def edge_rows(i, p, d):
        if i == 0:
            return own_blocks[d].at[p, 0:quarter]
        if i == last:
            return far_blocks[d].at[p, 0:quarter]
        return side_blocks[d].at[p, 0:quarter, pl.ds((i - 1) * width, width)]

    small = [
        pltpu.make_async_copy(src, dst, local_sem.at[at])
        for at, (src, dst) in enumerate((
            (order_hbm, order), (coupling_hbm, coupling), (targets_hbm, targets), (ranks_hbm, ranks),
            (scale_hbm, scale), (basis_hbm, basis), (bases_hbm, bases), (near_col_hbm, near_col), (tiles_hbm, tiles),
        ))
    ]
    for copy in small[:6]:
        copy.start()
    for i in (last, 0, 1, 2):
        for d in range(comps):
            pltpu.make_async_copy(columns_of(i, d), part(i, 3 + core, d), own_sem.at[i]).start()
    for copy in small[6:]:
        copy.start()

    barrier = pltpu.get_barrier_semaphore()

    def greet(d, carry):
        pl.semaphore_signal(barrier, inc=1, device_id=at_clu(d), device_id_type=MESH)
        return carry

    lax.fori_loop(1, n, greet, 0)
    for d in range(1, groups):
        pl.semaphore_signal(barrier, inc=1, device_id=at_grp(d), device_id_type=MESH)

    for block in blocks:
        block[edge, quarter:, :] = jnp.zeros((tile - quarter, block.shape[2]), BF16)
    ext_near[:, quarter:, :] = jnp.zeros((comps, ext_near.shape[1] - quarter, width), BF16)

    for copy in small[1:5]:
        copy.wait()
    lane = lax.broadcasted_iota(jnp.int32, (rank, 2 * table_rows), 1)
    row = lax.broadcasted_iota(jnp.int32, (rank, 2 * table_rows), 0)
    lane_row = (lane // table_rows) * cut + lax.rem(lane, cut)
    lane_slot = lax.rem(lane, table_rows) // cut
    repeat = (lane_row == row).astype(F32).astype(BF16)
    wide = jnp.dot(coupling[...], repeat, preferred_element_type=F32)
    for b in range(far_count):
        target = targets[0, b]
        slot_of, base, offset = target, 0, 0
        for level, count in spans:
            own = (c // 2) // (half // count)
            here = target - base - own - 1
            here = jnp.where(here < 0, here + count, here) + offset
            slot_of = jnp.where((target >= base) & (target < base + count), here, slot_of)
            base, offset = base + count, offset + count - 1
        keep = (lane_slot == slot_of) & (lane_row < ranks[0, b])
        scaled = jnp.where(keep, wide[b * rank:(b + 1) * rank, :] * scale[0, b], 0.0)
        high = scaled.astype(BF16)
        spread[b * rank:(b + 1) * rank, :2 * table_rows] = high
        spread[b * rank:(b + 1) * rank, 2 * table_rows:] = (scaled - high.astype(F32)).astype(BF16)
    small[5].wait()
    folded = lax.dot_general(basis[...], spread[...], (((0,), (0,)), ((), ())), preferred_element_type=F32)
    folded = folded[:, :2 * table_rows] + folded[:, 2 * table_rows:]
    w_out[...] = folded.reshape(groups, rows // groups, 2 * table_rows)

    sub = lax.broadcasted_iota(jnp.int32, (tile, tile), 0)
    lan = lax.broadcasted_iota(jnp.int32, (tile, tile), 1)
    upto = (sub <= lan).astype(BF16)

    def ranked(chosen):
        spots = jnp.broadcast_to(chosen.astype(F32), (8, tile)).astype(BF16)
        return (jnp.dot(spots, upto, preferred_element_type=F32)[0:1, :] - 1.0).astype(jnp.int32)

    def wrapped(spot):
        spot = jnp.where(spot < 0, spot + n * tile, spot)
        return jnp.where(spot >= n * tile, spot - n * tile, spot)

    def one_hot(spot, store, count):
        down = jnp.broadcast_to(spot.astype(F32), (128, tile)).T
        at = lax.broadcasted_iota(jnp.int32, (tile, 128), 1).astype(F32)
        for j in range(count):
            store(j, (down == at + float(j * 128)).astype(F32).astype(BF16))

    small[0].wait()
    spot = wrapped(order[...] - (c - core) * tile)
    beyond = spot >= 2 * tile
    spot = jnp.where(beyond, 2 * tile + ranked(beyond), spot)

    def store_own(j, value):
        own_pick[:, j * 128:(j + 1) * 128] = value

    one_hot(spot, store_own, own_pick.shape[1] // 128)

    def own_arrived(i):
        pltpu.make_async_copy(several(comps), several(comps), own_sem.at[i]).wait()

    own_arrived(last)
    pl.semaphore_wait(barrier, n - 1 + groups - 1)

    for by in (-1, 1, -2, 2):
        push([(order, orders.at[2 - by], order_recv.at[2 - by], at_clu(by))], order)

    def z_copies(i, d):
        return [
            (part(i, 3 + core, d), part(i, 1 + core, d), z_recv.at[i, d, 0], at_clu(2)),
            (part(i, 3 + core, d), part(i, 5 + core, d), z_recv.at[i, d, 1], at_clu(-2)),
        ]

    push(z_copies(last, 0), several(2))
    push(
        [(w_out.at[partners[i]], w_in.at[i], w_recv.at[0, i], at_grp(i)) for i in range(1, groups)],
        w_out.at[0:groups - 1],
    )

    def send_mate(i):
        push([(part(i, 3 + core, d), part(i, 3 + core, d), mate_recv.at[i], mate) for d in range(comps)], several(comps))

    send_mate(last)
    own_arrived(0)
    send_mate(0)

    def order_landed(by):
        landed(orders.at[2 + by], order_recv.at[2 + by])

    for by in (-1, 1):
        order_landed(by)
    away = orders[1 + 2 * core] - c * tile
    chosen = (away >= 0) & (away < tile)
    place = jnp.where(chosen, ranked(chosen), -1)
    left = (lax.broadcasted_iota(jnp.int32, (128, tile), 0) == place).astype(F32).astype(BF16)
    right = (sub == away).astype(F32).astype(BF16)
    pick = lax.dot_general(left, right, (((1,), (1,)), ((), ())), preferred_element_type=F32).astype(BF16)

    def pick_edge(at, own):
        for d in range(comps):
            ext_out[at, d] = jnp.dot(pick, own[d][3 + core], preferred_element_type=F32).astype(BF16)[:quarter]

    pick_edge(1, far_blocks)
    push(
        [
            (ext_out.at[1, d], edge_rows(last, 7 - edge, d), ext_recv.at[last], at_clu(6 * core - 3))
            for d in range(comps)
        ],
        ext_out.at[1],
    )
    for d in range(1, comps):
        push(z_copies(last, d), several(2))
    pick_edge(0, own_blocks)
    push([(ext_out.at[0], ext_near.at[:, 0:quarter], near_recv.at[0], at_clu(2 * core - 1))], ext_out.at[0])
    push(z_copies(0, 0), several(2))
    for i in (1, 2):
        own_arrived(i)
        send_mate(i)

    for by in (-2, 2):
        order_landed(by)
    orders[2] = order[...]
    small[7].wait()
    starts = []
    for j in range(near_count):
        spot0 = near_col[0, j] - c + 2
        spot0 = jnp.where(spot0 < 0, spot0 + n, spot0)
        spot0 = jnp.clip(jnp.where(spot0 >= n, spot0 - n, spot0), 0, 4)
        starts.append(spot0 + core)
        spot = wrapped(orders[spot0] - (c + spot0 - 3) * tile)
        low = 2 * core * tile
        beyond = (spot >= low) & (spot < low + tile) & (spot0 == 4 * core)
        spot = jnp.where(beyond, low + ranked(beyond), spot)

        def store_pick(at, value, j=j):
            picks[j, :, at * 128:(at + 1) * 128] = value

        one_hot(spot, store_pick, picks.shape[2] // 128)

    def relay(i, d):
        copies = []
        for side, p in enumerate((1 + core, 5 + core)):
            landed(part(i, p, d), z_recv.at[i, d, side])
            copies.append((part(i, p, d), part(i, p, d), across_recv.at[i, d], mate))
            if i == last:
                for to, at in ((1, 2), (2, 1)):
                    copies.append((part(i, p, d), part(at, p, d), z_recv.at[at, d, side], at_grp(to)))
        push(copies, several(len(copies)))

    def take(i, d):
        landed(several(2), across_recv.at[i, d])

    relay(last, 0)

    for i in range(1, groups):
        landed(w_in.at[i], w_recv.at[0, i])
    summed = w_out[g]
    for i in range(1, groups):
        summed = summed + w_in[i]
    w_own[...] = summed.astype(BF16)
    w_all[g] = summed.astype(BF16)
    push([(w_own, w_all.at[g], w_recv.at[1, i], at_grp(i)) for i in range(1, groups)], w_all.at[0:groups - 1])

    small[6].wait()
    landed(ext_out.at[0], near_recv.at[0])
    push(
        [
            (ext_near.at[d, 0:quarter], edge_rows(0, edge, d), ext_recv.at[0], at_clu(2 - 4 * core))
            for d in range(comps)
        ],
        ext_out.at[0],
    )
    landed(several(comps), mate_recv.at[0])
    piece = jnp.zeros((2 * piece_rows, width), F32)
    for d in range(comps):
        x = jnp.dot(own_pick[:, :2 * tile], own_blocks[d][3:5].reshape(2 * tile, width), preferred_element_type=F32)
        x = x + jnp.dot(own_pick[:, 2 * tile:], ext_near[d], preferred_element_type=F32)
        weights = jnp.concatenate(
            [bases[level, d, h * cut:(h + 1) * cut] for h in range(2) for level in range(levels)], axis=0
        )
        piece = piece + jnp.dot(weights, x.astype(BF16), preferred_element_type=F32)
    for h in range(2):
        piece_out[h] = piece[h * piece_rows:(h + 1) * piece_rows]
    push([(piece_out.at[1 - core], piece_mate, pair_recv.at[0], mate)], piece_mate)
    relay(last, 1)
    landed(piece_mate, pair_recv.at[0])
    pair = piece_out[core] + piece_mate[...]
    piece_out[2] = pair
    pieces[c // 2] = pair

    def piece_copy(d):
        return pltpu.make_async_remote_copy(
            src_ref=piece_out.at[2], dst_ref=pieces.at[c // 2], send_sem=piece_send.at[d],
            recv_sem=piece_recv.at[c // 2], device_id=at_clu(2 * d), device_id_type=MESH,
        )

    def start_piece(d, carry):
        piece_copy(d).start()
        return carry

    lax.fori_loop(1, half, start_piece, 0)
    for d in range(1, comps):
        push(z_copies(0, d), several(2))

    landed(ext_out.at[1], ext_recv.at[last])
    push(
        [
            (edge_rows(last, edge, d), edge_rows(at, edge, d), ext_recv.at[at], at_grp(to))
            for to, at in ((1, 2), (2, 1)) for d in range(comps)
        ],
        ext_out,
    )
    landed(several(comps), mate_recv.at[last])
    small[8].wait()

    def near(block, d):
        acc = None
        for j in range(near_count):
            held = block[d][pl.ds(starts[j], 3)].reshape(3 * tile, block[d].shape[2])
            x = jnp.dot(picks[j], held, preferred_element_type=F32).astype(BF16)
            term = jnp.dot(tiles[j, :, d * tile:(d + 1) * tile], x, preferred_element_type=F32)
            acc = term if acc is None else acc + term
        return acc

    take(last, 0)
    totals[...] = near(far_blocks, 0)
    relay(last, 2)
    for i in (1, 2):
        relay(i, 0)
    take(last, 1)
    totals[...] += near(far_blocks, 1)
    for i in (1, 2):
        relay(i, 1)

    def await_piece(d, carry):
        source = lax.rem(c // 2 + d, half)
        landed(pieces.at[source], piece_recv.at[source])
        return carry

    lax.fori_loop(1, half, await_piece, 0)
    at = 0
    for level, count in spans:
        members = half // count
        own = (c // 2) // members
        for step in range(count - 1):
            k = lax.rem(own + 1 + step, count)
            entry = lax.fori_loop(
                0, members,
                lambda m, acc, k=k, members=members, level=level: acc
                + pieces[k * members + m, level * cut:(level + 1) * cut, :],
                jnp.zeros((cut, width), F32),
            )
            table[core, at:at + cut, :] = entry
            at += cut
    push([(table.at[core], table.at[core], table_recv.at[0], mate)], table.at[0])

    def send_y(i, value):
        y_out[i] = value.astype(BF16)
        push([(y_out.at[i], y_in.at[i], y_recv.at[i], at_grp(i))], y_out.at[i])

    take(last, 2)
    send_y(last, totals[...] + near(far_blocks, 2))

    for i in (1, 2):
        landed(several(comps), mate_recv.at[i])
        landed(ext_out.at[0], ext_recv.at[i])
        take(i, 0)
    pair_total[...] = near(side_blocks, 0)
    for i in (1, 2):
        relay(i, 2)
    relay(0, 0)
    for i in (1, 2):
        take(i, 1)
    pair_total[...] += near(side_blocks, 1)
    for i in (1, 2):
        take(i, 2)
    both = pair_total[...] + near(side_blocks, 2)
    for i in (1, 2):
        send_y(i, both[:, (i - 1) * width:i * width])

    for i in range(1, groups):
        landed(w_own, w_recv.at[1, i])
    landed(table.at[0], table_recv.at[0])
    entries = table[...].reshape(2 * table_rows, width)
    high = entries.astype(BF16)
    low = (entries - high.astype(F32)).astype(BF16)
    weights = w_all[...].reshape(rows, 2 * table_rows)
    answer = jnp.dot(weights, high, preferred_element_type=F32) + jnp.dot(weights, low, preferred_element_type=F32)
    landed(ext_out.at[0], ext_recv.at[0])
    relay(0, 1)
    take(0, 0)
    totals[...] = answer + near(own_blocks, 0)
    relay(0, 2)
    take(0, 1)
    totals[...] += near(own_blocks, 1)
    for i in range(1, groups):
        landed(y_in.at[i], y_recv.at[i])
        totals[...] += y_in[i].astype(F32)
    for copy in sends:
        copy.wait_send()

    def end_piece(d, carry):
        piece_copy(d).wait_send()
        return carry

    lax.fori_loop(1, half, end_piece, 0)
    take(0, 2)
    out[...] = (totals[...] + near(own_blocks, 2)).reshape(comps, tile, width)


def solution(mesh):
    n, groups = mesh.shape["clu"], mesh.shape["grp"]

    def on_device(forces, order, bases, near_tiles, near_col, far_basis, far_coupling, far_scale, far_rank, far_target):
        comps, tile, columns = forces.shape
        levels, rank = bases.shape[:2]
        near_count, far_count = near_tiles.shape[1], far_basis.shape[1]
        width, rows, quarter = columns // groups, comps * tile, tile // 4
        cut = rank // 2
        piece_rows = levels * cut
        table_rows = sum(2 ** (level + 1) - 1 for level in range(levels)) * cut
        slots = 8
        pad = 128
        vmem, hbm = (pl.BlockSpec(memory_space=m) for m in (pltpu.VMEM, pl.ANY))
        dma = pltpu.SemaphoreType.DMA
        operands = (
            forces,
            order.reshape(1, tile),
            jnp.transpose(bases, (0, 2, 1, 3)),
            near_tiles.reshape(near_count, rows, rows),
            near_col,
            far_basis.reshape(far_count * rank, rows),
            far_coupling.reshape(far_count * rank, rank),
            far_scale,
            far_rank,
            far_target,
        )
        return pl.pallas_call(
            functools.partial(kernel, n, groups, levels, rank, comps),
            out_shape=jax.ShapeDtypeStruct((comps, tile, width), F32),
            in_specs=[hbm] * len(operands),
            out_specs=vmem,
            scratch_shapes=[
                pltpu.VMEM((1, tile), jnp.int32),
                pltpu.VMEM((levels, comps, rank, tile), BF16),
                pltpu.VMEM((far_count * rank, rank), BF16),
                pltpu.SMEM((1, near_count), jnp.int32),
                pltpu.SMEM((1, far_count), F32),
                pltpu.SMEM((1, far_count), jnp.int32),
                pltpu.SMEM((1, far_count), jnp.int32),
                pltpu.VMEM((near_count, rows, rows), BF16),
                pltpu.VMEM((far_count * rank, rows), BF16),
                pltpu.VMEM((2, comps, quarter, width), BF16),
                pltpu.VMEM((comps, pad, width), BF16),
                pltpu.VMEM((5, 1, tile), jnp.int32),
                pltpu.VMEM((far_count * rank, 4 * table_rows), BF16),
                pltpu.VMEM((near_count, tile, 3 * tile), BF16),
                pltpu.VMEM((tile, 2 * tile + pad), BF16),
                pltpu.VMEM((3, piece_rows, width), F32),
                pltpu.VMEM((piece_rows, width), F32),
                pltpu.VMEM((n // 2, piece_rows, width), F32),
                pltpu.VMEM((2, table_rows, width), F32),
                pltpu.VMEM((groups, rows // groups, 2 * table_rows), F32),
                pltpu.VMEM((groups, rows // groups, 2 * table_rows), F32),
                pltpu.VMEM((rows // groups, 2 * table_rows), BF16),
                pltpu.VMEM((groups, rows // groups, 2 * table_rows), BF16),
                pltpu.VMEM((groups, rows, width), BF16),
                pltpu.VMEM((groups, rows, width), BF16),
                pltpu.VMEM((rows, width), F32),
                pltpu.VMEM((rows, 2 * width), F32),
                dma((9,)), dma((groups,)), dma((SENDS,)), dma((n // 2,)),
                dma((5,)), dma((groups,)), dma((groups, comps, 2)), dma((groups, comps)), dma((groups,)), dma((1,)),
                dma((1,)), dma((n // 2,)), dma((1,)), dma((2, groups)), dma((groups,)),
                *(pltpu.VMEM((slots, tile, size), BF16) for size in (width, width, 2 * width) for _ in range(comps)),
            ],
            compiler_params=pltpu.CompilerParams(
                collective_id=0, has_side_effects=True, vmem_limit_bytes=28 * 1024 * 1024
            ),
        )(*(pltpu.with_memory_space_constraint(operand, pltpu.HBM) for operand in operands))

    placed = (
        P(None, "clu", None),
        P("clu"),
        P(None, None, None, "clu"),
        P("clu", "grp", None, None),
        P("clu", "grp"),
        P("clu", "grp", None, None),
        P("clu", "grp", None, None),
        P("clu", "grp"),
        P("clu", "grp"),
        P("clu", "grp"),
    )
    return jax.shard_map(
        on_device, mesh=mesh, in_specs=placed, out_specs=P(None, "clu", "grp"), check_vma=False
    )
```

```python
import functools

import jax
import jax.numpy as jnp
from jax import lax
from jax.experimental import pallas as pl
from jax.experimental.pallas import tpu as pltpu
from jax.sharding import PartitionSpec as P

MESH = pl.DeviceIdType.MESH
F32, BF16 = jnp.float32, jnp.bfloat16
SENDS = 48


def kernel(
    n, groups, levels, rank, comps,
    forces, order_hbm, bases_hbm, tiles_hbm, near_col_hbm, basis_hbm, coupling_hbm, scale_hbm, ranks_hbm, targets_hbm,
    out,
    order, bases, coupling, near_col, scale, ranks, targets, tiles, basis,
    ext_out, ext_near, orders, spread, picks, own_pick, piece_out, piece_mate, pieces,
    table, w_out, w_in, w_own, w_all, y_out, y_in, y_mid, totals, pair_total,
    local_sem, own_sem, send_sem, piece_send, order_recv, mate_recv, z_recv, across_recv, ext_recv, near_recv,
    pair_recv, piece_recv, table_recv, w_recv, y_recv, mid_recv,
    *blocks,
):
    g, c = lax.axis_index("grp"), lax.axis_index("clu")
    core = lax.rem(c, 2)
    tile, columns = forces.shape[1:]
    width = columns // groups
    quarter = tile // 4
    rows = comps * tile
    near_count = tiles.shape[0]
    far_count = targets.shape[1]
    half = n // 2
    cut = rank // 2
    piece_rows = levels * cut
    spans = [(level, 2 ** (level + 1)) for level in range(levels)]
    table_rows = sum(count - 1 for _, count in spans) * cut
    last = groups - 1
    own_blocks, far_blocks, side_blocks = (blocks[at * comps:(at + 1) * comps] for at in range(3))
    edge = 7 * core

    def at_clu(by):
        return {"grp": g, "clu": lax.rem(c + by + n, n)}

    partners = (g, g + 1 - 2 * lax.rem(g, 2), lax.rem(g + 2, groups), groups - 1 - g)

    def at_grp(i):
        return {"grp": partners[i], "clu": c}

    mate = {"grp": g, "clu": c + 1 - 2 * core}
    sends = []

    def remote(src, dst, recv, where, index=0):
        return pltpu.make_async_remote_copy(
            src_ref=src, dst_ref=dst, send_sem=send_sem.at[index], recv_sem=recv, device_id=where, device_id_type=MESH
        )

    def push(copies, bytes_of):
        assert len(sends) < SENDS
        for src, dst, recv, where in copies:
            remote(src, dst, recv, where, len(sends)).start()
        sends.append(remote(bytes_of, bytes_of, near_recv.at[0], mate, len(sends)))

    def landed(ref, recv):
        remote(ref, ref, recv, mate).wait_recv()

    def several(count):
        return own_blocks[0].at[0:count]

    def columns_of(i, d):
        return forces.at[d, :, pl.ds(pl.multiple_of(partners[i] * width, width), width)]

    def part(i, p, d):
        if i == 0:
            return own_blocks[d].at[p]
        if i == last:
            return far_blocks[d].at[p]
        return side_blocks[d].at[p, :, pl.ds((i - 1) * width, width)]

    def edge_rows(i, p, d):
        if i == 0:
            return own_blocks[d].at[p, 0:quarter]
        if i == last:
            return far_blocks[d].at[p, 0:quarter]
        return side_blocks[d].at[p, 0:quarter, pl.ds((i - 1) * width, width)]

    small = [
        pltpu.make_async_copy(src, dst, local_sem.at[at])
        for at, (src, dst) in enumerate((
            (order_hbm, order), (coupling_hbm, coupling), (targets_hbm, targets), (ranks_hbm, ranks),
            (scale_hbm, scale), (basis_hbm, basis), (bases_hbm, bases), (near_col_hbm, near_col), (tiles_hbm, tiles),
        ))
    ]
    for copy in small[:6]:
        copy.start()
    for i in (last, 0, 1, 2):
        for d in range(comps):
            pltpu.make_async_copy(columns_of(i, d), part(i, 3 + core, d), own_sem.at[i]).start()
    for copy in small[6:]:
        copy.start()

    barrier = pltpu.get_barrier_semaphore()

    def greet(d, carry):
        pl.semaphore_signal(barrier, inc=1, device_id=at_clu(d), device_id_type=MESH)
        return carry

    lax.fori_loop(1, n, greet, 0)
    for d in range(1, groups):
        pl.semaphore_signal(barrier, inc=1, device_id=at_grp(d), device_id_type=MESH)

    for block in blocks:
        block[edge, quarter:, :] = jnp.zeros((tile - quarter, block.shape[2]), BF16)
    ext_near[:, quarter:, :] = jnp.zeros((comps, ext_near.shape[1] - quarter, width), BF16)

    for copy in small[1:5]:
        copy.wait()
    lane = lax.broadcasted_iota(jnp.int32, (rank, 2 * table_rows), 1)
    row = lax.broadcasted_iota(jnp.int32, (rank, 2 * table_rows), 0)
    lane_row = (lane // table_rows) * cut + lax.rem(lane, cut)
    lane_slot = lax.rem(lane, table_rows) // cut
    repeat = (lane_row == row).astype(F32).astype(BF16)
    wide = jnp.dot(coupling[...], repeat, preferred_element_type=F32)
    for b in range(far_count):
        target = targets[0, b]
        slot_of, base, offset = target, 0, 0
        for level, count in spans:
            own = (c // 2) // (half // count)
            here = target - base - own - 1
            here = jnp.where(here < 0, here + count, here) + offset
            slot_of = jnp.where((target >= base) & (target < base + count), here, slot_of)
            base, offset = base + count, offset + count - 1
        keep = (lane_slot == slot_of) & (lane_row < ranks[0, b])
        scaled = jnp.where(keep, wide[b * rank:(b + 1) * rank, :] * scale[0, b], 0.0)
        high = scaled.astype(BF16)
        spread[b * rank:(b + 1) * rank, :2 * table_rows] = high
        spread[b * rank:(b + 1) * rank, 2 * table_rows:] = (scaled - high.astype(F32)).astype(BF16)
    small[5].wait()
    folded = lax.dot_general(basis[...], spread[...], (((0,), (0,)), ((), ())), preferred_element_type=F32)
    folded = folded[:, :2 * table_rows] + folded[:, 2 * table_rows:]
    w_out[...] = folded.reshape(groups, rows // groups, 2 * table_rows)

    sub = lax.broadcasted_iota(jnp.int32, (tile, tile), 0)
    lan = lax.broadcasted_iota(jnp.int32, (tile, tile), 1)
    upto = (sub <= lan).astype(BF16)

    def ranked(chosen):
        spots = jnp.broadcast_to(chosen.astype(F32), (8, tile)).astype(BF16)
        return (jnp.dot(spots, upto, preferred_element_type=F32)[0:1, :] - 1.0).astype(jnp.int32)

    def wrapped(spot):
        spot = jnp.where(spot < 0, spot + n * tile, spot)
        return jnp.where(spot >= n * tile, spot - n * tile, spot)

    def one_hot(spot, store, count):
        down = jnp.broadcast_to(spot.astype(F32), (128, tile)).T
        at = lax.broadcasted_iota(jnp.int32, (tile, 128), 1).astype(F32)
        for j in range(count):
            store(j, (down == at + float(j * 128)).astype(F32).astype(BF16))

    small[0].wait()
    spot = wrapped(order[...] - (c - core) * tile)
    beyond = spot >= 2 * tile
    spot = jnp.where(beyond, 2 * tile + ranked(beyond), spot)

    def store_own(j, value):
        own_pick[:, j * 128:(j + 1) * 128] = value

    one_hot(spot, store_own, own_pick.shape[1] // 128)

    def own_arrived(i):
        pltpu.make_async_copy(several(comps), several(comps), own_sem.at[i]).wait()

    own_arrived(last)
    pl.semaphore_wait(barrier, n - 1 + groups - 1)

    for by in (-1, 1, -2, 2):
        push([(order, orders.at[2 - by], order_recv.at[2 - by], at_clu(by))], order)

    def z_copies(i, d):
        return [
            (part(i, 3 + core, d), part(i, 1 + core, d), z_recv.at[i, d, 0], at_clu(2)),
            (part(i, 3 + core, d), part(i, 5 + core, d), z_recv.at[i, d, 1], at_clu(-2)),
        ]

    for d in range(comps - 1):
        push(z_copies(last, d), several(2))
    push(
        [(w_out.at[partners[i]], w_in.at[i], w_recv.at[0, i], at_grp(i)) for i in range(1, groups)],
        w_out.at[0:groups - 1],
    )

    def send_mate(i):
        push([(part(i, 3 + core, d), part(i, 3 + core, d), mate_recv.at[i], mate) for d in range(comps)], several(comps))

    send_mate(last)
    own_arrived(0)
    send_mate(0)

    def order_landed(by):
        landed(orders.at[2 + by], order_recv.at[2 + by])

    for by in (-1, 1):
        order_landed(by)
    away = orders[1 + 2 * core] - c * tile
    chosen = (away >= 0) & (away < tile)
    place = jnp.where(chosen, ranked(chosen), -1)
    left = (lax.broadcasted_iota(jnp.int32, (128, tile), 0) == place).astype(F32).astype(BF16)
    right = (sub == away).astype(F32).astype(BF16)
    pick = lax.dot_general(left, right, (((1,), (1,)), ((), ())), preferred_element_type=F32).astype(BF16)

    def pick_edge(at, own):
        for d in range(comps):
            ext_out[at, d] = jnp.dot(pick, own[d][3 + core], preferred_element_type=F32).astype(BF16)[:quarter]

    pick_edge(1, far_blocks)
    push(
        [
            (ext_out.at[1, d], edge_rows(last, 7 - edge, d), ext_recv.at[last], at_clu(6 * core - 3))
            for d in range(comps)
        ],
        ext_out.at[1],
    )
    push(z_copies(last, comps - 1), several(2))
    pick_edge(0, own_blocks)
    push([(ext_out.at[0], ext_near.at[:, 0:quarter], near_recv.at[0], at_clu(2 * core - 1))], ext_out.at[0])
    for d in range(comps - 1):
        push(z_copies(0, d), several(2))
    for i in (1, 2):
        own_arrived(i)
        send_mate(i)

    for by in (-2, 2):
        order_landed(by)
    orders[2] = order[...]
    small[7].wait()
    starts = []
    for j in range(near_count):
        spot0 = near_col[0, j] - c + 2
        spot0 = jnp.where(spot0 < 0, spot0 + n, spot0)
        spot0 = jnp.clip(jnp.where(spot0 >= n, spot0 - n, spot0), 0, 4)
        starts.append(spot0 + core)
        spot = wrapped(orders[spot0] - (c + spot0 - 3) * tile)
        low = 2 * core * tile
        beyond = (spot >= low) & (spot < low + tile) & (spot0 == 4 * core)
        spot = jnp.where(beyond, low + ranked(beyond), spot)

        def store_pick(at, value, j=j):
            picks[j, :, at * 128:(at + 1) * 128] = value

        one_hot(spot, store_pick, picks.shape[2] // 128)

    def relay(i, d):
        copies = []
        for side, p in enumerate((1 + core, 5 + core)):
            landed(part(i, p, d), z_recv.at[i, d, side])
            copies.append((part(i, p, d), part(i, p, d), across_recv.at[i, d], mate))
            if i == last:
                for to, at in ((1, 2), (2, 1)):
                    copies.append((part(i, p, d), part(at, p, d), z_recv.at[at, d, side], at_grp(to)))
        push(copies, several(len(copies)))

    def take(i, d):
        landed(several(2), across_recv.at[i, d])

    def near(block, d):
        acc = None
        for j in range(near_count):
            held = block[d][pl.ds(starts[j], 3)].reshape(3 * tile, block[d].shape[2])
            x = jnp.dot(picks[j], held, preferred_element_type=F32).astype(BF16)
            term = jnp.dot(tiles[j, :, d * tile:(d + 1) * tile], x, preferred_element_type=F32)
            acc = term if acc is None else acc + term
        return acc

    mid = rows // 2

    relay(last, 0)
    relay(last, 1)
    landed(ext_out.at[1], ext_recv.at[last])
    push(
        [
            (edge_rows(last, edge, d), edge_rows(at, edge, d), ext_recv.at[at], at_grp(to))
            for to, at in ((1, 2), (2, 1)) for d in range(comps)
        ],
        ext_out,
    )
    landed(several(comps), mate_recv.at[last])
    small[8].wait()
    take(last, 0)
    totals[...] = near(far_blocks, 0)

    for i in range(1, groups):
        landed(w_in.at[i], w_recv.at[0, i])
    summed = w_out[g]
    for i in range(1, groups):
        summed = summed + w_in[i]
    w_own[...] = summed.astype(BF16)
    w_all[g] = summed.astype(BF16)

    relay(last, 2)
    push([(w_own, w_all.at[g], w_recv.at[1, i], at_grp(i)) for i in range(1, groups)], w_all.at[0:groups - 1])
    take(last, 1)
    totals[...] += near(far_blocks, 1)
    for i in (1, 2):
        relay(i, 0)
    take(last, 2)
    y_out[last] = (totals[...] + near(far_blocks, 2)).astype(BF16)
    push(
        [
            (y_out.at[last, 0:mid], y_mid.at[0], mid_recv.at[0], at_grp(1)),
            (y_out.at[last, mid:rows], y_mid.at[1], mid_recv.at[1], at_grp(2)),
        ],
        y_out.at[last],
    )

    small[6].wait()
    landed(ext_out.at[0], near_recv.at[0])
    landed(several(comps), mate_recv.at[0])
    piece = jnp.zeros((2 * piece_rows, width), F32)
    for d in range(comps):
        x = jnp.dot(own_pick[:, :2 * tile], own_blocks[d][3:5].reshape(2 * tile, width), preferred_element_type=F32)
        x = x + jnp.dot(own_pick[:, 2 * tile:], ext_near[d], preferred_element_type=F32)
        weights = jnp.concatenate(
            [bases[level, d, h * cut:(h + 1) * cut] for h in range(2) for level in range(levels)], axis=0
        )
        piece = piece + jnp.dot(weights, x.astype(BF16), preferred_element_type=F32)
    for h in range(2):
        piece_out[h] = piece[h * piece_rows:(h + 1) * piece_rows]
    push([(piece_out.at[1 - core], piece_mate, pair_recv.at[0], mate)], piece_mate)
    for i in (1, 2):
        relay(i, 1)

    landed(piece_mate, pair_recv.at[0])
    pair = piece_out[core] + piece_mate[...]
    piece_out[2] = pair
    pieces[c // 2] = pair

    def piece_copy(d):
        return pltpu.make_async_remote_copy(
            src_ref=piece_out.at[2], dst_ref=pieces.at[c // 2], send_sem=piece_send.at[d],
            recv_sem=piece_recv.at[c // 2], device_id=at_clu(2 * d), device_id_type=MESH,
        )

    def start_piece(d, carry):
        piece_copy(d).start()
        return carry

    lax.fori_loop(1, half, start_piece, 0)
    push(z_copies(0, comps - 1), several(2))
    push(
        [
            (ext_near.at[d, 0:quarter], edge_rows(0, edge, d), ext_recv.at[0], at_clu(2 - 4 * core))
            for d in range(comps)
        ],
        ext_out.at[0],
    )

    for i in (1, 2):
        landed(several(comps), mate_recv.at[i])
        landed(ext_out.at[0], ext_recv.at[i])
        take(i, 0)
    pair_total[...] = near(side_blocks, 0)
    for i in (1, 2):
        relay(i, 2)
    for i in (1, 2):
        take(i, 1)
    pair_total[...] += near(side_blocks, 1)
    relay(0, 0)
    for i in (1, 2):
        take(i, 2)
    both = pair_total[...] + near(side_blocks, 2)

    def send_y(i, h, value):
        here = pl.ds(h * mid, mid)
        y_out[i, h * mid:(h + 1) * mid] = value.astype(BF16)
        push([(y_out.at[i, here], y_in.at[i, here], y_recv.at[i, h], at_grp(i))], y_mid.at[0])

    def half_of(i, h):
        return both[h * mid:(h + 1) * mid, (i - 1) * width:i * width]

    send_y(1, 0, half_of(1, 0))
    send_y(2, 1, half_of(2, 1))
    landed(y_mid.at[1], mid_recv.at[1])
    send_y(1, 1, half_of(1, 1) + y_mid[1].astype(F32))
    landed(y_mid.at[0], mid_recv.at[0])
    send_y(2, 0, half_of(2, 0) + y_mid[0].astype(F32))
    relay(0, 1)

    def await_piece(d, carry):
        source = lax.rem(c // 2 + d, half)
        landed(pieces.at[source], piece_recv.at[source])
        return carry

    lax.fori_loop(1, half, await_piece, 0)
    at = 0
    for level, count in spans:
        members = half // count
        own = (c // 2) // members
        for step in range(count - 1):
            k = lax.rem(own + 1 + step, count)
            entry = lax.fori_loop(
                0, members,
                lambda m, acc, k=k, members=members, level=level: acc
                + pieces[k * members + m, level * cut:(level + 1) * cut, :],
                jnp.zeros((cut, width), F32),
            )
            table[core, at:at + cut, :] = entry
            at += cut
    push([(table.at[core], table.at[core], table_recv.at[0], mate)], table.at[0])

    landed(ext_out.at[0], ext_recv.at[0])
    take(0, 0)
    totals[...] = near(own_blocks, 0)
    relay(0, 2)
    for i in range(1, groups):
        landed(w_own, w_recv.at[1, i])
    landed(table.at[0], table_recv.at[0])
    entries = table[...].reshape(2 * table_rows, width)
    high = entries.astype(BF16)
    low = (entries - high.astype(F32)).astype(BF16)
    weights = w_all[...].reshape(rows, 2 * table_rows)
    answer = jnp.dot(weights, high, preferred_element_type=F32) + jnp.dot(weights, low, preferred_element_type=F32)
    take(0, 1)
    totals[...] += answer + near(own_blocks, 1)
    take(0, 2)
    totals[...] += near(own_blocks, 2)

    for copy in sends:
        copy.wait_send()

    def end_piece(d, carry):
        piece_copy(d).wait_send()
        return carry

    lax.fori_loop(1, half, end_piece, 0)
    for i in (1, 2):
        for h in range(2):
            landed(y_mid.at[0], y_recv.at[i, h])
    out[...] = (totals[...] + y_in[1].astype(F32) + y_in[2].astype(F32)).reshape(comps, tile, width)


def solution(mesh):
    n, groups = mesh.shape["clu"], mesh.shape["grp"]

    def on_device(forces, order, bases, near_tiles, near_col, far_basis, far_coupling, far_scale, far_rank, far_target):
        comps, tile, columns = forces.shape
        levels, rank = bases.shape[:2]
        near_count, far_count = near_tiles.shape[1], far_basis.shape[1]
        width, rows, quarter = columns // groups, comps * tile, tile // 4
        cut = rank // 2
        piece_rows = levels * cut
        table_rows = sum(2 ** (level + 1) - 1 for level in range(levels)) * cut
        slots = 8
        pad = 128
        vmem, hbm = (pl.BlockSpec(memory_space=m) for m in (pltpu.VMEM, pl.ANY))
        dma = pltpu.SemaphoreType.DMA
        operands = (
            forces,
            order.reshape(1, tile),
            jnp.transpose(bases, (0, 2, 1, 3)),
            near_tiles.reshape(near_count, rows, rows),
            near_col,
            far_basis.reshape(far_count * rank, rows),
            far_coupling.reshape(far_count * rank, rank),
            far_scale,
            far_rank,
            far_target,
        )
        return pl.pallas_call(
            functools.partial(kernel, n, groups, levels, rank, comps),
            out_shape=jax.ShapeDtypeStruct((comps, tile, width), F32),
            in_specs=[hbm] * len(operands),
            out_specs=vmem,
            scratch_shapes=[
                pltpu.VMEM((1, tile), jnp.int32),
                pltpu.VMEM((levels, comps, rank, tile), BF16),
                pltpu.VMEM((far_count * rank, rank), BF16),
                pltpu.SMEM((1, near_count), jnp.int32),
                pltpu.SMEM((1, far_count), F32),
                pltpu.SMEM((1, far_count), jnp.int32),
                pltpu.SMEM((1, far_count), jnp.int32),
                pltpu.VMEM((near_count, rows, rows), BF16),
                pltpu.VMEM((far_count * rank, rows), BF16),
                pltpu.VMEM((2, comps, quarter, width), BF16),
                pltpu.VMEM((comps, pad, width), BF16),
                pltpu.VMEM((5, 1, tile), jnp.int32),
                pltpu.VMEM((far_count * rank, 4 * table_rows), BF16),
                pltpu.VMEM((near_count, tile, 3 * tile), BF16),
                pltpu.VMEM((tile, 2 * tile + pad), BF16),
                pltpu.VMEM((3, piece_rows, width), F32),
                pltpu.VMEM((piece_rows, width), F32),
                pltpu.VMEM((n // 2, piece_rows, width), F32),
                pltpu.VMEM((2, table_rows, width), F32),
                pltpu.VMEM((groups, rows // groups, 2 * table_rows), F32),
                pltpu.VMEM((groups, rows // groups, 2 * table_rows), F32),
                pltpu.VMEM((rows // groups, 2 * table_rows), BF16),
                pltpu.VMEM((groups, rows // groups, 2 * table_rows), BF16),
                pltpu.VMEM((groups, rows, width), BF16),
                pltpu.VMEM((groups, rows, width), BF16),
                pltpu.VMEM((2, rows // 2, width), BF16),
                pltpu.VMEM((rows, width), F32),
                pltpu.VMEM((rows, 2 * width), F32),
                dma((9,)), dma((groups,)), dma((SENDS,)), dma((n // 2,)),
                dma((5,)), dma((groups,)), dma((groups, comps, 2)), dma((groups, comps)), dma((groups,)), dma((1,)),
                dma((1,)), dma((n // 2,)), dma((1,)), dma((2, groups)), dma((groups, 2)), dma((2,)),
                *(pltpu.VMEM((slots, tile, size), BF16) for size in (width, width, 2 * width) for _ in range(comps)),
            ],
            compiler_params=pltpu.CompilerParams(
                collective_id=0, has_side_effects=True, vmem_limit_bytes=28 * 1024 * 1024
            ),
        )(*(pltpu.with_memory_space_constraint(operand, pltpu.HBM) for operand in operands))

    placed = (
        P(None, "clu", None),
        P("clu"),
        P(None, None, None, "clu"),
        P("clu", "grp", None, None),
        P("clu", "grp"),
        P("clu", "grp", None, None),
        P("clu", "grp", None, None),
        P("clu", "grp"),
        P("clu", "grp"),
        P("clu", "grp"),
    )
    return jax.shard_map(
        on_device, mesh=mesh, in_specs=placed, out_specs=P(None, "clu", "grp"), check_vma=False
    )
```

```python
import functools

import jax
import jax.numpy as jnp
from jax import lax
from jax.experimental import pallas as pl
from jax.experimental.pallas import tpu as pltpu
from jax.sharding import PartitionSpec as P

MESH = pl.DeviceIdType.MESH
F32, BF16 = jnp.float32, jnp.bfloat16
SENDS = 48


def kernel(n, groups, levels, rank, comps, *refs):
    dma = pltpu.SemaphoreType.DMA

    def scoped(*sems):
        body(n, groups, levels, rank, comps, *sems, *refs)

    pl.run_scoped(
        scoped,
        dma((9,)), dma((groups,)), dma((SENDS,)), dma((n // 2,)),
        dma((5,)), dma((groups,)), dma((groups, comps + 1, 2)), dma((groups, comps + 1)), dma((groups,)), dma((1,)),
        dma((1,)), dma((n // 2,)), dma((1,)), dma((2, groups)), dma((groups, 2)), dma((2,)),
    )


def body(
    n, groups, levels, rank, comps,
    local_sem, own_sem, send_sem, piece_send, order_recv, mate_recv, z_recv, across_recv, ext_recv, near_recv,
    pair_recv, piece_recv, table_recv, w_recv, y_recv, mid_recv,
    forces, order_hbm, bases_hbm, tiles_hbm, near_col_hbm, basis_hbm, coupling_hbm, scale_hbm, ranks_hbm, targets_hbm,
    out,
    order, bases, coupling, near_col, scale, ranks, targets, tiles, basis,
    ext_out, ext_near, orders, spread, picks, own_pick, piece_out, piece_mate, pieces,
    table, w_out, w_in, w_own, w_low, w_all, y_out, y_in, y_mid, totals, pair_total,
    *blocks,
):
    g, c = lax.axis_index("grp"), lax.axis_index("clu")
    core = lax.rem(c, 2)
    tile, columns = forces.shape[1:]
    width = columns // groups
    quarter = tile // 4
    rows = comps * tile
    near_count = tiles.shape[0]
    far_count = targets.shape[1]
    half = n // 2
    cut = rank // 2
    piece_rows = levels * cut
    spans = [(level, 2 ** (level + 1)) for level in range(levels)]
    table_rows = sum(count - 1 for _, count in spans) * cut
    last = groups - 1
    own_blocks, far_blocks, side_blocks = (blocks[at * comps:(at + 1) * comps] for at in range(3))
    edge = 7 * core

    def at_clu(by):
        return {"grp": g, "clu": lax.rem(c + by + n, n)}

    partners = (g, g + 1 - 2 * lax.rem(g, 2), lax.rem(g + 2, groups), groups - 1 - g)

    def at_grp(i):
        return {"grp": partners[i], "clu": c}

    mate = {"grp": g, "clu": c + 1 - 2 * core}
    sends = []

    def remote(src, dst, recv, where, index=0):
        return pltpu.make_async_remote_copy(
            src_ref=src, dst_ref=dst, send_sem=send_sem.at[index], recv_sem=recv, device_id=where, device_id_type=MESH
        )

    def push(copies, bytes_of):
        assert len(sends) < SENDS
        for src, dst, recv, where in copies:
            remote(src, dst, recv, where, len(sends)).start()
        sends.append(remote(bytes_of, bytes_of, near_recv.at[0], mate, len(sends)))

    def landed(ref, recv):
        remote(ref, ref, recv, mate).wait_recv()

    def several(count):
        return own_blocks[0].at[0:count]

    def columns_of(i, d):
        return forces.at[d, :, pl.ds(pl.multiple_of(partners[i] * width, width), width)]

    def place_of(i, p, d, lo=0, hi=tile):
        if i == 0:
            return own_blocks[d].at[p, lo:hi]
        if i == last:
            return far_blocks[d].at[p, lo:hi]
        return side_blocks[d].at[p, lo:hi, pl.ds((i - 1) * width, width)]

    chunks = [(d, 0, tile) for d in range(comps - 1)]
    chunks += [(comps - 1, 0, tile // 2), (comps - 1, tile // 2, tile)]
    parts = range(len(chunks))

    def part(i, p, k):
        return place_of(i, p, *chunks[k])

    def part_bytes(k, count):
        return own_blocks[0].at[0:count, 0:chunks[k][2] - chunks[k][1]]

    def edge_rows(i, p, d):
        return place_of(i, p, d, 0, quarter)

    small = [
        pltpu.make_async_copy(src, dst, local_sem.at[at])
        for at, (src, dst) in enumerate((
            (order_hbm, order), (coupling_hbm, coupling), (targets_hbm, targets), (ranks_hbm, ranks),
            (scale_hbm, scale), (basis_hbm, basis), (bases_hbm, bases), (near_col_hbm, near_col), (tiles_hbm, tiles),
        ))
    ]
    for copy in small[:6]:
        copy.start()
    for i in (last, 0, 1, 2):
        for d in range(comps):
            pltpu.make_async_copy(columns_of(i, d), place_of(i, 3 + core, d), own_sem.at[i]).start()
    for copy in small[6:]:
        copy.start()

    barrier = pltpu.get_barrier_semaphore()

    def greet(d, carry):
        pl.semaphore_signal(barrier, inc=1, device_id=at_clu(d), device_id_type=MESH)
        return carry

    lax.fori_loop(1, n, greet, 0)
    for d in range(1, groups):
        pl.semaphore_signal(barrier, inc=1, device_id=at_grp(d), device_id_type=MESH)

    for block in blocks:
        block[edge, quarter:, :] = jnp.zeros((tile - quarter, block.shape[2]), BF16)
    ext_near[:, quarter:, :] = jnp.zeros((comps, ext_near.shape[1] - quarter, width), BF16)

    for copy in small[1:5]:
        copy.wait()
    lane = lax.broadcasted_iota(jnp.int32, (rank, 2 * table_rows), 1)
    row = lax.broadcasted_iota(jnp.int32, (rank, 2 * table_rows), 0)
    lane_row = (lane // table_rows) * cut + lax.rem(lane, cut)
    lane_slot = lax.rem(lane, table_rows) // cut
    repeat = (lane_row == row).astype(F32).astype(BF16)
    wide = jnp.dot(coupling[...], repeat, preferred_element_type=F32)
    for b in range(far_count):
        target = targets[0, b]
        slot_of, base, offset = target, 0, 0
        for level, count in spans:
            own = (c // 2) // (half // count)
            here = target - base - own - 1
            here = jnp.where(here < 0, here + count, here) + offset
            slot_of = jnp.where((target >= base) & (target < base + count), here, slot_of)
            base, offset = base + count, offset + count - 1
        keep = (lane_slot == slot_of) & (lane_row < ranks[0, b])
        scaled = jnp.where(keep, wide[b * rank:(b + 1) * rank, :] * scale[0, b], 0.0)
        high = scaled.astype(BF16)
        spread[b * rank:(b + 1) * rank, :2 * table_rows] = high
        spread[b * rank:(b + 1) * rank, 2 * table_rows:] = (scaled - high.astype(F32)).astype(BF16)
    small[5].wait()
    folded = lax.dot_general(basis[...], spread[...], (((0,), (0,)), ((), ())), preferred_element_type=F32)
    folded = folded[:, :2 * table_rows] + folded[:, 2 * table_rows:]
    w_out[...] = folded.reshape(groups, rows // groups, 2 * table_rows)

    sub = lax.broadcasted_iota(jnp.int32, (tile, tile), 0)
    lan = lax.broadcasted_iota(jnp.int32, (tile, tile), 1)
    upto = (sub <= lan).astype(BF16)

    def ranked(chosen):
        spots = jnp.broadcast_to(chosen.astype(F32), (8, tile)).astype(BF16)
        return (jnp.dot(spots, upto, preferred_element_type=F32)[0:1, :] - 1.0).astype(jnp.int32)

    def wrapped(spot):
        spot = jnp.where(spot < 0, spot + n * tile, spot)
        return jnp.where(spot >= n * tile, spot - n * tile, spot)

    def one_hot(spot, store, count):
        down = jnp.broadcast_to(spot.astype(F32), (128, tile)).T
        at = lax.broadcasted_iota(jnp.int32, (tile, 128), 1).astype(F32)
        for j in range(count):
            store(j, (down == at + float(j * 128)).astype(F32).astype(BF16))

    small[0].wait()
    spot = wrapped(order[...] - (c - core) * tile)
    beyond = spot >= 2 * tile
    spot = jnp.where(beyond, 2 * tile + ranked(beyond), spot)

    def store_own(j, value):
        own_pick[:, j * 128:(j + 1) * 128] = value

    one_hot(spot, store_own, own_pick.shape[1] // 128)

    def own_arrived(i):
        pltpu.make_async_copy(several(comps), several(comps), own_sem.at[i]).wait()

    own_arrived(last)
    pl.semaphore_wait(barrier, n - 1 + groups - 1)

    for by in (-1, 1, -2, 2):
        push([(order, orders.at[2 - by], order_recv.at[2 - by], at_clu(by))], order)

    def send_z(i, k):
        push(
            [
                (part(i, 3 + core, k), part(i, 1 + core, k), z_recv.at[i, k, 0], at_clu(2)),
                (part(i, 3 + core, k), part(i, 5 + core, k), z_recv.at[i, k, 1], at_clu(-2)),
            ],
            part_bytes(k, 2),
        )

    for k in range(2):
        send_z(last, k)
    push(
        [(w_out.at[partners[i]], w_in.at[i], w_recv.at[0, i], at_grp(i)) for i in range(1, groups)],
        w_out.at[0:groups - 1],
    )

    def send_mate(i):
        push(
            [(place_of(i, 3 + core, d), place_of(i, 3 + core, d), mate_recv.at[i], mate) for d in range(comps)],
            several(comps),
        )

    send_mate(last)
    own_arrived(0)
    send_mate(0)

    def order_landed(by):
        landed(orders.at[2 + by], order_recv.at[2 + by])

    for by in (-1, 1):
        order_landed(by)
    away = orders[1 + 2 * core] - c * tile
    chosen = (away >= 0) & (away < tile)
    place = jnp.where(chosen, ranked(chosen), -1)
    left = (lax.broadcasted_iota(jnp.int32, (128, tile), 0) == place).astype(F32).astype(BF16)
    right = (sub == away).astype(F32).astype(BF16)
    pick = lax.dot_general(left, right, (((1,), (1,)), ((), ())), preferred_element_type=F32).astype(BF16)

    def pick_edge(at, own):
        for d in range(comps):
            ext_out[at, d] = jnp.dot(pick, own[d][3 + core], preferred_element_type=F32).astype(BF16)[:quarter]

    pick_edge(1, far_blocks)
    push(
        [
            (ext_out.at[1, d], edge_rows(last, 7 - edge, d), ext_recv.at[last], at_clu(6 * core - 3))
            for d in range(comps)
        ],
        ext_out.at[1],
    )
    for k in parts[2:]:
        send_z(last, k)
    pick_edge(0, own_blocks)
    push([(ext_out.at[0], ext_near.at[:, 0:quarter], near_recv.at[0], at_clu(2 * core - 1))], ext_out.at[0])
    for k in parts[:2]:
        send_z(0, k)
    for i in (1, 2):
        own_arrived(i)
        send_mate(i)

    for by in (-2, 2):
        order_landed(by)
    orders[2] = order[...]
    small[7].wait()
    starts = []
    for j in range(near_count):
        spot0 = near_col[0, j] - c + 2
        spot0 = jnp.where(spot0 < 0, spot0 + n, spot0)
        spot0 = jnp.clip(jnp.where(spot0 >= n, spot0 - n, spot0), 0, 4)
        starts.append(spot0 + core)
        spot = wrapped(orders[spot0] - (c + spot0 - 3) * tile)
        low = 2 * core * tile
        beyond = (spot >= low) & (spot < low + tile) & (spot0 == 4 * core)
        spot = jnp.where(beyond, low + ranked(beyond), spot)

        def store_pick(at, value, j=j):
            picks[j, :, at * 128:(at + 1) * 128] = value

        one_hot(spot, store_pick, picks.shape[2] // 128)

    def relay(i, k):
        copies = []
        for side, p in enumerate((1 + core, 5 + core)):
            landed(part(i, p, k), z_recv.at[i, k, side])
            if i == last:
                for to, at in ((1, 2), (2, 1)):
                    copies.append((part(i, p, k), part(at, p, k), z_recv.at[at, k, side], at_grp(to)))
            copies.append((part(i, p, k), part(i, p, k), across_recv.at[i, k], mate))
        push(copies, part_bytes(k, len(copies)))

    def take(i, *ks):
        for k in ks:
            landed(part_bytes(k, 2), across_recv.at[i, k])

    def near(block, d):
        acc = None
        for j in range(near_count):
            held = block[d][pl.ds(starts[j], 3)].reshape(3 * tile, block[d].shape[2])
            x = jnp.dot(picks[j], held, preferred_element_type=F32).astype(BF16)
            term = jnp.dot(tiles[j, :, d * tile:(d + 1) * tile], x, preferred_element_type=F32)
            acc = term if acc is None else acc + term
        return acc

    mid = rows // 2

    relay(last, 0)
    relay(last, 1)
    for i in range(1, groups):
        landed(w_in.at[i], w_recv.at[0, i])
    summed = w_out[g]
    for i in range(1, groups):
        summed = summed + w_in[i]
    high = summed.astype(BF16)
    w_own[...] = high
    w_all[g] = high
    w_low[...] = (summed - high.astype(F32)).astype(BF16)
    relay(last, 2)
    landed(ext_out.at[1], ext_recv.at[last])
    push(
        [
            (edge_rows(last, edge, d), edge_rows(at, edge, d), ext_recv.at[at], at_grp(to))
            for to, at in ((1, 2), (2, 1)) for d in range(comps)
        ],
        ext_out,
    )
    relay(last, 3)
    landed(several(comps), mate_recv.at[last])
    small[8].wait()
    take(last, 0)
    totals[...] = near(far_blocks, 0)
    for i in (1, 2):
        relay(i, 0)
    take(last, 1)
    totals[...] += near(far_blocks, 1)
    for i in (1, 2):
        relay(i, 1)
    take(last, 2, 3)
    y_out[last] = (totals[...] + near(far_blocks, 2)).astype(BF16)
    push(
        [
            (y_out.at[last, 0:mid], y_mid.at[0], mid_recv.at[0], at_grp(1)),
            (y_out.at[last, mid:rows], y_mid.at[1], mid_recv.at[1], at_grp(2)),
        ],
        y_out.at[last],
    )
    push([(w_own, w_all.at[g], w_recv.at[1, i], at_grp(i)) for i in range(1, groups)], w_all.at[0:groups - 1])

    for i in (1, 2):
        relay(i, 2)
    small[6].wait()
    landed(ext_out.at[0], near_recv.at[0])
    push(
        [
            (ext_near.at[d, 0:quarter], edge_rows(0, edge, d), ext_recv.at[0], at_clu(2 - 4 * core))
            for d in range(comps)
        ],
        ext_out.at[0],
    )
    landed(several(comps), mate_recv.at[0])
    piece = jnp.zeros((2 * piece_rows, width), F32)
    for d in range(comps):
        x = jnp.dot(own_pick[:, :2 * tile], own_blocks[d][3:5].reshape(2 * tile, width), preferred_element_type=F32)
        x = x + jnp.dot(own_pick[:, 2 * tile:], ext_near[d], preferred_element_type=F32)
        weights = jnp.concatenate(
            [bases[level, d, h * cut:(h + 1) * cut] for h in range(2) for level in range(levels)], axis=0
        )
        piece = piece + jnp.dot(weights, x.astype(BF16), preferred_element_type=F32)
    for h in range(2):
        piece_out[h] = piece[h * piece_rows:(h + 1) * piece_rows]
    push([(piece_out.at[1 - core], piece_mate, pair_recv.at[0], mate)], piece_mate)
    for i in (1, 2):
        relay(i, 3)

    landed(piece_mate, pair_recv.at[0])
    pair = piece_out[core] + piece_mate[...]
    piece_out[2] = pair
    pieces[c // 2] = pair

    def piece_copy(d):
        return pltpu.make_async_remote_copy(
            src_ref=piece_out.at[2], dst_ref=pieces.at[c // 2], send_sem=piece_send.at[d],
            recv_sem=piece_recv.at[c // 2], device_id=at_clu(2 * d), device_id_type=MESH,
        )

    def start_piece(d, carry):
        piece_copy(d).start()
        return carry

    lax.fori_loop(1, half, start_piece, 0)
    for k in parts[2:]:
        send_z(0, k)

    for i in (1, 2):
        landed(several(comps), mate_recv.at[i])
        landed(ext_out.at[0], ext_recv.at[i])
        take(i, 0)
    pair_total[...] = near(side_blocks, 0)
    for i in (1, 2):
        take(i, 1)
    pair_total[...] += near(side_blocks, 1)
    relay(0, 0)
    for i in (1, 2):
        take(i, 2, 3)
    both = pair_total[...] + near(side_blocks, 2)

    def send_y(i, h, value):
        here = pl.ds(h * mid, mid)
        y_out[i, h * mid:(h + 1) * mid] = value.astype(BF16)
        push([(y_out.at[i, here], y_in.at[i, here], y_recv.at[i, h], at_grp(i))], y_mid.at[0])

    def half_of(i, h):
        return both[h * mid:(h + 1) * mid, (i - 1) * width:i * width]

    send_y(1, 0, half_of(1, 0))
    send_y(2, 1, half_of(2, 1))
    landed(y_mid.at[1], mid_recv.at[1])
    send_y(1, 1, half_of(1, 1) + y_mid[1].astype(F32))
    landed(y_mid.at[0], mid_recv.at[0])
    send_y(2, 0, half_of(2, 0) + y_mid[0].astype(F32))
    relay(0, 1)

    landed(ext_out.at[0], ext_recv.at[0])
    take(0, 0)
    totals[...] = near(own_blocks, 0)

    def await_piece(d, carry):
        source = lax.rem(c // 2 + d, half)
        landed(pieces.at[source], piece_recv.at[source])
        return carry

    lax.fori_loop(1, half, await_piece, 0)
    at = 0
    for level, count in spans:
        members = half // count
        own = (c // 2) // members
        for step in range(count - 1):
            k = lax.rem(own + 1 + step, count)
            entry = lax.fori_loop(
                0, members,
                lambda m, acc, k=k, members=members, level=level: acc
                + pieces[k * members + m, level * cut:(level + 1) * cut, :],
                jnp.zeros((cut, width), F32),
            )
            table[core, at:at + cut, :] = entry
            at += cut
    push([(table.at[core], table.at[core], table_recv.at[0], mate)], table.at[0])

    take(0, 1)
    totals[...] += near(own_blocks, 1)
    relay(0, 2)
    for i in range(1, groups):
        landed(w_own, w_recv.at[1, i])
    landed(table.at[0], table_recv.at[0])
    entries = table[...].reshape(2 * table_rows, width)
    high = entries.astype(BF16)
    low = (entries - high.astype(F32)).astype(BF16)
    weights = w_all[...].reshape(rows, 2 * table_rows)
    answer = jnp.dot(weights, high, preferred_element_type=F32) + jnp.dot(weights, low, preferred_element_type=F32)
    totals[...] += answer
    own_rows = pl.ds(pl.multiple_of(g * (rows // groups), rows // groups), rows // groups)
    totals[own_rows] += jnp.dot(w_low[...], high, preferred_element_type=F32)
    relay(0, 3)
    take(0, 2, 3)
    totals[...] += near(own_blocks, 2)

    for copy in sends:
        copy.wait_send()

    def end_piece(d, carry):
        piece_copy(d).wait_send()
        return carry

    lax.fori_loop(1, half, end_piece, 0)
    for i in (1, 2):
        for h in range(2):
            landed(y_mid.at[0], y_recv.at[i, h])
    out[...] = (totals[...] + y_in[1].astype(F32) + y_in[2].astype(F32)).reshape(comps, tile, width)


def solution(mesh):
    n, groups = mesh.shape["clu"], mesh.shape["grp"]

    def on_device(forces, order, bases, near_tiles, near_col, far_basis, far_coupling, far_scale, far_rank, far_target):
        comps, tile, columns = forces.shape
        levels, rank = bases.shape[:2]
        near_count, far_count = near_tiles.shape[1], far_basis.shape[1]
        width, rows, quarter = columns // groups, comps * tile, tile // 4
        cut = rank // 2
        piece_rows = levels * cut
        table_rows = sum(2 ** (level + 1) - 1 for level in range(levels)) * cut
        slots = 8
        pad = 128
        vmem, hbm = (pl.BlockSpec(memory_space=m) for m in (pltpu.VMEM, pl.ANY))
        operands = (
            forces,
            order.reshape(1, tile),
            jnp.transpose(bases, (0, 2, 1, 3)),
            near_tiles.reshape(near_count, rows, rows),
            near_col,
            far_basis.reshape(far_count * rank, rows),
            far_coupling.reshape(far_count * rank, rank),
            far_scale,
            far_rank,
            far_target,
        )
        return pl.pallas_call(
            functools.partial(kernel, n, groups, levels, rank, comps),
            out_shape=jax.ShapeDtypeStruct((comps, tile, width), F32),
            in_specs=[hbm] * len(operands),
            out_specs=vmem,
            scratch_shapes=[
                pltpu.VMEM((1, tile), jnp.int32),
                pltpu.VMEM((levels, comps, rank, tile), BF16),
                pltpu.VMEM((far_count * rank, rank), BF16),
                pltpu.SMEM((1, near_count), jnp.int32),
                pltpu.SMEM((1, far_count), F32),
                pltpu.SMEM((1, far_count), jnp.int32),
                pltpu.SMEM((1, far_count), jnp.int32),
                pltpu.VMEM((near_count, rows, rows), BF16),
                pltpu.VMEM((far_count * rank, rows), BF16),
                pltpu.VMEM((2, comps, quarter, width), BF16),
                pltpu.VMEM((comps, pad, width), BF16),
                pltpu.VMEM((5, 1, tile), jnp.int32),
                pltpu.VMEM((far_count * rank, 4 * table_rows), BF16),
                pltpu.VMEM((near_count, tile, 3 * tile), BF16),
                pltpu.VMEM((tile, 2 * tile + pad), BF16),
                pltpu.VMEM((3, piece_rows, width), F32),
                pltpu.VMEM((piece_rows, width), F32),
                pltpu.VMEM((n // 2, piece_rows, width), F32),
                pltpu.VMEM((2, table_rows, width), F32),
                pltpu.VMEM((groups, rows // groups, 2 * table_rows), F32),
                pltpu.VMEM((groups, rows // groups, 2 * table_rows), F32),
                pltpu.VMEM((rows // groups, 2 * table_rows), BF16),
                pltpu.VMEM((rows // groups, 2 * table_rows), BF16),
                pltpu.VMEM((groups, rows // groups, 2 * table_rows), BF16),
                pltpu.VMEM((groups, rows, width), BF16),
                pltpu.VMEM((groups, rows, width), BF16),
                pltpu.VMEM((2, rows // 2, width), BF16),
                pltpu.VMEM((rows, width), F32),
                pltpu.VMEM((rows, 2 * width), F32),
                *(pltpu.VMEM((slots, tile, size), BF16) for size in (width, width, 2 * width) for _ in range(comps)),
            ],
            compiler_params=pltpu.CompilerParams(
                collective_id=0, has_side_effects=True, vmem_limit_bytes=28 * 1024 * 1024
            ),
        )(*(pltpu.with_memory_space_constraint(operand, pltpu.HBM) for operand in operands))

    placed = (
        P(None, "clu", None),
        P("clu"),
        P(None, None, None, "clu"),
        P("clu", "grp", None, None),
        P("clu", "grp"),
        P("clu", "grp", None, None),
        P("clu", "grp", None, None),
        P("clu", "grp"),
        P("clu", "grp"),
        P("clu", "grp"),
    )
    return jax.shard_map(
        on_device, mesh=mesh, in_specs=placed, out_specs=P(None, "clu", "grp"), check_vma=False
    )
```

```python
import functools

import jax
import jax.numpy as jnp
from jax import lax
from jax.experimental import pallas as pl
from jax.experimental.pallas import tpu as pltpu
from jax.sharding import PartitionSpec as P

MESH = pl.DeviceIdType.MESH
F32, BF16 = jnp.float32, jnp.bfloat16
SENDS = 48


def kernel(n, groups, levels, rank, comps, *refs):
    dma = pltpu.SemaphoreType.DMA

    def scoped(*sems):
        body(n, groups, levels, rank, comps, *sems, *refs)

    pl.run_scoped(
        scoped,
        dma((9,)), dma((groups,)), dma((SENDS,)), dma((n // 2,)),
        dma((5,)), dma((groups,)), dma((groups, comps + 1, 2)), dma((groups, comps + 1)), dma((groups,)), dma((1,)),
        dma((1,)), dma((n // 2,)), dma((1,)), dma((2, groups)), dma((groups, 2)), dma((2,)),
    )


def body(
    n, groups, levels, rank, comps,
    local_sem, own_sem, send_sem, piece_send, order_recv, mate_recv, z_recv, across_recv, ext_recv, near_recv,
    pair_recv, piece_recv, table_recv, w_recv, y_recv, mid_recv,
    forces, order_hbm, bases_hbm, tiles_hbm, near_col_hbm, basis_hbm, coupling_hbm, scale_hbm, ranks_hbm, targets_hbm,
    out,
    order, bases, coupling, near_col, scale, ranks, targets, tiles, basis,
    ext_out, ext_near, orders, spread, picks, own_pick, piece_out, piece_mate, pieces,
    table, w_out, w_in, w_own, w_low, w_all, y_out, y_in, y_mid, totals, pair_total,
    *blocks,
):
    g, c = lax.axis_index("grp"), lax.axis_index("clu")
    core = lax.rem(c, 2)
    tile, columns = forces.shape[1:]
    width = columns // groups
    quarter = tile // 4
    rows = comps * tile
    near_count = tiles.shape[0]
    far_count = targets.shape[1]
    half = n // 2
    cut = rank // 2
    piece_rows = levels * cut
    spans = [(level, 2 ** (level + 1)) for level in range(levels)]
    table_rows = sum(count - 1 for _, count in spans) * cut
    last = groups - 1
    own_blocks, far_blocks, side_blocks = (blocks[at * comps:(at + 1) * comps] for at in range(3))
    edge = 7 * core

    def at_clu(by):
        return {"grp": g, "clu": lax.rem(c + by + n, n)}

    partners = (g, g + 1 - 2 * lax.rem(g, 2), lax.rem(g + 2, groups), groups - 1 - g)

    def at_grp(i):
        return {"grp": partners[i], "clu": c}

    mate = {"grp": g, "clu": c + 1 - 2 * core}
    sends = []

    def remote(src, dst, recv, where, index=0):
        return pltpu.make_async_remote_copy(
            src_ref=src, dst_ref=dst, send_sem=send_sem.at[index], recv_sem=recv, device_id=where, device_id_type=MESH
        )

    def push(copies, bytes_of):
        assert len(sends) < SENDS
        for src, dst, recv, where in copies:
            remote(src, dst, recv, where, len(sends)).start()
        sends.append(remote(bytes_of, bytes_of, near_recv.at[0], mate, len(sends)))

    def landed(ref, recv):
        remote(ref, ref, recv, mate).wait_recv()

    def several(count):
        return own_blocks[0].at[0:count]

    def columns_of(i, d):
        return forces.at[d, :, pl.ds(pl.multiple_of(partners[i] * width, width), width)]

    def place_of(i, p, d, lo=0, hi=tile):
        if i == 0:
            return own_blocks[d].at[p, lo:hi]
        if i == last:
            return far_blocks[d].at[p, lo:hi]
        return side_blocks[d].at[p, lo:hi, pl.ds((i - 1) * width, width)]

    chunks = [(d, 0, tile) for d in range(comps - 1)]
    chunks += [(comps - 1, 0, tile // 2), (comps - 1, tile // 2, tile)]
    parts = range(len(chunks))

    def part(i, p, k):
        return place_of(i, p, *chunks[k])

    def part_bytes(k, count):
        return own_blocks[0].at[0:count, 0:chunks[k][2] - chunks[k][1]]

    def edge_rows(i, p, d):
        return place_of(i, p, d, 0, quarter)

    small = [
        pltpu.make_async_copy(src, dst, local_sem.at[at])
        for at, (src, dst) in enumerate((
            (order_hbm, order), (coupling_hbm, coupling), (targets_hbm, targets), (ranks_hbm, ranks),
            (scale_hbm, scale), (basis_hbm, basis), (bases_hbm, bases), (near_col_hbm, near_col), (tiles_hbm, tiles),
        ))
    ]
    for d in range(comps):
        pltpu.make_async_copy(columns_of(last, d), place_of(last, 3 + core, d), own_sem.at[last]).start()
    small[0].start()

    barrier = pltpu.get_barrier_semaphore()

    def greet(d, carry):
        pl.semaphore_signal(barrier, inc=1, device_id=at_clu(d), device_id_type=MESH)
        return carry

    lax.fori_loop(1, n, greet, 0)
    for d in range(1, groups):
        pl.semaphore_signal(barrier, inc=1, device_id=at_grp(d), device_id_type=MESH)

    for copy in small[1:6]:
        copy.start()
    for i in (0, 1, 2):
        for d in range(comps):
            pltpu.make_async_copy(columns_of(i, d), place_of(i, 3 + core, d), own_sem.at[i]).start()
    for copy in small[6:]:
        copy.start()

    for block in blocks:
        block[edge, quarter:, :] = jnp.zeros((tile - quarter, block.shape[2]), BF16)
    ext_near[:, quarter:, :] = jnp.zeros((comps, ext_near.shape[1] - quarter, width), BF16)

    sub = lax.broadcasted_iota(jnp.int32, (tile, tile), 0)
    lan = lax.broadcasted_iota(jnp.int32, (tile, tile), 1)
    upto = (sub <= lan).astype(BF16)

    def ranked(chosen):
        spots = jnp.broadcast_to(chosen.astype(F32), (8, tile)).astype(BF16)
        return (jnp.dot(spots, upto, preferred_element_type=F32)[0:1, :] - 1.0).astype(jnp.int32)

    def wrapped(spot):
        spot = jnp.where(spot < 0, spot + n * tile, spot)
        return jnp.where(spot >= n * tile, spot - n * tile, spot)

    def one_hot(spot, store, count):
        down = jnp.broadcast_to(spot.astype(F32), (128, tile)).T
        at = lax.broadcasted_iota(jnp.int32, (tile, 128), 1).astype(F32)
        for j in range(count):
            store(j, (down == at + float(j * 128)).astype(F32).astype(BF16))

    def own_arrived(i):
        pltpu.make_async_copy(several(comps), several(comps), own_sem.at[i]).wait()

    small[0].wait()
    own_arrived(last)
    pl.semaphore_wait(barrier, n - 1 + groups - 1)

    for by in (-1, 1, -2, 2):
        push([(order, orders.at[2 - by], order_recv.at[2 - by], at_clu(by))], order)

    def send_z(i, k):
        push(
            [
                (part(i, 3 + core, k), part(i, 1 + core, k), z_recv.at[i, k, 0], at_clu(2)),
                (part(i, 3 + core, k), part(i, 5 + core, k), z_recv.at[i, k, 1], at_clu(-2)),
            ],
            part_bytes(k, 2),
        )

    for k in range(2):
        send_z(last, k)
    for copy in small[1:5]:
        copy.wait()
    lane = lax.broadcasted_iota(jnp.int32, (rank, 2 * table_rows), 1)
    row = lax.broadcasted_iota(jnp.int32, (rank, 2 * table_rows), 0)
    lane_row = (lane // table_rows) * cut + lax.rem(lane, cut)
    lane_slot = lax.rem(lane, table_rows) // cut
    repeat = (lane_row == row).astype(F32).astype(BF16)
    wide = jnp.dot(coupling[...], repeat, preferred_element_type=F32)
    for b in range(far_count):
        target = targets[0, b]
        slot_of, base, offset = target, 0, 0
        for level, count in spans:
            own = (c // 2) // (half // count)
            here = target - base - own - 1
            here = jnp.where(here < 0, here + count, here) + offset
            slot_of = jnp.where((target >= base) & (target < base + count), here, slot_of)
            base, offset = base + count, offset + count - 1
        keep = (lane_slot == slot_of) & (lane_row < ranks[0, b])
        scaled = jnp.where(keep, wide[b * rank:(b + 1) * rank, :] * scale[0, b], 0.0)
        high = scaled.astype(BF16)
        spread[b * rank:(b + 1) * rank, :2 * table_rows] = high
        spread[b * rank:(b + 1) * rank, 2 * table_rows:] = (scaled - high.astype(F32)).astype(BF16)
    small[5].wait()
    folded = lax.dot_general(basis[...], spread[...], (((0,), (0,)), ((), ())), preferred_element_type=F32)
    folded = folded[:, :2 * table_rows] + folded[:, 2 * table_rows:]
    w_out[...] = folded.reshape(groups, rows // groups, 2 * table_rows)

    push(
        [(w_out.at[partners[i]], w_in.at[i], w_recv.at[0, i], at_grp(i)) for i in range(1, groups)],
        w_out.at[0:groups - 1],
    )

    def send_mate(i):
        push(
            [(place_of(i, 3 + core, d), place_of(i, 3 + core, d), mate_recv.at[i], mate) for d in range(comps)],
            several(comps),
        )

    send_mate(last)
    own_arrived(0)
    send_mate(0)

    def order_landed(by):
        landed(orders.at[2 + by], order_recv.at[2 + by])

    spot = wrapped(order[...] - (c - core) * tile)
    beyond = spot >= 2 * tile
    spot = jnp.where(beyond, 2 * tile + ranked(beyond), spot)

    def store_own(j, value):
        own_pick[:, j * 128:(j + 1) * 128] = value

    one_hot(spot, store_own, own_pick.shape[1] // 128)

    for by in (-1, 1):
        order_landed(by)
    away = orders[1 + 2 * core] - c * tile
    chosen = (away >= 0) & (away < tile)
    place = jnp.where(chosen, ranked(chosen), -1)
    left = (lax.broadcasted_iota(jnp.int32, (128, tile), 0) == place).astype(F32).astype(BF16)
    right = (sub == away).astype(F32).astype(BF16)
    pick = lax.dot_general(left, right, (((1,), (1,)), ((), ())), preferred_element_type=F32).astype(BF16)

    def pick_edge(at, own):
        for d in range(comps):
            ext_out[at, d] = jnp.dot(pick, own[d][3 + core], preferred_element_type=F32).astype(BF16)[:quarter]

    pick_edge(1, far_blocks)
    push(
        [
            (ext_out.at[1, d], edge_rows(last, 7 - edge, d), ext_recv.at[last], at_clu(6 * core - 3))
            for d in range(comps)
        ],
        ext_out.at[1],
    )
    for k in parts[2:]:
        send_z(last, k)
    pick_edge(0, own_blocks)
    push([(ext_out.at[0], ext_near.at[:, 0:quarter], near_recv.at[0], at_clu(2 * core - 1))], ext_out.at[0])
    for i in (1, 2):
        own_arrived(i)
        send_mate(i)

    for by in (-2, 2):
        order_landed(by)
    orders[2] = order[...]
    small[7].wait()
    starts = []
    for j in range(near_count):
        spot0 = near_col[0, j] - c + 2
        spot0 = jnp.where(spot0 < 0, spot0 + n, spot0)
        spot0 = jnp.clip(jnp.where(spot0 >= n, spot0 - n, spot0), 0, 4)
        starts.append(spot0 + core)
        spot = wrapped(orders[spot0] - (c + spot0 - 3) * tile)
        low = 2 * core * tile
        beyond = (spot >= low) & (spot < low + tile) & (spot0 == 4 * core)
        spot = jnp.where(beyond, low + ranked(beyond), spot)

        def store_pick(at, value, j=j):
            picks[j, :, at * 128:(at + 1) * 128] = value

        one_hot(spot, store_pick, picks.shape[2] // 128)

    def relay(i, k):
        copies = []
        for side, p in enumerate((1 + core, 5 + core)):
            landed(part(i, p, k), z_recv.at[i, k, side])
            if i == last:
                for to, at in ((1, 2), (2, 1)):
                    copies.append((part(i, p, k), part(at, p, k), z_recv.at[at, k, side], at_grp(to)))
            copies.append((part(i, p, k), part(i, p, k), across_recv.at[i, k], mate))
        push(copies, part_bytes(k, len(copies)))

    def take(i, *ks):
        for k in ks:
            landed(part_bytes(k, 2), across_recv.at[i, k])

    def near(block, lo, hi):
        acc = None
        for j in range(near_count):
            found = [
                jnp.dot(
                    picks[j], block[d][pl.ds(starts[j], 3)].reshape(3 * tile, block[d].shape[2]),
                    preferred_element_type=F32,
                ).astype(BF16)
                for d in range(lo, hi)
            ]
            term = jnp.dot(
                tiles[j, :, lo * tile:hi * tile], jnp.concatenate(found, axis=0), preferred_element_type=F32
            )
            acc = term if acc is None else acc + term
        return acc

    mid = rows // 2

    relay(last, 0)
    relay(last, 1)
    send_z(0, 0)
    for i in range(1, groups):
        landed(w_in.at[i], w_recv.at[0, i])
    summed = w_out[g]
    for i in range(1, groups):
        summed = summed + w_in[i]
    high = summed.astype(BF16)
    w_own[...] = high
    w_all[g] = high
    w_low[...] = (summed - high.astype(F32)).astype(BF16)
    relay(last, 2)
    send_z(0, 1)
    landed(ext_out.at[1], ext_recv.at[last])
    push(
        [
            (edge_rows(last, edge, d), edge_rows(at, edge, d), ext_recv.at[at], at_grp(to))
            for to, at in ((1, 2), (2, 1)) for d in range(comps)
        ],
        ext_out,
    )
    landed(several(comps), mate_recv.at[last])
    small[8].wait()
    take(last, 0, 1)
    totals[...] = near(far_blocks, 0, comps - 1)
    relay(last, 3)
    for i in (1, 2):
        relay(i, 0)
    take(last, 2, 3)
    y_out[last] = (totals[...] + near(far_blocks, comps - 1, comps)).astype(BF16)
    push(
        [
            (y_out.at[last, 0:mid], y_mid.at[0], mid_recv.at[0], at_grp(1)),
            (y_out.at[last, mid:rows], y_mid.at[1], mid_recv.at[1], at_grp(2)),
        ],
        y_out.at[last],
    )
    push([(w_own, w_all.at[g], w_recv.at[1, i], at_grp(i)) for i in range(1, groups)], w_all.at[0:groups - 1])

    for k in (1, 2):
        for i in (1, 2):
            relay(i, k)
    small[6].wait()
    landed(ext_out.at[0], near_recv.at[0])
    push(
        [
            (ext_near.at[d, 0:quarter], edge_rows(0, edge, d), ext_recv.at[0], at_clu(2 - 4 * core))
            for d in range(comps)
        ],
        ext_out.at[0],
    )
    landed(several(comps), mate_recv.at[0])
    piece = jnp.zeros((2 * piece_rows, width), F32)
    for d in range(comps):
        x = jnp.dot(own_pick[:, :2 * tile], own_blocks[d][3:5].reshape(2 * tile, width), preferred_element_type=F32)
        x = x + jnp.dot(own_pick[:, 2 * tile:], ext_near[d], preferred_element_type=F32)
        weights = jnp.concatenate(
            [bases[level, d, h * cut:(h + 1) * cut] for h in range(2) for level in range(levels)], axis=0
        )
        piece = piece + jnp.dot(weights, x.astype(BF16), preferred_element_type=F32)
    for h in range(2):
        piece_out[h] = piece[h * piece_rows:(h + 1) * piece_rows]
    push([(piece_out.at[1 - core], piece_mate, pair_recv.at[0], mate)], piece_mate)
    for i in (1, 2):
        relay(i, 3)

    landed(piece_mate, pair_recv.at[0])
    pair = piece_out[core] + piece_mate[...]
    piece_out[2] = pair
    pieces[c // 2] = pair

    def piece_copy(d):
        return pltpu.make_async_remote_copy(
            src_ref=piece_out.at[2], dst_ref=pieces.at[c // 2], send_sem=piece_send.at[d],
            recv_sem=piece_recv.at[c // 2], device_id=at_clu(2 * d), device_id_type=MESH,
        )

    def start_piece(d, carry):
        piece_copy(d).start()
        return carry

    lax.fori_loop(1, half, start_piece, 0)
    for k in parts[2:]:
        send_z(0, k)

    for i in (1, 2):
        landed(several(comps), mate_recv.at[i])
        landed(ext_out.at[0], ext_recv.at[i])
        take(i, 0, 1)
    pair_total[...] = near(side_blocks, 0, comps - 1)
    relay(0, 0)
    for i in (1, 2):
        take(i, 2, 3)
    both = pair_total[...] + near(side_blocks, comps - 1, comps)

    def send_y(i, h, value):
        here = pl.ds(h * mid, mid)
        y_out[i, h * mid:(h + 1) * mid] = value.astype(BF16)
        push([(y_out.at[i, here], y_in.at[i, here], y_recv.at[i, h], at_grp(i))], y_mid.at[0])

    def half_of(i, h):
        return both[h * mid:(h + 1) * mid, (i - 1) * width:i * width]

    send_y(1, 0, half_of(1, 0))
    send_y(2, 1, half_of(2, 1))
    landed(y_mid.at[1], mid_recv.at[1])
    send_y(1, 1, half_of(1, 1) + y_mid[1].astype(F32))
    landed(y_mid.at[0], mid_recv.at[0])
    send_y(2, 0, half_of(2, 0) + y_mid[0].astype(F32))
    relay(0, 1)

    landed(ext_out.at[0], ext_recv.at[0])
    take(0, 0)
    totals[...] = near(own_blocks, 0, 1)

    def await_piece(d, carry):
        source = lax.rem(c // 2 + d, half)
        landed(pieces.at[source], piece_recv.at[source])
        return carry

    lax.fori_loop(1, half, await_piece, 0)
    at = 0
    for level, count in spans:
        members = half // count
        own = (c // 2) // members
        for step in range(count - 1):
            k = lax.rem(own + 1 + step, count)
            entry = lax.fori_loop(
                0, members,
                lambda m, acc, k=k, members=members, level=level: acc
                + pieces[k * members + m, level * cut:(level + 1) * cut, :],
                jnp.zeros((cut, width), F32),
            )
            table[core, at:at + cut, :] = entry
            at += cut
    push([(table.at[core], table.at[core], table_recv.at[0], mate)], table.at[0])

    take(0, 1)
    totals[...] += near(own_blocks, 1, 2)
    relay(0, 2)
    for i in range(1, groups):
        landed(w_own, w_recv.at[1, i])
    landed(table.at[0], table_recv.at[0])
    entries = table[...].reshape(2 * table_rows, width)
    high = entries.astype(BF16)
    low = (entries - high.astype(F32)).astype(BF16)
    weights = w_all[...].reshape(rows, 2 * table_rows)
    answer = jnp.dot(weights, high, preferred_element_type=F32) + jnp.dot(weights, low, preferred_element_type=F32)
    totals[...] += answer
    own_rows = pl.ds(pl.multiple_of(g * (rows // groups), rows // groups), rows // groups)
    totals[own_rows] += jnp.dot(w_low[...], high, preferred_element_type=F32)
    relay(0, 3)
    take(0, 2, 3)
    totals[...] += near(own_blocks, comps - 1, comps)

    for copy in sends:
        copy.wait_send()

    def end_piece(d, carry):
        piece_copy(d).wait_send()
        return carry

    lax.fori_loop(1, half, end_piece, 0)
    for i in (1, 2):
        for h in range(2):
            landed(y_mid.at[0], y_recv.at[i, h])
    out[...] = (totals[...] + y_in[1].astype(F32) + y_in[2].astype(F32)).reshape(comps, tile, width)


def solution(mesh):
    n, groups = mesh.shape["clu"], mesh.shape["grp"]

    def on_device(forces, order, bases, near_tiles, near_col, far_basis, far_coupling, far_scale, far_rank, far_target):
        comps, tile, columns = forces.shape
        levels, rank = bases.shape[:2]
        near_count, far_count = near_tiles.shape[1], far_basis.shape[1]
        width, rows, quarter = columns // groups, comps * tile, tile // 4
        cut = rank // 2
        piece_rows = levels * cut
        table_rows = sum(2 ** (level + 1) - 1 for level in range(levels)) * cut
        slots = 8
        pad = 128
        vmem, hbm = (pl.BlockSpec(memory_space=m) for m in (pltpu.VMEM, pl.ANY))
        operands = (
            forces,
            order.reshape(1, tile),
            jnp.transpose(bases, (0, 2, 1, 3)),
            near_tiles.reshape(near_count, rows, rows),
            near_col,
            far_basis.reshape(far_count * rank, rows),
            far_coupling.reshape(far_count * rank, rank),
            far_scale,
            far_rank,
            far_target,
        )
        return pl.pallas_call(
            functools.partial(kernel, n, groups, levels, rank, comps),
            out_shape=jax.ShapeDtypeStruct((comps, tile, width), F32),
            in_specs=[hbm] * len(operands),
            out_specs=vmem,
            scratch_shapes=[
                pltpu.VMEM((1, tile), jnp.int32),
                pltpu.VMEM((levels, comps, rank, tile), BF16),
                pltpu.VMEM((far_count * rank, rank), BF16),
                pltpu.SMEM((1, near_count), jnp.int32),
                pltpu.SMEM((1, far_count), F32),
                pltpu.SMEM((1, far_count), jnp.int32),
                pltpu.SMEM((1, far_count), jnp.int32),
                pltpu.VMEM((near_count, rows, rows), BF16),
                pltpu.VMEM((far_count * rank, rows), BF16),
                pltpu.VMEM((2, comps, quarter, width), BF16),
                pltpu.VMEM((comps, pad, width), BF16),
                pltpu.VMEM((5, 1, tile), jnp.int32),
                pltpu.VMEM((far_count * rank, 4 * table_rows), BF16),
                pltpu.VMEM((near_count, tile, 3 * tile), BF16),
                pltpu.VMEM((tile, 2 * tile + pad), BF16),
                pltpu.VMEM((3, piece_rows, width), F32),
                pltpu.VMEM((piece_rows, width), F32),
                pltpu.VMEM((n // 2, piece_rows, width), F32),
                pltpu.VMEM((2, table_rows, width), F32),
                pltpu.VMEM((groups, rows // groups, 2 * table_rows), F32),
                pltpu.VMEM((groups, rows // groups, 2 * table_rows), F32),
                pltpu.VMEM((rows // groups, 2 * table_rows), BF16),
                pltpu.VMEM((rows // groups, 2 * table_rows), BF16),
                pltpu.VMEM((groups, rows // groups, 2 * table_rows), BF16),
                pltpu.VMEM((groups, rows, width), BF16),
                pltpu.VMEM((groups, rows, width), BF16),
                pltpu.VMEM((2, rows // 2, width), BF16),
                pltpu.VMEM((rows, width), F32),
                pltpu.VMEM((rows, 2 * width), F32),
                *(pltpu.VMEM((slots, tile, size), BF16) for size in (width, width, 2 * width) for _ in range(comps)),
            ],
            compiler_params=pltpu.CompilerParams(
                collective_id=0, has_side_effects=True, vmem_limit_bytes=28 * 1024 * 1024
            ),
        )(*(pltpu.with_memory_space_constraint(operand, pltpu.HBM) for operand in operands))

    placed = (
        P(None, "clu", None),
        P("clu"),
        P(None, None, None, "clu"),
        P("clu", "grp", None, None),
        P("clu", "grp"),
        P("clu", "grp", None, None),
        P("clu", "grp", None, None),
        P("clu", "grp"),
        P("clu", "grp"),
        P("clu", "grp"),
    )
    return jax.shard_map(
        on_device, mesh=mesh, in_specs=placed, out_specs=P(None, "clu", "grp"), check_vma=False
    )
```

```python
import functools

import jax
import jax.numpy as jnp
from jax import lax
from jax.experimental import pallas as pl
from jax.experimental.pallas import tpu as pltpu
from jax.sharding import PartitionSpec as P

MESH = pl.DeviceIdType.MESH
F32, BF16 = jnp.float32, jnp.bfloat16
SENDS = 48


def kernel(n, groups, levels, rank, comps, *refs):
    dma = pltpu.SemaphoreType.DMA

    def scoped(*sems):
        body(n, groups, levels, rank, comps, *sems, *refs)

    pl.run_scoped(
        scoped,
        dma((9,)), dma((groups,)), dma((SENDS,)), dma((n // 2,)),
        dma((5,)), dma((groups,)), dma((groups, comps + 1, 2)), dma((groups, comps + 1)), dma((groups,)), dma((1,)),
        dma((1,)), dma((n // 2,)), dma((1,)), dma((2, groups)), dma((groups, 2)), dma((2,)),
    )


def body(
    n, groups, levels, rank, comps,
    local_sem, own_sem, send_sem, piece_send, order_recv, mate_recv, z_recv, across_recv, ext_recv, near_recv,
    pair_recv, piece_recv, table_recv, w_recv, y_recv, mid_recv,
    forces, order_hbm, bases_hbm, tiles_hbm, near_col_hbm, basis_hbm, coupling_hbm, scale_hbm, ranks_hbm, targets_hbm,
    out,
    order, bases, coupling, near_col, scale, ranks, targets, tiles, basis,
    ext_out, ext_near, orders, spread, picks, own_pick, piece_out, piece_mate, pieces,
    table, w_out, w_in, w_own, w_low, w_all, y_out, y_in, y_mid, totals, pair_total,
    *blocks,
):
    g, c = lax.axis_index("grp"), lax.axis_index("clu")
    core = lax.rem(c, 2)
    tile, columns = forces.shape[1:]
    width = columns // groups
    quarter = tile // 4
    rows = comps * tile
    near_count = tiles.shape[0]
    far_count = targets.shape[1]
    half = n // 2
    cut = rank // 2
    piece_rows = levels * cut
    spans = [(level, 2 ** (level + 1)) for level in range(levels)]
    table_rows = sum(count - 1 for _, count in spans) * cut
    last = groups - 1
    own_blocks, far_blocks, side_blocks = (blocks[at * comps:(at + 1) * comps] for at in range(3))
    edge = 7 * core

    def at_clu(by):
        return {"grp": g, "clu": lax.rem(c + by + n, n)}

    partners = (g, g + 1 - 2 * lax.rem(g, 2), lax.rem(g + 2, groups), groups - 1 - g)

    def at_grp(i):
        return {"grp": partners[i], "clu": c}

    mate = {"grp": g, "clu": c + 1 - 2 * core}
    sends = []

    def remote(src, dst, recv, where, index=0):
        return pltpu.make_async_remote_copy(
            src_ref=src, dst_ref=dst, send_sem=send_sem.at[index], recv_sem=recv, device_id=where, device_id_type=MESH
        )

    def push(copies, bytes_of):
        assert len(sends) < SENDS
        for src, dst, recv, where in copies:
            remote(src, dst, recv, where, len(sends)).start()
        sends.append(remote(bytes_of, bytes_of, near_recv.at[0], mate, len(sends)))

    def landed(ref, recv):
        remote(ref, ref, recv, mate).wait_recv()

    def several(count):
        return own_blocks[0].at[0:count]

    def columns_of(i, d):
        return forces.at[d, :, pl.ds(pl.multiple_of(partners[i] * width, width), width)]

    def place_of(i, p, d, lo=0, hi=tile):
        if i == 0:
            return own_blocks[d].at[p, lo:hi]
        if i == last:
            return far_blocks[d].at[p, lo:hi]
        return side_blocks[d].at[p, lo:hi, pl.ds((i - 1) * width, width)]

    chunks = [(d, 0, tile) for d in range(comps - 1)]
    chunks += [(comps - 1, 0, tile // 2), (comps - 1, tile // 2, tile)]
    parts = range(len(chunks))

    def part(i, p, k):
        return place_of(i, p, *chunks[k])

    def part_bytes(k, count):
        return own_blocks[0].at[0:count, 0:chunks[k][2] - chunks[k][1]]

    def edge_rows(i, p, d):
        return place_of(i, p, d, 0, quarter)

    small = [
        pltpu.make_async_copy(src, dst, local_sem.at[at])
        for at, (src, dst) in enumerate((
            (order_hbm, order), (coupling_hbm, coupling), (targets_hbm, targets), (ranks_hbm, ranks),
            (scale_hbm, scale), (basis_hbm, basis), (bases_hbm, bases), (near_col_hbm, near_col), (tiles_hbm, tiles),
        ))
    ]
    for copy in small[:6]:
        copy.start()
    for i in (last, 0, 1, 2):
        for d in range(comps):
            pltpu.make_async_copy(columns_of(i, d), place_of(i, 3 + core, d), own_sem.at[i]).start()
    for copy in small[6:]:
        copy.start()

    barrier = pltpu.get_barrier_semaphore()

    def greet(d, carry):
        pl.semaphore_signal(barrier, inc=1, device_id=at_clu(d), device_id_type=MESH)
        return carry

    lax.fori_loop(1, n, greet, 0)
    for d in range(1, groups):
        pl.semaphore_signal(barrier, inc=1, device_id=at_grp(d), device_id_type=MESH)

    for block in blocks:
        block[edge, quarter:, :] = jnp.zeros((tile - quarter, block.shape[2]), BF16)
    ext_near[:, quarter:, :] = jnp.zeros((comps, ext_near.shape[1] - quarter, width), BF16)

    for copy in small[1:5]:
        copy.wait()
    lane = lax.broadcasted_iota(jnp.int32, (rank, 2 * table_rows), 1)
    row = lax.broadcasted_iota(jnp.int32, (rank, 2 * table_rows), 0)
    lane_row = (lane // table_rows) * cut + lax.rem(lane, cut)
    lane_slot = lax.rem(lane, table_rows) // cut
    repeat = (lane_row == row).astype(F32).astype(BF16)
    wide = jnp.dot(coupling[...], repeat, preferred_element_type=F32)
    for b in range(far_count):
        target = targets[0, b]
        slot_of, base, offset = target, 0, 0
        for level, count in spans:
            own = (c // 2) // (half // count)
            here = target - base - own - 1
            here = jnp.where(here < 0, here + count, here) + offset
            slot_of = jnp.where((target >= base) & (target < base + count), here, slot_of)
            base, offset = base + count, offset + count - 1
        keep = (lane_slot == slot_of) & (lane_row < ranks[0, b])
        scaled = jnp.where(keep, wide[b * rank:(b + 1) * rank, :] * scale[0, b], 0.0)
        high = scaled.astype(BF16)
        spread[b * rank:(b + 1) * rank, :2 * table_rows] = high
        spread[b * rank:(b + 1) * rank, 2 * table_rows:] = (scaled - high.astype(F32)).astype(BF16)
    small[5].wait()
    folded = lax.dot_general(basis[...], spread[...], (((0,), (0,)), ((), ())), preferred_element_type=F32)
    folded = folded[:, :2 * table_rows] + folded[:, 2 * table_rows:]
    w_out[...] = folded.reshape(groups, rows // groups, 2 * table_rows)

    sub = lax.broadcasted_iota(jnp.int32, (tile, tile), 0)
    lan = lax.broadcasted_iota(jnp.int32, (tile, tile), 1)
    upto = (sub <= lan).astype(BF16)

    def ranked(chosen):
        spots = jnp.broadcast_to(chosen.astype(F32), (8, tile)).astype(BF16)
        return (jnp.dot(spots, upto, preferred_element_type=F32)[0:1, :] - 1.0).astype(jnp.int32)

    def wrapped(spot):
        spot = jnp.where(spot < 0, spot + n * tile, spot)
        return jnp.where(spot >= n * tile, spot - n * tile, spot)

    def one_hot(spot, store, count):
        down = jnp.broadcast_to(spot.astype(F32), (128, tile)).T
        at = lax.broadcasted_iota(jnp.int32, (tile, 128), 1).astype(F32)
        for j in range(count):
            store(j, (down == at + float(j * 128)).astype(F32).astype(BF16))

    def own_arrived(i):
        pltpu.make_async_copy(several(comps), several(comps), own_sem.at[i]).wait()

    small[0].wait()
    own_arrived(last)
    pl.semaphore_wait(barrier, n - 1 + groups - 1)

    for by in (-1, 1, -2, 2):
        push([(order, orders.at[2 - by], order_recv.at[2 - by], at_clu(by))], order)

    def send_z(i, k):
        push(
            [
                (part(i, 3 + core, k), part(i, 1 + core, k), z_recv.at[i, k, 0], at_clu(2)),
                (part(i, 3 + core, k), part(i, 5 + core, k), z_recv.at[i, k, 1], at_clu(-2)),
            ],
            part_bytes(k, 2),
        )

    for k in range(2):
        send_z(last, k)
    push(
        [(w_out.at[partners[i]], w_in.at[i], w_recv.at[0, i], at_grp(i)) for i in range(1, groups)],
        w_out.at[0:groups - 1],
    )

    def send_mate(i):
        push(
            [(place_of(i, 3 + core, d), place_of(i, 3 + core, d), mate_recv.at[i], mate) for d in range(comps)],
            several(comps),
        )

    send_mate(last)
    own_arrived(0)
    send_mate(0)

    def order_landed(by):
        landed(orders.at[2 + by], order_recv.at[2 + by])

    spot = wrapped(order[...] - (c - core) * tile)
    beyond = spot >= 2 * tile
    spot = jnp.where(beyond, 2 * tile + ranked(beyond), spot)

    def store_own(j, value):
        own_pick[:, j * 128:(j + 1) * 128] = value

    one_hot(spot, store_own, own_pick.shape[1] // 128)

    for by in (-1, 1):
        order_landed(by)
    away = orders[1 + 2 * core] - c * tile
    chosen = (away >= 0) & (away < tile)
    place = jnp.where(chosen, ranked(chosen), -1)
    left = (lax.broadcasted_iota(jnp.int32, (128, tile), 0) == place).astype(F32).astype(BF16)
    right = (sub == away).astype(F32).astype(BF16)
    pick = lax.dot_general(left, right, (((1,), (1,)), ((), ())), preferred_element_type=F32).astype(BF16)

    def pick_edge(at, own):
        for d in range(comps):
            ext_out[at, d] = jnp.dot(pick, own[d][3 + core], preferred_element_type=F32).astype(BF16)[:quarter]

    for k in parts[2:]:
        send_z(last, k)
    pick_edge(1, far_blocks)
    push(
        [
            (ext_out.at[1, d], edge_rows(last, 7 - edge, d), ext_recv.at[last], at_clu(6 * core - 3))
            for d in range(comps)
        ],
        ext_out.at[1],
    )
    pick_edge(0, own_blocks)
    for i in (1, 2):
        own_arrived(i)
        send_mate(i)

    for by in (-2, 2):
        order_landed(by)
    orders[2] = order[...]
    small[7].wait()
    starts = []
    for j in range(near_count):
        spot0 = near_col[0, j] - c + 2
        spot0 = jnp.where(spot0 < 0, spot0 + n, spot0)
        spot0 = jnp.clip(jnp.where(spot0 >= n, spot0 - n, spot0), 0, 4)
        starts.append(spot0 + core)
        spot = wrapped(orders[spot0] - (c + spot0 - 3) * tile)
        low = 2 * core * tile
        beyond = (spot >= low) & (spot < low + tile) & (spot0 == 4 * core)
        spot = jnp.where(beyond, low + ranked(beyond), spot)

        def store_pick(at, value, j=j):
            picks[j, :, at * 128:(at + 1) * 128] = value

        one_hot(spot, store_pick, picks.shape[2] // 128)

    def relay(i, k):
        copies = []
        for side, p in enumerate((1 + core, 5 + core)):
            landed(part(i, p, k), z_recv.at[i, k, side])
            if i == last:
                for to, at in ((1, 2), (2, 1)):
                    copies.append((part(i, p, k), part(at, p, k), z_recv.at[at, k, side], at_grp(to)))
            copies.append((part(i, p, k), part(i, p, k), across_recv.at[i, k], mate))
        push(copies, part_bytes(k, len(copies)))

    def take(i, *ks):
        for k in ks:
            landed(part_bytes(k, 2), across_recv.at[i, k])

    def near(block, lo, hi):
        acc = None
        for j in range(near_count):
            found = [
                jnp.dot(
                    picks[j], block[d][pl.ds(starts[j], 3)].reshape(3 * tile, block[d].shape[2]),
                    preferred_element_type=F32,
                ).astype(BF16)
                for d in range(lo, hi)
            ]
            term = jnp.dot(
                tiles[j, :, lo * tile:hi * tile], jnp.concatenate(found, axis=0), preferred_element_type=F32
            )
            acc = term if acc is None else acc + term
        return acc

    mid = rows // 2

    relay(last, 0)
    relay(last, 1)
    push([(ext_out.at[0], ext_near.at[:, 0:quarter], near_recv.at[0], at_clu(2 * core - 1))], ext_out.at[0])
    for i in range(1, groups):
        landed(w_in.at[i], w_recv.at[0, i])
    summed = w_out[g]
    for i in range(1, groups):
        summed = summed + w_in[i]
    high = summed.astype(BF16)
    w_own[...] = high
    w_all[g] = high
    w_low[...] = (summed - high.astype(F32)).astype(BF16)
    relay(last, 2)
    relay(last, 3)
    for k in parts[:2]:
        send_z(0, k)
    for i in (1, 2):
        relay(i, 0)
    landed(ext_out.at[1], ext_recv.at[last])
    push(
        [
            (edge_rows(last, edge, d), edge_rows(at, edge, d), ext_recv.at[at], at_grp(to))
            for to, at in ((1, 2), (2, 1)) for d in range(comps)
        ],
        ext_out,
    )
    landed(several(comps), mate_recv.at[last])
    small[8].wait()
    take(last, 0, 1, 2, 3)
    y_out[last] = near(far_blocks, 0, comps).astype(BF16)
    push(
        [
            (y_out.at[last, 0:mid], y_mid.at[0], mid_recv.at[0], at_grp(1)),
            (y_out.at[last, mid:rows], y_mid.at[1], mid_recv.at[1], at_grp(2)),
        ],
        y_out.at[last],
    )
    push([(w_own, w_all.at[g], w_recv.at[1, i], at_grp(i)) for i in range(1, groups)], w_all.at[0:groups - 1])

    for k in (1, 2):
        for i in (1, 2):
            relay(i, k)
    small[6].wait()
    landed(ext_out.at[0], near_recv.at[0])
    push(
        [
            (ext_near.at[d, 0:quarter], edge_rows(0, edge, d), ext_recv.at[0], at_clu(2 - 4 * core))
            for d in range(comps)
        ],
        ext_out.at[0],
    )
    landed(several(comps), mate_recv.at[0])
    piece = jnp.zeros((2 * piece_rows, width), F32)
    for d in range(comps):
        x = jnp.dot(own_pick[:, :2 * tile], own_blocks[d][3:5].reshape(2 * tile, width), preferred_element_type=F32)
        x = x + jnp.dot(own_pick[:, 2 * tile:], ext_near[d], preferred_element_type=F32)
        weights = jnp.concatenate(
            [bases[level, d, h * cut:(h + 1) * cut] for h in range(2) for level in range(levels)], axis=0
        )
        piece = piece + jnp.dot(weights, x.astype(BF16), preferred_element_type=F32)
    for h in range(2):
        piece_out[h] = piece[h * piece_rows:(h + 1) * piece_rows]
    push([(piece_out.at[1 - core], piece_mate, pair_recv.at[0], mate)], piece_mate)
    for i in (1, 2):
        relay(i, 3)

    landed(piece_mate, pair_recv.at[0])
    pair = piece_out[core] + piece_mate[...]
    piece_out[2] = pair
    pieces[c // 2] = pair

    def piece_copy(d):
        return pltpu.make_async_remote_copy(
            src_ref=piece_out.at[2], dst_ref=pieces.at[c // 2], send_sem=piece_send.at[d],
            recv_sem=piece_recv.at[c // 2], device_id=at_clu(2 * d), device_id_type=MESH,
        )

    def start_piece(d, carry):
        piece_copy(d).start()
        return carry

    lax.fori_loop(1, half, start_piece, 0)
    for k in parts[2:]:
        send_z(0, k)

    for i in (1, 2):
        landed(several(comps), mate_recv.at[i])
        landed(ext_out.at[0], ext_recv.at[i])
        take(i, 0, 1, 2, 3)
    both = near(side_blocks, 0, comps)

    def send_y(i, h, value):
        here = pl.ds(h * mid, mid)
        y_out[i, h * mid:(h + 1) * mid] = value.astype(BF16)
        push([(y_out.at[i, here], y_in.at[i, here], y_recv.at[i, h], at_grp(i))], y_mid.at[0])

    def half_of(i, h):
        return both[h * mid:(h + 1) * mid, (i - 1) * width:i * width]

    send_y(1, 0, half_of(1, 0))
    send_y(2, 1, half_of(2, 1))
    landed(y_mid.at[1], mid_recv.at[1])
    send_y(1, 1, half_of(1, 1) + y_mid[1].astype(F32))
    landed(y_mid.at[0], mid_recv.at[0])
    send_y(2, 0, half_of(2, 0) + y_mid[0].astype(F32))
    relay(0, 0)
    relay(0, 1)

    landed(ext_out.at[0], ext_recv.at[0])
    take(0, 0)
    totals[...] = near(own_blocks, 0, 1)

    def await_piece(d, carry):
        source = lax.rem(c // 2 + d, half)
        landed(pieces.at[source], piece_recv.at[source])
        return carry

    lax.fori_loop(1, half, await_piece, 0)
    at = 0
    for level, count in spans:
        members = half // count
        own = (c // 2) // members
        for step in range(count - 1):
            k = lax.rem(own + 1 + step, count)
            entry = lax.fori_loop(
                0, members,
                lambda m, acc, k=k, members=members, level=level: acc
                + pieces[k * members + m, level * cut:(level + 1) * cut, :],
                jnp.zeros((cut, width), F32),
            )
            table[core, at:at + cut, :] = entry
            at += cut
    push([(table.at[core], table.at[core], table_recv.at[0], mate)], table.at[0])

    take(0, 1)
    totals[...] += near(own_blocks, 1, 2)
    relay(0, 2)
    for i in range(1, groups):
        landed(w_own, w_recv.at[1, i])
    landed(table.at[0], table_recv.at[0])
    entries = table[...].reshape(2 * table_rows, width)
    high = entries.astype(BF16)
    low = (entries - high.astype(F32)).astype(BF16)
    weights = w_all[...].reshape(rows, 2 * table_rows)
    answer = jnp.dot(weights, high, preferred_element_type=F32) + jnp.dot(weights, low, preferred_element_type=F32)
    totals[...] += answer
    own_rows = pl.ds(pl.multiple_of(g * (rows // groups), rows // groups), rows // groups)
    totals[own_rows] += jnp.dot(w_low[...], high, preferred_element_type=F32)
    relay(0, 3)
    take(0, 2, 3)
    totals[...] += near(own_blocks, comps - 1, comps)

    for copy in sends:
        copy.wait_send()

    def end_piece(d, carry):
        piece_copy(d).wait_send()
        return carry

    lax.fori_loop(1, half, end_piece, 0)
    for i in (1, 2):
        for h in range(2):
            landed(y_mid.at[0], y_recv.at[i, h])
    out[...] = (totals[...] + y_in[1].astype(F32) + y_in[2].astype(F32)).reshape(comps, tile, width)


def solution(mesh):
    n, groups = mesh.shape["clu"], mesh.shape["grp"]

    def on_device(forces, order, bases, near_tiles, near_col, far_basis, far_coupling, far_scale, far_rank, far_target):
        comps, tile, columns = forces.shape
        levels, rank = bases.shape[:2]
        near_count, far_count = near_tiles.shape[1], far_basis.shape[1]
        width, rows, quarter = columns // groups, comps * tile, tile // 4
        cut = rank // 2
        piece_rows = levels * cut
        table_rows = sum(2 ** (level + 1) - 1 for level in range(levels)) * cut
        slots = 8
        pad = 128
        vmem, hbm = (pl.BlockSpec(memory_space=m) for m in (pltpu.VMEM, pl.ANY))
        operands = (
            forces,
            order.reshape(1, tile),
            jnp.transpose(bases, (0, 2, 1, 3)),
            near_tiles.reshape(near_count, rows, rows),
            near_col,
            far_basis.reshape(far_count * rank, rows),
            far_coupling.reshape(far_count * rank, rank),
            far_scale,
            far_rank,
            far_target,
        )
        return pl.pallas_call(
            functools.partial(kernel, n, groups, levels, rank, comps),
            out_shape=jax.ShapeDtypeStruct((comps, tile, width), F32),
            in_specs=[hbm] * len(operands),
            out_specs=vmem,
            scratch_shapes=[
                pltpu.VMEM((1, tile), jnp.int32),
                pltpu.VMEM((levels, comps, rank, tile), BF16),
                pltpu.VMEM((far_count * rank, rank), BF16),
                pltpu.SMEM((1, near_count), jnp.int32),
                pltpu.SMEM((1, far_count), F32),
                pltpu.SMEM((1, far_count), jnp.int32),
                pltpu.SMEM((1, far_count), jnp.int32),
                pltpu.VMEM((near_count, rows, rows), BF16),
                pltpu.VMEM((far_count * rank, rows), BF16),
                pltpu.VMEM((2, comps, quarter, width), BF16),
                pltpu.VMEM((comps, pad, width), BF16),
                pltpu.VMEM((5, 1, tile), jnp.int32),
                pltpu.VMEM((far_count * rank, 4 * table_rows), BF16),
                pltpu.VMEM((near_count, tile, 3 * tile), BF16),
                pltpu.VMEM((tile, 2 * tile + pad), BF16),
                pltpu.VMEM((3, piece_rows, width), F32),
                pltpu.VMEM((piece_rows, width), F32),
                pltpu.VMEM((n // 2, piece_rows, width), F32),
                pltpu.VMEM((2, table_rows, width), F32),
                pltpu.VMEM((groups, rows // groups, 2 * table_rows), F32),
                pltpu.VMEM((groups, rows // groups, 2 * table_rows), F32),
                pltpu.VMEM((rows // groups, 2 * table_rows), BF16),
                pltpu.VMEM((rows // groups, 2 * table_rows), BF16),
                pltpu.VMEM((groups, rows // groups, 2 * table_rows), BF16),
                pltpu.VMEM((groups, rows, width), BF16),
                pltpu.VMEM((groups, rows, width), BF16),
                pltpu.VMEM((2, rows // 2, width), BF16),
                pltpu.VMEM((rows, width), F32),
                pltpu.VMEM((rows, 2 * width), F32),
                *(pltpu.VMEM((slots, tile, size), BF16) for size in (width, width, 2 * width) for _ in range(comps)),
            ],
            compiler_params=pltpu.CompilerParams(
                collective_id=0, has_side_effects=True, vmem_limit_bytes=28 * 1024 * 1024
            ),
        )(*(pltpu.with_memory_space_constraint(operand, pltpu.HBM) for operand in operands))

    placed = (
        P(None, "clu", None),
        P("clu"),
        P(None, None, None, "clu"),
        P("clu", "grp", None, None),
        P("clu", "grp"),
        P("clu", "grp", None, None),
        P("clu", "grp", None, None),
        P("clu", "grp"),
        P("clu", "grp"),
        P("clu", "grp"),
    )
    return jax.shard_map(
        on_device, mesh=mesh, in_specs=placed, out_specs=P(None, "clu", "grp"), check_vma=False
    )
```

```python
import functools

import jax
import jax.numpy as jnp
from jax import lax
from jax.experimental import pallas as pl
from jax.experimental.pallas import tpu as pltpu
from jax.sharding import PartitionSpec as P

MESH = pl.DeviceIdType.MESH
F32, BF16 = jnp.float32, jnp.bfloat16
SENDS = 48


def kernel(n, groups, levels, rank, comps, *refs):
    dma = pltpu.SemaphoreType.DMA

    def scoped(*sems):
        body(n, groups, levels, rank, comps, *sems, *refs)

    pl.run_scoped(
        scoped,
        dma((9,)), dma((groups,)), dma((SENDS,)), dma((n // 2,)),
        dma((5,)), dma((groups,)), dma((groups, comps + 1, 2)), dma((groups, comps + 1)), dma((groups,)), dma((1,)),
        dma((1,)), dma((n // 2,)), dma((1,)), dma((2, groups)), dma((groups, 2)), dma((2,)),
    )


def body(
    n, groups, levels, rank, comps,
    local_sem, own_sem, send_sem, piece_send, order_recv, mate_recv, z_recv, across_recv, ext_recv, near_recv,
    pair_recv, piece_recv, table_recv, w_recv, y_recv, mid_recv,
    forces, order_hbm, bases_hbm, tiles_hbm, near_col_hbm, basis_hbm, coupling_hbm, scale_hbm, ranks_hbm, targets_hbm,
    out,
    order, bases, coupling, near_col, scale, ranks, targets, tiles, basis,
    ext_out, ext_near, orders, spread, picks, own_pick, piece_out, piece_mate, pieces,
    table, w_out, w_in, w_own, w_low, w_all, y_out, y_in, y_mid, totals, pair_total,
    *blocks,
):
    g, c = lax.axis_index("grp"), lax.axis_index("clu")
    core = lax.rem(c, 2)
    tile, columns = forces.shape[1:]
    width = columns // groups
    quarter = tile // 4
    rows = comps * tile
    near_count = tiles.shape[0]
    far_count = targets.shape[1]
    half = n // 2
    cut = rank // 2
    piece_rows = levels * cut
    spans = [(level, 2 ** (level + 1)) for level in range(levels)]
    table_rows = sum(count - 1 for _, count in spans) * cut
    last = groups - 1
    own_blocks, far_blocks, side_blocks = (blocks[at * comps:(at + 1) * comps] for at in range(3))
    edge = 7 * core

    def at_clu(by):
        return {"grp": g, "clu": lax.rem(c + by + n, n)}

    partners = (g, g + 1 - 2 * lax.rem(g, 2), lax.rem(g + 2, groups), groups - 1 - g)

    def at_grp(i):
        return {"grp": partners[i], "clu": c}

    mate = {"grp": g, "clu": c + 1 - 2 * core}
    sends = []

    def remote(src, dst, recv, where, index=0):
        return pltpu.make_async_remote_copy(
            src_ref=src, dst_ref=dst, send_sem=send_sem.at[index], recv_sem=recv, device_id=where, device_id_type=MESH
        )

    def push(copies, bytes_of):
        assert len(sends) < SENDS
        for src, dst, recv, where in copies:
            remote(src, dst, recv, where, len(sends)).start()
        sends.append(remote(bytes_of, bytes_of, near_recv.at[0], mate, len(sends)))

    def landed(ref, recv):
        remote(ref, ref, recv, mate).wait_recv()

    def several(count):
        return own_blocks[0].at[0:count]

    def columns_of(i, d):
        return forces.at[d, :, pl.ds(pl.multiple_of(partners[i] * width, width), width)]

    def place_of(i, p, d, lo=0, hi=tile):
        if i == 0:
            return own_blocks[d].at[p, lo:hi]
        if i == last:
            return far_blocks[d].at[p, lo:hi]
        return side_blocks[d].at[p, lo:hi, pl.ds((i - 1) * width, width)]

    chunks = [(d, 0, tile) for d in range(comps - 1)]
    chunks += [(comps - 1, 0, tile // 2), (comps - 1, tile // 2, tile)]
    parts = range(len(chunks))

    def part(i, p, k):
        return place_of(i, p, *chunks[k])

    def part_bytes(k, count):
        return own_blocks[0].at[0:count, 0:chunks[k][2] - chunks[k][1]]

    def edge_rows(i, p, d):
        return place_of(i, p, d, 0, quarter)

    small = [
        pltpu.make_async_copy(src, dst, local_sem.at[at])
        for at, (src, dst) in enumerate((
            (order_hbm, order), (coupling_hbm, coupling), (targets_hbm, targets), (ranks_hbm, ranks),
            (scale_hbm, scale), (basis_hbm, basis), (bases_hbm, bases), (near_col_hbm, near_col), (tiles_hbm, tiles),
        ))
    ]
    for copy in small[:6]:
        copy.start()
    for i in (last, 0, 1, 2):
        for d in range(comps):
            pltpu.make_async_copy(columns_of(i, d), place_of(i, 3 + core, d), own_sem.at[i]).start()
    for copy in small[6:]:
        copy.start()

    barrier = pltpu.get_barrier_semaphore()

    def greet(d, carry):
        pl.semaphore_signal(barrier, inc=1, device_id=at_clu(d), device_id_type=MESH)
        return carry

    lax.fori_loop(1, n, greet, 0)
    for d in range(1, groups):
        pl.semaphore_signal(barrier, inc=1, device_id=at_grp(d), device_id_type=MESH)

    for block in blocks:
        block[edge, quarter:, :] = jnp.zeros((tile - quarter, block.shape[2]), BF16)
    ext_near[:, quarter:, :] = jnp.zeros((comps, ext_near.shape[1] - quarter, width), BF16)

    for copy in small[1:5]:
        copy.wait()
    lane = lax.broadcasted_iota(jnp.int32, (rank, 2 * table_rows), 1)
    row = lax.broadcasted_iota(jnp.int32, (rank, 2 * table_rows), 0)
    lane_row = (lane // table_rows) * cut + lax.rem(lane, cut)
    lane_slot = lax.rem(lane, table_rows) // cut
    repeat = (lane_row == row).astype(F32).astype(BF16)
    wide = jnp.dot(coupling[...], repeat, preferred_element_type=F32)
    for b in range(far_count):
        target = targets[0, b]
        slot_of, base, offset = target, 0, 0
        for level, count in spans:
            own = (c // 2) // (half // count)
            here = target - base - own - 1
            here = jnp.where(here < 0, here + count, here) + offset
            slot_of = jnp.where((target >= base) & (target < base + count), here, slot_of)
            base, offset = base + count, offset + count - 1
        keep = (lane_slot == slot_of) & (lane_row < ranks[0, b])
        scaled = jnp.where(keep, wide[b * rank:(b + 1) * rank, :] * scale[0, b], 0.0)
        high = scaled.astype(BF16)
        spread[b * rank:(b + 1) * rank, :2 * table_rows] = high
        spread[b * rank:(b + 1) * rank, 2 * table_rows:] = (scaled - high.astype(F32)).astype(BF16)
    small[5].wait()
    folded = lax.dot_general(basis[...], spread[...], (((0,), (0,)), ((), ())), preferred_element_type=F32)
    folded = folded[:, :2 * table_rows] + folded[:, 2 * table_rows:]
    w_out[...] = folded.reshape(groups, rows // groups, 2 * table_rows)

    sub = lax.broadcasted_iota(jnp.int32, (tile, tile), 0)
    lan = lax.broadcasted_iota(jnp.int32, (tile, tile), 1)
    upto = (sub <= lan).astype(BF16)

    def ranked(chosen):
        spots = jnp.broadcast_to(chosen.astype(F32), (8, tile)).astype(BF16)
        return (jnp.dot(spots, upto, preferred_element_type=F32)[0:1, :] - 1.0).astype(jnp.int32)

    def wrapped(spot):
        spot = jnp.where(spot < 0, spot + n * tile, spot)
        return jnp.where(spot >= n * tile, spot - n * tile, spot)

    def one_hot(spot, store, count):
        down = jnp.broadcast_to(spot.astype(F32), (128, tile)).T
        at = lax.broadcasted_iota(jnp.int32, (tile, 128), 1).astype(F32)
        for j in range(count):
            store(j, (down == at + float(j * 128)).astype(F32).astype(BF16))

    def own_arrived(i):
        pltpu.make_async_copy(several(comps), several(comps), own_sem.at[i]).wait()

    small[0].wait()
    own_arrived(last)
    pl.semaphore_wait(barrier, n - 1 + groups - 1)

    for by in (-1, 1, -2, 2):
        push([(order, orders.at[2 - by], order_recv.at[2 - by], at_clu(by))], order)

    def send_z(i, k):
        push(
            [
                (part(i, 3 + core, k), part(i, 1 + core, k), z_recv.at[i, k, 0], at_clu(2)),
                (part(i, 3 + core, k), part(i, 5 + core, k), z_recv.at[i, k, 1], at_clu(-2)),
            ],
            part_bytes(k, 2),
        )

    for k in range(2):
        send_z(last, k)
    push(
        [(w_out.at[partners[i]], w_in.at[i], w_recv.at[0, i], at_grp(i)) for i in range(1, groups)],
        w_out.at[0:groups - 1],
    )

    def send_mate(i):
        push(
            [(place_of(i, 3 + core, d), place_of(i, 3 + core, d), mate_recv.at[i], mate) for d in range(comps)],
            several(comps),
        )

    send_mate(last)
    own_arrived(0)
    send_mate(0)

    def order_landed(by):
        landed(orders.at[2 + by], order_recv.at[2 + by])

    spot = wrapped(order[...] - (c - core) * tile)
    beyond = spot >= 2 * tile
    spot = jnp.where(beyond, 2 * tile + ranked(beyond), spot)

    def store_own(j, value):
        own_pick[:, j * 128:(j + 1) * 128] = value

    one_hot(spot, store_own, own_pick.shape[1] // 128)

    for by in (-1, 1):
        order_landed(by)
    away = orders[1 + 2 * core] - c * tile
    chosen = (away >= 0) & (away < tile)
    place = jnp.where(chosen, ranked(chosen), -1)
    left = (lax.broadcasted_iota(jnp.int32, (128, tile), 0) == place).astype(F32).astype(BF16)
    right = (sub == away).astype(F32).astype(BF16)
    pick = lax.dot_general(left, right, (((1,), (1,)), ((), ())), preferred_element_type=F32).astype(BF16)

    def pick_edge(at, own):
        for d in range(comps):
            ext_out[at, d] = jnp.dot(pick, own[d][3 + core], preferred_element_type=F32).astype(BF16)[:quarter]

    for k in parts[2:]:
        send_z(last, k)
    pick_edge(1, far_blocks)
    push(
        [
            (ext_out.at[1, d], edge_rows(last, 7 - edge, d), ext_recv.at[last], at_clu(6 * core - 3))
            for d in range(comps)
        ],
        ext_out.at[1],
    )
    pick_edge(0, own_blocks)
    for i in (1, 2):
        own_arrived(i)
        send_mate(i)

    for by in (-2, 2):
        order_landed(by)
    orders[2] = order[...]
    small[7].wait()
    starts = []
    for j in range(near_count):
        spot0 = near_col[0, j] - c + 2
        spot0 = jnp.where(spot0 < 0, spot0 + n, spot0)
        spot0 = jnp.clip(jnp.where(spot0 >= n, spot0 - n, spot0), 0, 4)
        starts.append(spot0 + core)
        spot = wrapped(orders[spot0] - (c + spot0 - 3) * tile)
        low = 2 * core * tile
        beyond = (spot >= low) & (spot < low + tile) & (spot0 == 4 * core)
        spot = jnp.where(beyond, low + ranked(beyond), spot)

        def store_pick(at, value, j=j):
            picks[j, :, at * 128:(at + 1) * 128] = value

        one_hot(spot, store_pick, picks.shape[2] // 128)

    def relay(i, k):
        copies = []
        for side, p in enumerate((1 + core, 5 + core)):
            landed(part(i, p, k), z_recv.at[i, k, side])
            if i == last:
                for to, at in ((1, 2), (2, 1)):
                    copies.append((part(i, p, k), part(at, p, k), z_recv.at[at, k, side], at_grp(to)))
            copies.append((part(i, p, k), part(i, p, k), across_recv.at[i, k], mate))
        push(copies, part_bytes(k, len(copies)))

    def take(i, *ks):
        for k in ks:
            landed(part_bytes(k, 2), across_recv.at[i, k])

    def gathered(block, lo, hi):
        found = []
        for j in range(near_count):
            parts_of = [
                jnp.dot(
                    picks[j], block[d][pl.ds(starts[j], 3)].reshape(3 * tile, block[d].shape[2]),
                    preferred_element_type=F32,
                ).astype(BF16)
                for d in range(lo, hi)
            ]
            found.append(jnp.concatenate(parts_of, axis=0))
        return found

    def product(found, lo, hi, top, bottom):
        acc = None
        for j in range(near_count):
            term = jnp.dot(tiles[j, top:bottom, lo * tile:hi * tile], found[j], preferred_element_type=F32)
            acc = term if acc is None else acc + term
        return acc

    def near(block, lo, hi):
        return product(gathered(block, lo, hi), lo, hi, 0, rows)

    mid = rows // 2

    relay(last, 0)
    relay(last, 1)
    push([(ext_out.at[0], ext_near.at[:, 0:quarter], near_recv.at[0], at_clu(2 * core - 1))], ext_out.at[0])
    for i in range(1, groups):
        landed(w_in.at[i], w_recv.at[0, i])
    summed = w_out[g]
    for i in range(1, groups):
        summed = summed + w_in[i]
    high = summed.astype(BF16)
    w_own[...] = high
    w_all[g] = high
    w_low[...] = (summed - high.astype(F32)).astype(BF16)
    relay(last, 2)
    relay(last, 3)
    for k in parts[:2]:
        send_z(0, k)
    for i in (1, 2):
        relay(i, 0)
    landed(ext_out.at[1], ext_recv.at[last])
    push(
        [
            (edge_rows(last, edge, d), edge_rows(at, edge, d), ext_recv.at[at], at_grp(to))
            for to, at in ((1, 2), (2, 1)) for d in range(comps)
        ],
        ext_out,
    )
    landed(several(comps), mate_recv.at[last])
    small[8].wait()
    take(last, 0, 1, 2, 3)
    y_out[last] = near(far_blocks, 0, comps).astype(BF16)
    push(
        [
            (y_out.at[last, 0:mid], y_mid.at[0], mid_recv.at[0], at_grp(1)),
            (y_out.at[last, mid:rows], y_mid.at[1], mid_recv.at[1], at_grp(2)),
        ],
        y_out.at[last],
    )
    push([(w_own, w_all.at[g], w_recv.at[1, i], at_grp(i)) for i in range(1, groups)], w_all.at[0:groups - 1])

    for k in (1, 2):
        for i in (1, 2):
            relay(i, k)
    small[6].wait()
    landed(ext_out.at[0], near_recv.at[0])
    push(
        [
            (ext_near.at[d, 0:quarter], edge_rows(0, edge, d), ext_recv.at[0], at_clu(2 - 4 * core))
            for d in range(comps)
        ],
        ext_out.at[0],
    )
    landed(several(comps), mate_recv.at[0])
    piece = jnp.zeros((2 * piece_rows, width), F32)
    for d in range(comps):
        x = jnp.dot(own_pick[:, :2 * tile], own_blocks[d][3:5].reshape(2 * tile, width), preferred_element_type=F32)
        x = x + jnp.dot(own_pick[:, 2 * tile:], ext_near[d], preferred_element_type=F32)
        weights = jnp.concatenate(
            [bases[level, d, h * cut:(h + 1) * cut] for h in range(2) for level in range(levels)], axis=0
        )
        piece = piece + jnp.dot(weights, x.astype(BF16), preferred_element_type=F32)
    for h in range(2):
        piece_out[h] = piece[h * piece_rows:(h + 1) * piece_rows]
    push([(piece_out.at[1 - core], piece_mate, pair_recv.at[0], mate)], piece_mate)
    for i in (1, 2):
        relay(i, 3)

    landed(piece_mate, pair_recv.at[0])
    pair = piece_out[core] + piece_mate[...]
    piece_out[2] = pair
    pieces[c // 2] = pair

    def piece_copy(d):
        return pltpu.make_async_remote_copy(
            src_ref=piece_out.at[2], dst_ref=pieces.at[c // 2], send_sem=piece_send.at[d],
            recv_sem=piece_recv.at[c // 2], device_id=at_clu(2 * d), device_id_type=MESH,
        )

    def start_piece(d, carry):
        piece_copy(d).start()
        return carry

    lax.fori_loop(1, half, start_piece, 0)
    for k in parts[2:]:
        send_z(0, k)

    for i in (1, 2):
        landed(several(comps), mate_recv.at[i])
        landed(ext_out.at[0], ext_recv.at[i])
        take(i, 0, 1, 2, 3)
    found = gathered(side_blocks, 0, comps)

    def send_y(i, h, value):
        here = pl.ds(h * mid, mid)
        y_out[i, h * mid:(h + 1) * mid] = value.astype(BF16)
        push([(y_out.at[i, here], y_in.at[i, here], y_recv.at[i, h], at_grp(i))], y_mid.at[0])

    for h, plain, added in ((0, 1, 2), (1, 2, 1)):
        both = product(found, 0, comps, h * mid, (h + 1) * mid)
        send_y(plain, h, both[:, (plain - 1) * width:plain * width])
        landed(y_mid.at[h], mid_recv.at[h])
        send_y(added, h, both[:, (added - 1) * width:added * width] + y_mid[h].astype(F32))
    relay(0, 0)
    relay(0, 1)

    landed(ext_out.at[0], ext_recv.at[0])
    take(0, 0)
    totals[...] = near(own_blocks, 0, 1)

    def await_piece(d, carry):
        source = lax.rem(c // 2 + d, half)
        landed(pieces.at[source], piece_recv.at[source])
        return carry

    lax.fori_loop(1, half, await_piece, 0)
    at = 0
    for level, count in spans:
        members = half // count
        own = (c // 2) // members
        for step in range(count - 1):
            k = lax.rem(own + 1 + step, count)
            entry = lax.fori_loop(
                0, members,
                lambda m, acc, k=k, members=members, level=level: acc
                + pieces[k * members + m, level * cut:(level + 1) * cut, :],
                jnp.zeros((cut, width), F32),
            )
            table[core, at:at + cut, :] = entry
            at += cut
    push([(table.at[core], table.at[core], table_recv.at[0], mate)], table.at[0])

    take(0, 1)
    totals[...] += near(own_blocks, 1, 2)
    relay(0, 2)
    for i in range(1, groups):
        landed(w_own, w_recv.at[1, i])
    landed(table.at[0], table_recv.at[0])
    entries = table[...].reshape(2 * table_rows, width)
    high = entries.astype(BF16)
    low = (entries - high.astype(F32)).astype(BF16)
    weights = w_all[...].reshape(rows, 2 * table_rows)
    answer = jnp.dot(weights, high, preferred_element_type=F32) + jnp.dot(weights, low, preferred_element_type=F32)
    totals[...] += answer
    own_rows = pl.ds(pl.multiple_of(g * (rows // groups), rows // groups), rows // groups)
    totals[own_rows] += jnp.dot(w_low[...], high, preferred_element_type=F32)
    relay(0, 3)
    take(0, 2, 3)
    totals[...] += near(own_blocks, comps - 1, comps)

    for copy in sends:
        copy.wait_send()

    def end_piece(d, carry):
        piece_copy(d).wait_send()
        return carry

    lax.fori_loop(1, half, end_piece, 0)
    for i in (1, 2):
        for h in range(2):
            landed(y_mid.at[0], y_recv.at[i, h])
    out[...] = (totals[...] + y_in[1].astype(F32) + y_in[2].astype(F32)).reshape(comps, tile, width)


def solution(mesh):
    n, groups = mesh.shape["clu"], mesh.shape["grp"]

    def on_device(forces, order, bases, near_tiles, near_col, far_basis, far_coupling, far_scale, far_rank, far_target):
        comps, tile, columns = forces.shape
        levels, rank = bases.shape[:2]
        near_count, far_count = near_tiles.shape[1], far_basis.shape[1]
        width, rows, quarter = columns // groups, comps * tile, tile // 4
        cut = rank // 2
        piece_rows = levels * cut
        table_rows = sum(2 ** (level + 1) - 1 for level in range(levels)) * cut
        slots = 8
        pad = 128
        vmem, hbm = (pl.BlockSpec(memory_space=m) for m in (pltpu.VMEM, pl.ANY))
        operands = (
            forces,
            order.reshape(1, tile),
            jnp.transpose(bases, (0, 2, 1, 3)),
            near_tiles.reshape(near_count, rows, rows),
            near_col,
            far_basis.reshape(far_count * rank, rows),
            far_coupling.reshape(far_count * rank, rank),
            far_scale,
            far_rank,
            far_target,
        )
        return pl.pallas_call(
            functools.partial(kernel, n, groups, levels, rank, comps),
            out_shape=jax.ShapeDtypeStruct((comps, tile, width), F32),
            in_specs=[hbm] * len(operands),
            out_specs=vmem,
            scratch_shapes=[
                pltpu.VMEM((1, tile), jnp.int32),
                pltpu.VMEM((levels, comps, rank, tile), BF16),
                pltpu.VMEM((far_count * rank, rank), BF16),
                pltpu.SMEM((1, near_count), jnp.int32),
                pltpu.SMEM((1, far_count), F32),
                pltpu.SMEM((1, far_count), jnp.int32),
                pltpu.SMEM((1, far_count), jnp.int32),
                pltpu.VMEM((near_count, rows, rows), BF16),
                pltpu.VMEM((far_count * rank, rows), BF16),
                pltpu.VMEM((2, comps, quarter, width), BF16),
                pltpu.VMEM((comps, pad, width), BF16),
                pltpu.VMEM((5, 1, tile), jnp.int32),
                pltpu.VMEM((far_count * rank, 4 * table_rows), BF16),
                pltpu.VMEM((near_count, tile, 3 * tile), BF16),
                pltpu.VMEM((tile, 2 * tile + pad), BF16),
                pltpu.VMEM((3, piece_rows, width), F32),
                pltpu.VMEM((piece_rows, width), F32),
                pltpu.VMEM((n // 2, piece_rows, width), F32),
                pltpu.VMEM((2, table_rows, width), F32),
                pltpu.VMEM((groups, rows // groups, 2 * table_rows), F32),
                pltpu.VMEM((groups, rows // groups, 2 * table_rows), F32),
                pltpu.VMEM((rows // groups, 2 * table_rows), BF16),
                pltpu.VMEM((rows // groups, 2 * table_rows), BF16),
                pltpu.VMEM((groups, rows // groups, 2 * table_rows), BF16),
                pltpu.VMEM((groups, rows, width), BF16),
                pltpu.VMEM((groups, rows, width), BF16),
                pltpu.VMEM((2, rows // 2, width), BF16),
                pltpu.VMEM((rows, width), F32),
                pltpu.VMEM((rows, 2 * width), F32),
                *(pltpu.VMEM((slots, tile, size), BF16) for size in (width, width, 2 * width) for _ in range(comps)),
            ],
            compiler_params=pltpu.CompilerParams(
                collective_id=0, has_side_effects=True, vmem_limit_bytes=28 * 1024 * 1024
            ),
        )(*(pltpu.with_memory_space_constraint(operand, pltpu.HBM) for operand in operands))

    placed = (
        P(None, "clu", None),
        P("clu"),
        P(None, None, None, "clu"),
        P("clu", "grp", None, None),
        P("clu", "grp"),
        P("clu", "grp", None, None),
        P("clu", "grp", None, None),
        P("clu", "grp"),
        P("clu", "grp"),
        P("clu", "grp"),
    )
    return jax.shard_map(
        on_device, mesh=mesh, in_specs=placed, out_specs=P(None, "clu", "grp"), check_vma=False
    )
```

```python
import functools

import jax
import jax.numpy as jnp
from jax import lax
from jax.experimental import pallas as pl
from jax.experimental.pallas import tpu as pltpu
from jax.sharding import PartitionSpec as P

MESH = pl.DeviceIdType.MESH
F32, BF16 = jnp.float32, jnp.bfloat16
SENDS = 48


def kernel(n, groups, levels, rank, comps, *refs):
    dma = pltpu.SemaphoreType.DMA

    def scoped(*sems):
        body(n, groups, levels, rank, comps, *sems, *refs)

    pl.run_scoped(
        scoped,
        dma((9,)), dma((groups,)), dma((SENDS,)), dma((n // 2,)),
        dma((5,)), dma((groups,)), dma((groups, comps + 1, 2)), dma((groups, comps + 1)), dma((groups,)), dma((1,)),
        dma((1,)), dma((n // 2,)), dma((1,)), dma((2, groups)), dma((groups, 2)), dma((2,)),
    )


def body(
    n, groups, levels, rank, comps,
    local_sem, own_sem, send_sem, piece_send, order_recv, mate_recv, z_recv, across_recv, ext_recv, near_recv,
    pair_recv, piece_recv, table_recv, w_recv, y_recv, mid_recv,
    forces, order_hbm, bases_hbm, tiles_hbm, near_col_hbm, basis_hbm, coupling_hbm, scale_hbm, ranks_hbm, targets_hbm,
    out,
    order, bases, coupling, near_col, scale, ranks, targets, tiles, basis,
    ext_out, ext_near, orders, spread, picks, own_pick, piece_out, piece_mate, pieces,
    table, w_out, w_in, w_own, w_low, w_all, y_out, y_in, y_mid, totals, pair_total,
    *blocks,
):
    g, c = lax.axis_index("grp"), lax.axis_index("clu")
    core = lax.rem(c, 2)
    tile, columns = forces.shape[1:]
    width = columns // groups
    quarter = tile // 4
    rows = comps * tile
    near_count = tiles.shape[0]
    far_count = targets.shape[1]
    half = n // 2
    cut = rank // 2
    piece_rows = levels * cut
    spans = [(level, 2 ** (level + 1)) for level in range(levels)]
    table_rows = sum(count - 1 for _, count in spans) * cut
    last = groups - 1
    own_blocks, far_blocks, side_blocks = (blocks[at * comps:(at + 1) * comps] for at in range(3))
    edge = 7 * core
    flip = 1 - jnp.minimum(c // 2, 1)

    def at_clu(by):
        return {"grp": g, "clu": lax.rem(c + by + n, n)}

    partners = (g, g + 1 - 2 * lax.rem(g, 2), lax.rem(g + 2, groups), groups - 1 - g)

    def at_grp(i):
        return {"grp": partners[i], "clu": c}

    mate = {"grp": g, "clu": c + 1 - 2 * core}
    sends = []

    def remote(src, dst, recv, where, index=0):
        return pltpu.make_async_remote_copy(
            src_ref=src, dst_ref=dst, send_sem=send_sem.at[index], recv_sem=recv, device_id=where, device_id_type=MESH
        )

    def push(copies, bytes_of):
        assert len(sends) < SENDS
        for src, dst, recv, where in copies:
            remote(src, dst, recv, where, len(sends)).start()
        sends.append(remote(bytes_of, bytes_of, near_recv.at[0], mate, len(sends)))

    def landed(ref, recv):
        remote(ref, ref, recv, mate).wait_recv()

    def several(count):
        return own_blocks[0].at[0:count]

    def columns_of(i, d):
        return forces.at[d, :, pl.ds(pl.multiple_of(partners[i] * width, width), width)]

    def place_of(i, p, d, lo=0, hi=tile):
        if i == 0:
            return own_blocks[d].at[p, lo:hi]
        if i == last:
            return far_blocks[d].at[p, lo:hi]
        return side_blocks[d].at[p, lo:hi, pl.ds((i - 1) * width, width)]

    chunks = [(d, 0, tile) for d in range(comps - 1)]
    chunks += [(comps - 1, 0, tile // 2), (comps - 1, tile // 2, tile)]
    parts = range(len(chunks))

    def part(i, p, k):
        return place_of(i, p, *chunks[k])

    def part_bytes(k, count):
        return own_blocks[0].at[0:count, 0:chunks[k][2] - chunks[k][1]]

    def edge_rows(i, p, d):
        return place_of(i, p, d, 0, quarter)

    small = [
        pltpu.make_async_copy(src, dst, local_sem.at[at])
        for at, (src, dst) in enumerate((
            (order_hbm, order), (coupling_hbm, coupling), (targets_hbm, targets), (ranks_hbm, ranks),
            (scale_hbm, scale), (basis_hbm, basis), (bases_hbm, bases), (near_col_hbm, near_col), (tiles_hbm, tiles),
        ))
    ]
    for copy in small[:6]:
        copy.start()
    for i in (last, 0, 1, 2):
        for d in range(comps):
            pltpu.make_async_copy(columns_of(i, d), place_of(i, 3 + core, d), own_sem.at[i]).start()
    for copy in small[6:]:
        copy.start()

    barrier = pltpu.get_barrier_semaphore()

    def greet(d, carry):
        pl.semaphore_signal(barrier, inc=1, device_id=at_clu(d), device_id_type=MESH)
        return carry

    lax.fori_loop(1, n, greet, 0)
    for d in range(1, groups):
        pl.semaphore_signal(barrier, inc=1, device_id=at_grp(d), device_id_type=MESH)

    for block in blocks:
        block[edge, quarter:, :] = jnp.zeros((tile - quarter, block.shape[2]), BF16)
    ext_near[:, quarter:, :] = jnp.zeros((comps, ext_near.shape[1] - quarter, width), BF16)

    for copy in small[1:5]:
        copy.wait()
    lane = lax.broadcasted_iota(jnp.int32, (rank, 2 * table_rows), 1)
    row = lax.broadcasted_iota(jnp.int32, (rank, 2 * table_rows), 0)
    lane_row = (lane // table_rows) * cut + lax.rem(lane, cut)
    lane_slot = lax.rem(lane, table_rows) // cut
    repeat = (lane_row == row).astype(F32).astype(BF16)
    wide = jnp.dot(coupling[...], repeat, preferred_element_type=F32)
    for b in range(far_count):
        target = targets[0, b]
        slot_of, base, offset = target, 0, 0
        for level, count in spans:
            own = (c // 2) // (half // count)
            here = target - base - own - 1
            here = jnp.where(here < 0, here + count, here) + offset
            slot_of = jnp.where((target >= base) & (target < base + count), here, slot_of)
            base, offset = base + count, offset + count - 1
        keep = (lane_slot == slot_of) & (lane_row < ranks[0, b])
        scaled = jnp.where(keep, wide[b * rank:(b + 1) * rank, :] * scale[0, b], 0.0)
        high = scaled.astype(BF16)
        spread[b * rank:(b + 1) * rank, :2 * table_rows] = high
        spread[b * rank:(b + 1) * rank, 2 * table_rows:] = (scaled - high.astype(F32)).astype(BF16)
    small[5].wait()
    folded = lax.dot_general(basis[...], spread[...], (((0,), (0,)), ((), ())), preferred_element_type=F32)
    folded = folded[:, :2 * table_rows] + folded[:, 2 * table_rows:]
    w_out[...] = folded.reshape(groups, rows // groups, 2 * table_rows)

    sub = lax.broadcasted_iota(jnp.int32, (tile, tile), 0)
    lan = lax.broadcasted_iota(jnp.int32, (tile, tile), 1)
    upto = (sub <= lan).astype(BF16)

    def ranked(chosen):
        spots = jnp.broadcast_to(chosen.astype(F32), (8, tile)).astype(BF16)
        return (jnp.dot(spots, upto, preferred_element_type=F32)[0:1, :] - 1.0).astype(jnp.int32)

    def wrapped(spot):
        spot = jnp.where(spot < 0, spot + n * tile, spot)
        return jnp.where(spot >= n * tile, spot - n * tile, spot)

    def one_hot(spot, store, count):
        down = jnp.broadcast_to(spot.astype(F32), (128, tile)).T
        at = lax.broadcasted_iota(jnp.int32, (tile, 128), 1).astype(F32)
        for j in range(count):
            store(j, (down == at + float(j * 128)).astype(F32).astype(BF16))

    def own_arrived(i):
        pltpu.make_async_copy(several(comps), several(comps), own_sem.at[i]).wait()

    small[0].wait()
    own_arrived(last)
    pl.semaphore_wait(barrier, n - 1 + groups - 1)

    for by in (-1, 1, -2, 2):
        push([(order, orders.at[2 - by], order_recv.at[2 - by], at_clu(by))], order)

    def send_z(i, k):
        push(
            [
                (
                    part(i, 3 + core, k), part(i, 1 + core + 4 * side, k), z_recv.at[i, k, side],
                    at_clu(2 - 4 * side),
                )
                for side in (flip, 1 - flip)
            ],
            part_bytes(k, 2),
        )

    for k in range(2):
        send_z(last, k)
    push(
        [(w_out.at[partners[i]], w_in.at[i], w_recv.at[0, i], at_grp(i)) for i in range(1, groups)],
        w_out.at[0:groups - 1],
    )

    def send_mate(i):
        push(
            [(place_of(i, 3 + core, d), place_of(i, 3 + core, d), mate_recv.at[i], mate) for d in range(comps)],
            several(comps),
        )

    send_mate(last)
    own_arrived(0)
    send_mate(0)

    def order_landed(by):
        landed(orders.at[2 + by], order_recv.at[2 + by])

    spot = wrapped(order[...] - (c - core) * tile)
    beyond = spot >= 2 * tile
    spot = jnp.where(beyond, 2 * tile + ranked(beyond), spot)

    def store_own(j, value):
        own_pick[:, j * 128:(j + 1) * 128] = value

    one_hot(spot, store_own, own_pick.shape[1] // 128)

    for by in (-1, 1):
        order_landed(by)
    away = orders[1 + 2 * core] - c * tile
    chosen = (away >= 0) & (away < tile)
    place = jnp.where(chosen, ranked(chosen), -1)
    left = (lax.broadcasted_iota(jnp.int32, (128, tile), 0) == place).astype(F32).astype(BF16)
    right = (sub == away).astype(F32).astype(BF16)
    pick = lax.dot_general(left, right, (((1,), (1,)), ((), ())), preferred_element_type=F32).astype(BF16)

    def pick_edge(at, own):
        for d in range(comps):
            ext_out[at, d] = jnp.dot(pick, own[d][3 + core], preferred_element_type=F32).astype(BF16)[:quarter]

    for k in parts[2:]:
        send_z(last, k)
    pick_edge(1, far_blocks)
    push(
        [
            (ext_out.at[1, d], edge_rows(last, 7 - edge, d), ext_recv.at[last], at_clu(6 * core - 3))
            for d in range(comps)
        ],
        ext_out.at[1],
    )
    pick_edge(0, own_blocks)
    for i in (1, 2):
        own_arrived(i)
        send_mate(i)

    for by in (-2, 2):
        order_landed(by)
    orders[2] = order[...]
    small[7].wait()
    starts = []
    for j in range(near_count):
        spot0 = near_col[0, j] - c + 2
        spot0 = jnp.where(spot0 < 0, spot0 + n, spot0)
        spot0 = jnp.clip(jnp.where(spot0 >= n, spot0 - n, spot0), 0, 4)
        starts.append(spot0 + core)
        spot = wrapped(orders[spot0] - (c + spot0 - 3) * tile)
        low = 2 * core * tile
        beyond = (spot >= low) & (spot < low + tile) & (spot0 == 4 * core)
        spot = jnp.where(beyond, low + ranked(beyond), spot)

        def store_pick(at, value, j=j):
            picks[j, :, at * 128:(at + 1) * 128] = value

        one_hot(spot, store_pick, picks.shape[2] // 128)

    def relay(i, k):
        copies = []
        for side, p in enumerate((1 + core, 5 + core)):
            landed(part(i, p, k), z_recv.at[i, k, side])
            if i == last:
                for to, at in ((1, 2), (2, 1)):
                    copies.append((part(i, p, k), part(at, p, k), z_recv.at[at, k, side], at_grp(to)))
            copies.append((part(i, p, k), part(i, p, k), across_recv.at[i, k], mate))
        push(copies, part_bytes(k, len(copies)))

    def take(i, *ks):
        for k in ks:
            landed(part_bytes(k, 2), across_recv.at[i, k])

    def gathered(block, lo, hi):
        found = []
        for j in range(near_count):
            parts_of = [
                jnp.dot(
                    picks[j], block[d][pl.ds(starts[j], 3)].reshape(3 * tile, block[d].shape[2]),
                    preferred_element_type=F32,
                ).astype(BF16)
                for d in range(lo, hi)
            ]
            found.append(jnp.concatenate(parts_of, axis=0))
        return found

    def product(found, lo, hi, top, bottom):
        acc = None
        for j in range(near_count):
            term = jnp.dot(tiles[j, top:bottom, lo * tile:hi * tile], found[j], preferred_element_type=F32)
            acc = term if acc is None else acc + term
        return acc

    def near(block, lo, hi):
        return product(gathered(block, lo, hi), lo, hi, 0, rows)

    mid = rows // 2

    relay(last, 0)
    relay(last, 1)
    push([(ext_out.at[0], ext_near.at[:, 0:quarter], near_recv.at[0], at_clu(2 * core - 1))], ext_out.at[0])
    for i in range(1, groups):
        landed(w_in.at[i], w_recv.at[0, i])
    summed = w_out[g]
    for i in range(1, groups):
        summed = summed + w_in[i]
    high = summed.astype(BF16)
    w_own[...] = high
    w_all[g] = high
    w_low[...] = (summed - high.astype(F32)).astype(BF16)
    relay(last, 2)
    relay(last, 3)
    for k in parts[:2]:
        send_z(0, k)
    for i in (1, 2):
        relay(i, 0)
    landed(ext_out.at[1], ext_recv.at[last])
    push(
        [
            (edge_rows(last, edge, d), edge_rows(at, edge, d), ext_recv.at[at], at_grp(to))
            for to, at in ((1, 2), (2, 1)) for d in range(comps)
        ],
        ext_out,
    )
    landed(several(comps), mate_recv.at[last])
    small[8].wait()
    take(last, 0, 1, 2, 3)
    y_out[last] = near(far_blocks, 0, comps).astype(BF16)
    push(
        [
            (y_out.at[last, 0:mid], y_mid.at[0], mid_recv.at[0], at_grp(1)),
            (y_out.at[last, mid:rows], y_mid.at[1], mid_recv.at[1], at_grp(2)),
        ],
        y_out.at[last],
    )
    push([(w_own, w_all.at[g], w_recv.at[1, i], at_grp(i)) for i in range(1, groups)], w_all.at[0:groups - 1])

    for k in (1, 2):
        for i in (1, 2):
            relay(i, k)
    small[6].wait()
    landed(ext_out.at[0], near_recv.at[0])
    push(
        [
            (ext_near.at[d, 0:quarter], edge_rows(0, edge, d), ext_recv.at[0], at_clu(2 - 4 * core))
            for d in range(comps)
        ],
        ext_out.at[0],
    )
    landed(several(comps), mate_recv.at[0])
    piece = jnp.zeros((2 * piece_rows, width), F32)
    for d in range(comps):
        x = jnp.dot(own_pick[:, :2 * tile], own_blocks[d][3:5].reshape(2 * tile, width), preferred_element_type=F32)
        x = x + jnp.dot(own_pick[:, 2 * tile:], ext_near[d], preferred_element_type=F32)
        weights = jnp.concatenate(
            [bases[level, d, h * cut:(h + 1) * cut] for h in range(2) for level in range(levels)], axis=0
        )
        piece = piece + jnp.dot(weights, x.astype(BF16), preferred_element_type=F32)
    for h in range(2):
        piece_out[h] = piece[h * piece_rows:(h + 1) * piece_rows]
    push([(piece_out.at[1 - core], piece_mate, pair_recv.at[0], mate)], piece_mate)
    for i in (1, 2):
        relay(i, 3)

    landed(piece_mate, pair_recv.at[0])
    pair = piece_out[core] + piece_mate[...]
    piece_out[2] = pair
    pieces[c // 2] = pair

    def piece_copy(d):
        return pltpu.make_async_remote_copy(
            src_ref=piece_out.at[2], dst_ref=pieces.at[c // 2], send_sem=piece_send.at[d],
            recv_sem=piece_recv.at[c // 2], device_id=at_clu(2 * d), device_id_type=MESH,
        )

    def start_piece(d, carry):
        piece_copy(d).start()
        return carry

    lax.fori_loop(1, half, start_piece, 0)
    for k in parts[2:]:
        send_z(0, k)

    for i in (1, 2):
        landed(several(comps), mate_recv.at[i])
        landed(ext_out.at[0], ext_recv.at[i])
        take(i, 0, 1, 2, 3)
    found = gathered(side_blocks, 0, comps)

    def send_y(i, h, value):
        here = pl.ds(h * mid, mid)
        y_out[i, h * mid:(h + 1) * mid] = value.astype(BF16)
        push([(y_out.at[i, here], y_in.at[i, here], y_recv.at[i, h], at_grp(i))], y_mid.at[0])

    for h, plain, added in ((0, 1, 2), (1, 2, 1)):
        both = product(found, 0, comps, h * mid, (h + 1) * mid)
        send_y(plain, h, both[:, (plain - 1) * width:plain * width])
        landed(y_mid.at[h], mid_recv.at[h])
        send_y(added, h, both[:, (added - 1) * width:added * width] + y_mid[h].astype(F32))
    relay(0, 0)
    relay(0, 1)

    landed(ext_out.at[0], ext_recv.at[0])
    take(0, 0)
    totals[...] = near(own_blocks, 0, 1)

    def await_piece(d, carry):
        source = lax.rem(c // 2 + d, half)
        landed(pieces.at[source], piece_recv.at[source])
        return carry

    lax.fori_loop(1, half, await_piece, 0)
    at = 0
    for level, count in spans:
        members = half // count
        own = (c // 2) // members
        for step in range(count - 1):
            k = lax.rem(own + 1 + step, count)
            entry = lax.fori_loop(
                0, members,
                lambda m, acc, k=k, members=members, level=level: acc
                + pieces[k * members + m, level * cut:(level + 1) * cut, :],
                jnp.zeros((cut, width), F32),
            )
            table[core, at:at + cut, :] = entry
            at += cut
    push([(table.at[core], table.at[core], table_recv.at[0], mate)], table.at[0])

    take(0, 1)
    totals[...] += near(own_blocks, 1, 2)
    relay(0, 2)
    for i in range(1, groups):
        landed(w_own, w_recv.at[1, i])
    landed(table.at[0], table_recv.at[0])
    entries = table[...].reshape(2 * table_rows, width)
    high = entries.astype(BF16)
    low = (entries - high.astype(F32)).astype(BF16)
    weights = w_all[...].reshape(rows, 2 * table_rows)
    answer = jnp.dot(weights, high, preferred_element_type=F32) + jnp.dot(weights, low, preferred_element_type=F32)
    totals[...] += answer
    own_rows = pl.ds(pl.multiple_of(g * (rows // groups), rows // groups), rows // groups)
    totals[own_rows] += jnp.dot(w_low[...], high, preferred_element_type=F32)
    relay(0, 3)
    take(0, 2, 3)
    totals[...] += near(own_blocks, comps - 1, comps)

    for copy in sends:
        copy.wait_send()

    def end_piece(d, carry):
        piece_copy(d).wait_send()
        return carry

    lax.fori_loop(1, half, end_piece, 0)
    for i in (1, 2):
        for h in range(2):
            landed(y_mid.at[0], y_recv.at[i, h])
    out[...] = (totals[...] + y_in[1].astype(F32) + y_in[2].astype(F32)).reshape(comps, tile, width)


def solution(mesh):
    n, groups = mesh.shape["clu"], mesh.shape["grp"]

    def on_device(forces, order, bases, near_tiles, near_col, far_basis, far_coupling, far_scale, far_rank, far_target):
        comps, tile, columns = forces.shape
        levels, rank = bases.shape[:2]
        near_count, far_count = near_tiles.shape[1], far_basis.shape[1]
        width, rows, quarter = columns // groups, comps * tile, tile // 4
        cut = rank // 2
        piece_rows = levels * cut
        table_rows = sum(2 ** (level + 1) - 1 for level in range(levels)) * cut
        slots = 8
        pad = 128
        vmem, hbm = (pl.BlockSpec(memory_space=m) for m in (pltpu.VMEM, pl.ANY))
        operands = (
            forces,
            order.reshape(1, tile),
            jnp.transpose(bases, (0, 2, 1, 3)),
            near_tiles.reshape(near_count, rows, rows),
            near_col,
            far_basis.reshape(far_count * rank, rows),
            far_coupling.reshape(far_count * rank, rank),
            far_scale,
            far_rank,
            far_target,
        )
        return pl.pallas_call(
            functools.partial(kernel, n, groups, levels, rank, comps),
            out_shape=jax.ShapeDtypeStruct((comps, tile, width), F32),
            in_specs=[hbm] * len(operands),
            out_specs=vmem,
            scratch_shapes=[
                pltpu.VMEM((1, tile), jnp.int32),
                pltpu.VMEM((levels, comps, rank, tile), BF16),
                pltpu.VMEM((far_count * rank, rank), BF16),
                pltpu.SMEM((1, near_count), jnp.int32),
                pltpu.SMEM((1, far_count), F32),
                pltpu.SMEM((1, far_count), jnp.int32),
                pltpu.SMEM((1, far_count), jnp.int32),
                pltpu.VMEM((near_count, rows, rows), BF16),
                pltpu.VMEM((far_count * rank, rows), BF16),
                pltpu.VMEM((2, comps, quarter, width), BF16),
                pltpu.VMEM((comps, pad, width), BF16),
                pltpu.VMEM((5, 1, tile), jnp.int32),
                pltpu.VMEM((far_count * rank, 4 * table_rows), BF16),
                pltpu.VMEM((near_count, tile, 3 * tile), BF16),
                pltpu.VMEM((tile, 2 * tile + pad), BF16),
                pltpu.VMEM((3, piece_rows, width), F32),
                pltpu.VMEM((piece_rows, width), F32),
                pltpu.VMEM((n // 2, piece_rows, width), F32),
                pltpu.VMEM((2, table_rows, width), F32),
                pltpu.VMEM((groups, rows // groups, 2 * table_rows), F32),
                pltpu.VMEM((groups, rows // groups, 2 * table_rows), F32),
                pltpu.VMEM((rows // groups, 2 * table_rows), BF16),
                pltpu.VMEM((rows // groups, 2 * table_rows), BF16),
                pltpu.VMEM((groups, rows // groups, 2 * table_rows), BF16),
                pltpu.VMEM((groups, rows, width), BF16),
                pltpu.VMEM((groups, rows, width), BF16),
                pltpu.VMEM((2, rows // 2, width), BF16),
                pltpu.VMEM((rows, width), F32),
                pltpu.VMEM((rows, 2 * width), F32),
                *(pltpu.VMEM((slots, tile, size), BF16) for size in (width, width, 2 * width) for _ in range(comps)),
            ],
            compiler_params=pltpu.CompilerParams(
                collective_id=0, has_side_effects=True, vmem_limit_bytes=28 * 1024 * 1024
            ),
        )(*(pltpu.with_memory_space_constraint(operand, pltpu.HBM) for operand in operands))

    placed = (
        P(None, "clu", None),
        P("clu"),
        P(None, None, None, "clu"),
        P("clu", "grp", None, None),
        P("clu", "grp"),
        P("clu", "grp", None, None),
        P("clu", "grp", None, None),
        P("clu", "grp"),
        P("clu", "grp"),
        P("clu", "grp"),
    )
    return jax.shard_map(
        on_device, mesh=mesh, in_specs=placed, out_specs=P(None, "clu", "grp"), check_vma=False
    )
```

```python
import functools

import jax
import jax.numpy as jnp
from jax import lax
from jax.experimental import pallas as pl
from jax.experimental.pallas import tpu as pltpu
from jax.sharding import PartitionSpec as P

MESH = pl.DeviceIdType.MESH
F32, BF16 = jnp.float32, jnp.bfloat16
SENDS = 48


def kernel(n, groups, levels, rank, comps, *refs):
    dma = pltpu.SemaphoreType.DMA

    def scoped(*sems):
        body(n, groups, levels, rank, comps, *sems, *refs)

    pl.run_scoped(
        scoped,
        dma((9,)), dma((groups,)), dma((SENDS,)), dma((n // 2,)),
        dma((5,)), dma((groups,)), dma((groups, comps + 1, 2)), dma((groups, comps + 1)), dma((groups,)), dma((1,)),
        dma((1,)), dma((n // 2,)), dma((1,)), dma((2, groups)), dma((groups, 2)), dma((2,)),
    )


def body(
    n, groups, levels, rank, comps,
    local_sem, own_sem, send_sem, piece_send, order_recv, mate_recv, z_recv, across_recv, ext_recv, near_recv,
    pair_recv, piece_recv, table_recv, w_recv, y_recv, mid_recv,
    forces, order_hbm, bases_hbm, tiles_hbm, near_col_hbm, basis_hbm, coupling_hbm, scale_hbm, ranks_hbm, targets_hbm,
    out,
    order, bases, coupling, near_col, scale, ranks, targets, tiles, basis,
    ext_out, ext_near, orders, spread, picks, own_pick, piece_out, piece_mate, pieces,
    table, w_out, w_in, w_own, w_low, w_all, y_out, y_in, y_mid, totals, pair_total,
    *blocks,
):
    g, c = lax.axis_index("grp"), lax.axis_index("clu")
    core = lax.rem(c, 2)
    tile, columns = forces.shape[1:]
    width = columns // groups
    quarter = tile // 4
    rows = comps * tile
    near_count = tiles.shape[0]
    far_count = targets.shape[1]
    half = n // 2
    cut = rank // 2
    piece_rows = levels * cut
    spans = [(level, 2 ** (level + 1)) for level in range(levels)]
    table_rows = sum(count - 1 for _, count in spans) * cut
    last = groups - 1
    own_blocks, far_blocks, side_blocks = (blocks[at * comps:(at + 1) * comps] for at in range(3))
    edge = 7 * core
    flip = 1 - jnp.minimum(c // 2, 1)

    def at_clu(by):
        return {"grp": g, "clu": lax.rem(c + by + n, n)}

    partners = (g, g + 1 - 2 * lax.rem(g, 2), lax.rem(g + 2, groups), groups - 1 - g)

    def at_grp(i):
        return {"grp": partners[i], "clu": c}

    mate = {"grp": g, "clu": c + 1 - 2 * core}
    sends = []

    def remote(src, dst, recv, where, index=0):
        return pltpu.make_async_remote_copy(
            src_ref=src, dst_ref=dst, send_sem=send_sem.at[index], recv_sem=recv, device_id=where, device_id_type=MESH
        )

    def push(copies, bytes_of):
        assert len(sends) < SENDS
        for src, dst, recv, where in copies:
            remote(src, dst, recv, where, len(sends)).start()
        sends.append(remote(bytes_of, bytes_of, near_recv.at[0], mate, len(sends)))

    def landed(ref, recv):
        remote(ref, ref, recv, mate).wait_recv()

    def several(count):
        return own_blocks[0].at[0:count]

    def columns_of(i, d):
        return forces.at[d, :, pl.ds(pl.multiple_of(partners[i] * width, width), width)]

    def place_of(i, p, d, lo=0, hi=tile):
        if i == 0:
            return own_blocks[d].at[p, lo:hi]
        if i == last:
            return far_blocks[d].at[p, lo:hi]
        return side_blocks[d].at[p, lo:hi, pl.ds((i - 1) * width, width)]

    chunks = [(d, 0, tile) for d in range(comps - 1)]
    chunks += [(comps - 1, 0, tile // 2), (comps - 1, tile // 2, tile)]
    parts = range(len(chunks))

    def part(i, p, k):
        return place_of(i, p, *chunks[k])

    def part_bytes(k, count):
        return own_blocks[0].at[0:count, 0:chunks[k][2] - chunks[k][1]]

    def edge_rows(i, p, d):
        return place_of(i, p, d, 0, quarter)

    small = [
        pltpu.make_async_copy(src, dst, local_sem.at[at])
        for at, (src, dst) in enumerate((
            (order_hbm, order), (coupling_hbm, coupling), (targets_hbm, targets), (ranks_hbm, ranks),
            (scale_hbm, scale), (basis_hbm, basis), (bases_hbm, bases), (near_col_hbm, near_col), (tiles_hbm, tiles),
        ))
    ]
    for copy in small[:6]:
        copy.start()
    for i in (last, 0, 1, 2):
        for d in range(comps):
            pltpu.make_async_copy(columns_of(i, d), place_of(i, 3 + core, d), own_sem.at[i]).start()
    for copy in small[6:]:
        copy.start()

    barrier = pltpu.get_barrier_semaphore()

    def greet(d, carry):
        pl.semaphore_signal(barrier, inc=1, device_id=at_clu(d), device_id_type=MESH)
        return carry

    lax.fori_loop(1, n, greet, 0)
    for d in range(1, groups):
        pl.semaphore_signal(barrier, inc=1, device_id=at_grp(d), device_id_type=MESH)

    for block in blocks:
        block[edge, quarter:, :] = jnp.zeros((tile - quarter, block.shape[2]), BF16)
    ext_near[:, quarter:, :] = jnp.zeros((comps, ext_near.shape[1] - quarter, width), BF16)

    for copy in small[1:5]:
        copy.wait()
    lane = lax.broadcasted_iota(jnp.int32, (rank, 2 * table_rows), 1)
    row = lax.broadcasted_iota(jnp.int32, (rank, 2 * table_rows), 0)
    lane_row = (lane // table_rows) * cut + lax.rem(lane, cut)
    lane_slot = lax.rem(lane, table_rows) // cut
    repeat = (lane_row == row).astype(F32).astype(BF16)
    wide = jnp.dot(coupling[...], repeat, preferred_element_type=F32)
    for b in range(far_count):
        target = targets[0, b]
        slot_of, base, offset = target, 0, 0
        for level, count in spans:
            own = (c // 2) // (half // count)
            here = target - base - own - 1
            here = jnp.where(here < 0, here + count, here) + offset
            slot_of = jnp.where((target >= base) & (target < base + count), here, slot_of)
            base, offset = base + count, offset + count - 1
        keep = (lane_slot == slot_of) & (lane_row < ranks[0, b])
        scaled = jnp.where(keep, wide[b * rank:(b + 1) * rank, :] * scale[0, b], 0.0)
        high = scaled.astype(BF16)
        spread[b * rank:(b + 1) * rank, :2 * table_rows] = high
        spread[b * rank:(b + 1) * rank, 2 * table_rows:] = (scaled - high.astype(F32)).astype(BF16)
    small[5].wait()
    folded = lax.dot_general(basis[...], spread[...], (((0,), (0,)), ((), ())), preferred_element_type=F32)
    folded = folded[:, :2 * table_rows] + folded[:, 2 * table_rows:]
    w_out[...] = folded.reshape(groups, rows // groups, 2 * table_rows)

    sub = lax.broadcasted_iota(jnp.int32, (tile, tile), 0)
    lan = lax.broadcasted_iota(jnp.int32, (tile, tile), 1)
    upto = (sub <= lan).astype(BF16)

    def ranked(chosen):
        spots = jnp.broadcast_to(chosen.astype(F32), (8, tile)).astype(BF16)
        return (jnp.dot(spots, upto, preferred_element_type=F32)[0:1, :] - 1.0).astype(jnp.int32)

    def wrapped(spot):
        spot = jnp.where(spot < 0, spot + n * tile, spot)
        return jnp.where(spot >= n * tile, spot - n * tile, spot)

    def one_hot(spot, store, count):
        down = jnp.broadcast_to(spot.astype(F32), (128, tile)).T
        at = lax.broadcasted_iota(jnp.int32, (tile, 128), 1).astype(F32)
        for j in range(count):
            store(j, (down == at + float(j * 128)).astype(F32).astype(BF16))

    def own_arrived(i):
        pltpu.make_async_copy(several(comps), several(comps), own_sem.at[i]).wait()

    small[0].wait()
    own_arrived(last)
    pl.semaphore_wait(barrier, n - 1 + groups - 1)

    for by in (-1, 1, -2, 2):
        push([(order, orders.at[2 - by], order_recv.at[2 - by], at_clu(by))], order)

    def send_z(i, k):
        push(
            [
                (
                    part(i, 3 + core, k), part(i, 1 + core + 4 * side, k), z_recv.at[i, k, side],
                    at_clu(2 - 4 * side),
                )
                for side in (flip, 1 - flip)
            ],
            part_bytes(k, 2),
        )

    for k in range(2):
        send_z(last, k)
    push(
        [(w_out.at[partners[i]], w_in.at[i], w_recv.at[0, i], at_grp(i)) for i in range(1, groups)],
        w_out.at[0:groups - 1],
    )

    def send_mate(i):
        push(
            [(place_of(i, 3 + core, d), place_of(i, 3 + core, d), mate_recv.at[i], mate) for d in range(comps)],
            several(comps),
        )

    send_mate(last)
    own_arrived(0)
    send_mate(0)

    def order_landed(by):
        landed(orders.at[2 + by], order_recv.at[2 + by])

    spot = wrapped(order[...] - (c - core) * tile)
    beyond = spot >= 2 * tile
    spot = jnp.where(beyond, 2 * tile + ranked(beyond), spot)

    def store_own(j, value):
        own_pick[:, j * 128:(j + 1) * 128] = value

    one_hot(spot, store_own, own_pick.shape[1] // 128)

    for by in (-1, 1):
        order_landed(by)
    away = orders[1 + 2 * core] - c * tile
    chosen = (away >= 0) & (away < tile)
    place = jnp.where(chosen, ranked(chosen), -1)
    left = (lax.broadcasted_iota(jnp.int32, (128, tile), 0) == place).astype(F32).astype(BF16)
    right = (sub == away).astype(F32).astype(BF16)
    pick = lax.dot_general(left, right, (((1,), (1,)), ((), ())), preferred_element_type=F32).astype(BF16)

    def pick_edge(at, own):
        for d in range(comps):
            ext_out[at, d] = jnp.dot(pick, own[d][3 + core], preferred_element_type=F32).astype(BF16)[:quarter]

    for k in parts[2:]:
        send_z(last, k)
    pick_edge(1, far_blocks)
    push(
        [
            (ext_out.at[1, d], edge_rows(last, 7 - edge, d), ext_recv.at[last], at_clu(6 * core - 3))
            for d in range(comps)
        ],
        ext_out.at[1],
    )
    pick_edge(0, own_blocks)
    for i in (1, 2):
        own_arrived(i)
        send_mate(i)

    for by in (-2, 2):
        order_landed(by)
    orders[2] = order[...]
    small[7].wait()
    starts = []
    for j in range(near_count):
        spot0 = near_col[0, j] - c + 2
        spot0 = jnp.where(spot0 < 0, spot0 + n, spot0)
        spot0 = jnp.clip(jnp.where(spot0 >= n, spot0 - n, spot0), 0, 4)
        starts.append(spot0 + core)
        spot = wrapped(orders[spot0] - (c + spot0 - 3) * tile)
        low = 2 * core * tile
        beyond = (spot >= low) & (spot < low + tile) & (spot0 == 4 * core)
        spot = jnp.where(beyond, low + ranked(beyond), spot)

        def store_pick(at, value, j=j):
            picks[j, :, at * 128:(at + 1) * 128] = value

        one_hot(spot, store_pick, picks.shape[2] // 128)

    def relay(i, k):
        copies = []
        for side, p in enumerate((1 + core, 5 + core)):
            landed(part(i, p, k), z_recv.at[i, k, side])
            if i == last:
                for to, at in ((1, 2), (2, 1)):
                    copies.append((part(i, p, k), part(at, p, k), z_recv.at[at, k, side], at_grp(to)))
            copies.append((part(i, p, k), part(i, p, k), across_recv.at[i, k], mate))
        push(copies, part_bytes(k, len(copies)))

    def take(i, *ks):
        for k in ks:
            landed(part_bytes(k, 2), across_recv.at[i, k])

    def gathered(block, lo, hi):
        found = []
        for j in range(near_count):
            parts_of = [
                jnp.dot(
                    picks[j], block[d][pl.ds(starts[j], 3)].reshape(3 * tile, block[d].shape[2]),
                    preferred_element_type=F32,
                ).astype(BF16)
                for d in range(lo, hi)
            ]
            found.append(jnp.concatenate(parts_of, axis=0))
        return found

    def product(found, lo, hi, top, bottom):
        acc = None
        for j in range(near_count):
            term = jnp.dot(tiles[j, top:bottom, lo * tile:hi * tile], found[j], preferred_element_type=F32)
            acc = term if acc is None else acc + term
        return acc

    def near(block, lo, hi):
        return product(gathered(block, lo, hi), lo, hi, 0, rows)

    mid = rows // 2

    relay(last, 0)
    relay(last, 1)
    push([(ext_out.at[0], ext_near.at[:, 0:quarter], near_recv.at[0], at_clu(2 * core - 1))], ext_out.at[0])
    for i in range(1, groups):
        landed(w_in.at[i], w_recv.at[0, i])
    summed = w_out[g]
    for i in range(1, groups):
        summed = summed + w_in[i]
    high = summed.astype(BF16)
    w_own[...] = high
    w_all[g] = high
    w_low[...] = (summed - high.astype(F32)).astype(BF16)
    relay(last, 2)
    relay(last, 3)
    for k in parts[:2]:
        send_z(0, k)
    for i in (1, 2):
        relay(i, 0)
    landed(ext_out.at[1], ext_recv.at[last])
    push(
        [
            (edge_rows(last, edge, d), edge_rows(at, edge, d), ext_recv.at[at], at_grp(to))
            for to, at in ((1, 2), (2, 1)) for d in range(comps)
        ],
        ext_out,
    )
    landed(several(comps), mate_recv.at[last])
    small[8].wait()
    take(last, 0, 1, 2, 3)
    y_out[last] = near(far_blocks, 0, comps).astype(BF16)
    push(
        [
            (y_out.at[last, 0:mid], y_mid.at[0], mid_recv.at[0], at_grp(1)),
            (y_out.at[last, mid:rows], y_mid.at[1], mid_recv.at[1], at_grp(2)),
        ],
        y_out.at[last],
    )
    push([(w_own, w_all.at[g], w_recv.at[1, i], at_grp(i)) for i in range(1, groups)], w_all.at[0:groups - 1])

    for k in (1, 2):
        for i in (1, 2):
            relay(i, k)
    small[6].wait()
    landed(ext_out.at[0], near_recv.at[0])
    push(
        [
            (ext_near.at[d, 0:quarter], edge_rows(0, edge, d), ext_recv.at[0], at_clu(2 - 4 * core))
            for d in range(comps)
        ],
        ext_out.at[0],
    )
    landed(several(comps), mate_recv.at[0])
    chip = jnp.concatenate([own_blocks[d][3:5].reshape(2 * tile, width) for d in range(comps)], axis=1)
    near_edge = jnp.concatenate([ext_near[d] for d in range(comps)], axis=1)
    x = jnp.dot(own_pick[:, :2 * tile], chip, preferred_element_type=F32)
    x = (x + jnp.dot(own_pick[:, 2 * tile:], near_edge, preferred_element_type=F32)).astype(BF16)
    stacked = jnp.concatenate([x[:, d * width:(d + 1) * width] for d in range(comps)], axis=0)
    weights = jnp.concatenate(
        [
            jnp.concatenate([bases[level, d, h * cut:(h + 1) * cut] for d in range(comps)], axis=1)
            for h in range(2) for level in range(levels)
        ],
        axis=0,
    )
    piece = jnp.dot(weights, stacked, preferred_element_type=F32)
    for h in range(2):
        piece_out[h] = piece[h * piece_rows:(h + 1) * piece_rows]
    push([(piece_out.at[1 - core], piece_mate, pair_recv.at[0], mate)], piece_mate)
    for i in (1, 2):
        relay(i, 3)

    landed(piece_mate, pair_recv.at[0])
    pair = piece_out[core] + piece_mate[...]
    piece_out[2] = pair
    pieces[c // 2] = pair

    def piece_copy(d):
        return pltpu.make_async_remote_copy(
            src_ref=piece_out.at[2], dst_ref=pieces.at[c // 2], send_sem=piece_send.at[d],
            recv_sem=piece_recv.at[c // 2], device_id=at_clu(2 * d), device_id_type=MESH,
        )

    def start_piece(d, carry):
        piece_copy(d).start()
        return carry

    lax.fori_loop(1, half, start_piece, 0)
    for k in parts[2:]:
        send_z(0, k)

    for i in (1, 2):
        landed(several(comps), mate_recv.at[i])
        landed(ext_out.at[0], ext_recv.at[i])
        take(i, 0, 1, 2, 3)
    found = gathered(side_blocks, 0, comps)

    def send_y(i, h, value):
        here = pl.ds(h * mid, mid)
        y_out[i, h * mid:(h + 1) * mid] = value.astype(BF16)
        push([(y_out.at[i, here], y_in.at[i, here], y_recv.at[i, h], at_grp(i))], y_mid.at[0])

    for h, plain, added in ((0, 1, 2), (1, 2, 1)):
        both = product(found, 0, comps, h * mid, (h + 1) * mid)
        send_y(plain, h, both[:, (plain - 1) * width:plain * width])
        landed(y_mid.at[h], mid_recv.at[h])
        send_y(added, h, both[:, (added - 1) * width:added * width] + y_mid[h].astype(F32))
    relay(0, 0)
    relay(0, 1)

    landed(ext_out.at[0], ext_recv.at[0])
    take(0, 0)
    totals[...] = near(own_blocks, 0, 1)

    def await_piece(d, carry):
        source = lax.rem(c // 2 + d, half)
        landed(pieces.at[source], piece_recv.at[source])
        return carry

    lax.fori_loop(1, half, await_piece, 0)
    at = 0
    for level, count in spans:
        members = half // count
        own = (c // 2) // members
        for step in range(count - 1):
            k = lax.rem(own + 1 + step, count)
            entry = lax.fori_loop(
                0, members,
                lambda m, acc, k=k, members=members, level=level: acc
                + pieces[k * members + m, level * cut:(level + 1) * cut, :],
                jnp.zeros((cut, width), F32),
            )
            table[core, at:at + cut, :] = entry
            at += cut
    push([(table.at[core], table.at[core], table_recv.at[0], mate)], table.at[0])

    take(0, 1)
    totals[...] += near(own_blocks, 1, 2)
    relay(0, 2)
    for i in range(1, groups):
        landed(w_own, w_recv.at[1, i])
    landed(table.at[0], table_recv.at[0])
    entries = table[...].reshape(2 * table_rows, width)
    high = entries.astype(BF16)
    low = (entries - high.astype(F32)).astype(BF16)
    weights = w_all[...].reshape(rows, 2 * table_rows)
    answer = jnp.dot(weights, high, preferred_element_type=F32) + jnp.dot(weights, low, preferred_element_type=F32)
    totals[...] += answer
    own_rows = pl.ds(pl.multiple_of(g * (rows // groups), rows // groups), rows // groups)
    totals[own_rows] += jnp.dot(w_low[...], high, preferred_element_type=F32)
    relay(0, 3)
    for copy in sends:
        copy.wait_send()

    def end_piece(d, carry):
        piece_copy(d).wait_send()
        return carry

    lax.fori_loop(1, half, end_piece, 0)

    take(0, 2, 3)
    totals[...] += near(own_blocks, comps - 1, comps)

    for i in (1, 2):
        for h in range(2):
            landed(y_mid.at[0], y_recv.at[i, h])
    out[...] = (totals[...] + y_in[1].astype(F32) + y_in[2].astype(F32)).reshape(comps, tile, width)


def solution(mesh):
    n, groups = mesh.shape["clu"], mesh.shape["grp"]

    def on_device(forces, order, bases, near_tiles, near_col, far_basis, far_coupling, far_scale, far_rank, far_target):
        comps, tile, columns = forces.shape
        levels, rank = bases.shape[:2]
        near_count, far_count = near_tiles.shape[1], far_basis.shape[1]
        width, rows, quarter = columns // groups, comps * tile, tile // 4
        cut = rank // 2
        piece_rows = levels * cut
        table_rows = sum(2 ** (level + 1) - 1 for level in range(levels)) * cut
        slots = 8
        pad = 128
        vmem, hbm = (pl.BlockSpec(memory_space=m) for m in (pltpu.VMEM, pl.ANY))
        operands = (
            forces,
            order.reshape(1, tile),
            jnp.transpose(bases, (0, 2, 1, 3)),
            near_tiles.reshape(near_count, rows, rows),
            near_col,
            far_basis.reshape(far_count * rank, rows),
            far_coupling.reshape(far_count * rank, rank),
            far_scale,
            far_rank,
            far_target,
        )
        return pl.pallas_call(
            functools.partial(kernel, n, groups, levels, rank, comps),
            out_shape=jax.ShapeDtypeStruct((comps, tile, width), F32),
            in_specs=[hbm] * len(operands),
            out_specs=vmem,
            scratch_shapes=[
                pltpu.VMEM((1, tile), jnp.int32),
                pltpu.VMEM((levels, comps, rank, tile), BF16),
                pltpu.VMEM((far_count * rank, rank), BF16),
                pltpu.SMEM((1, near_count), jnp.int32),
                pltpu.SMEM((1, far_count), F32),
                pltpu.SMEM((1, far_count), jnp.int32),
                pltpu.SMEM((1, far_count), jnp.int32),
                pltpu.VMEM((near_count, rows, rows), BF16),
                pltpu.VMEM((far_count * rank, rows), BF16),
                pltpu.VMEM((2, comps, quarter, width), BF16),
                pltpu.VMEM((comps, pad, width), BF16),
                pltpu.VMEM((5, 1, tile), jnp.int32),
                pltpu.VMEM((far_count * rank, 4 * table_rows), BF16),
                pltpu.VMEM((near_count, tile, 3 * tile), BF16),
                pltpu.VMEM((tile, 2 * tile + pad), BF16),
                pltpu.VMEM((3, piece_rows, width), F32),
                pltpu.VMEM((piece_rows, width), F32),
                pltpu.VMEM((n // 2, piece_rows, width), F32),
                pltpu.VMEM((2, table_rows, width), F32),
                pltpu.VMEM((groups, rows // groups, 2 * table_rows), F32),
                pltpu.VMEM((groups, rows // groups, 2 * table_rows), F32),
                pltpu.VMEM((rows // groups, 2 * table_rows), BF16),
                pltpu.VMEM((rows // groups, 2 * table_rows), BF16),
                pltpu.VMEM((groups, rows // groups, 2 * table_rows), BF16),
                pltpu.VMEM((groups, rows, width), BF16),
                pltpu.VMEM((groups, rows, width), BF16),
                pltpu.VMEM((2, rows // 2, width), BF16),
                pltpu.VMEM((rows, width), F32),
                pltpu.VMEM((rows, 2 * width), F32),
                *(pltpu.VMEM((slots, tile, size), BF16) for size in (width, width, 2 * width) for _ in range(comps)),
            ],
            compiler_params=pltpu.CompilerParams(
                collective_id=0, has_side_effects=True, vmem_limit_bytes=28 * 1024 * 1024
            ),
        )(*(pltpu.with_memory_space_constraint(operand, pltpu.HBM) for operand in operands))

    placed = (
        P(None, "clu", None),
        P("clu"),
        P(None, None, None, "clu"),
        P("clu", "grp", None, None),
        P("clu", "grp"),
        P("clu", "grp", None, None),
        P("clu", "grp", None, None),
        P("clu", "grp"),
        P("clu", "grp"),
        P("clu", "grp"),
    )
    return jax.shard_map(
        on_device, mesh=mesh, in_specs=placed, out_specs=P(None, "clu", "grp"), check_vma=False
    )
```
